256 devices in a mesh: gx: 8 (over y, core), gy: 8 (over z), gz: 4 (over x).
Axes of the slice: x: 4, y: 4, z: 8, core: 2. Of those that a mesh axis runs over, the one named last changes fastest.
Arguments:
- density: float32 [256, 128, 512], P('gx', 'gy', 'gz'), may hold values from -8 to 8
Outputs:
- potential: float32 [256, 128, 512], P('gx', 'gy', 'gz')
The draws below stay inside these ranges and needn't reach their ends.
All inputs are finite; a program needn't handle non-finite values.
Results may differ from the reference program's by a relative error of at most 0.00002.
Values sent between devices are 32-bit elements; how exact they have to be, the bound alone decides.
A program may use at most 128 MiB of HBM per device.

```python
import jax
import jax.numpy as jnp
from jax import lax

LEVELS = 7
CSWEEPS = 4
NX = 256
NY = 128
NZ = 512


def rough_field(key, shape):
    return jnp.clip(jax.random.normal(key, shape, jnp.float32), -4.0, 4.0)


def draw_density(key, part):
    first_key = jax.random.fold_in(key, 21)
    second_key = jax.random.fold_in(key, 22)
    shape = (NX, NY, NZ)
    first = rough_field(first_key, shape)
    second = rough_field(second_key, shape)
    beside_all = jnp.zeros(shape, jnp.float32)
    for which in range(3):
        beside_all = beside_all + jnp.roll(first, 1, which) + jnp.roll(first, -1, which)
    sharp = 6.0 * first - beside_all
    total = 0.4 * sharp + 0.4 * second
    return jnp.clip(total, -8.0, 8.0).astype(jnp.float32)


def setup_inputs(seed: int = 0) -> dict:
    key_of = jax.random.split(jax.random.key(seed), 2)
    density = draw_density(jax.random.fold_in(key_of[1], 71), 0)
    return dict(density=density)


rsd_beta = 0.5
centre = 4.0 + 2.0 * (1.0 + rsd_beta)


def stencil_sum(padded):
    plane = padded[2:, 1:-1, 1:-1] + padded[:-2, 1:-1, 1:-1] + padded[1:-1, 2:, 1:-1] + padded[1:-1, :-2, 1:-1]
    sight = padded[1:-1, 1:-1, 2:] + padded[1:-1, 1:-1, :-2]
    return plane + (1.0 + rsd_beta) * sight


def parity_of(shape):
    total = lax.broadcasted_iota(jnp.int32, shape, 0) + lax.broadcasted_iota(jnp.int32, shape, 1)
    total = total + lax.broadcasted_iota(jnp.int32, shape, 2)
    return total % 2


def half_sweep(field, source, scale, chosen):
    update = (source / scale + stencil_sum(jnp.pad(field, 1))) / centre
    return jnp.where(chosen, update, field)


def full_sweep(field, source, scale, parity):
    field = half_sweep(field, source, scale, parity == 0)
    return half_sweep(field, source, scale, parity == 1)


def restrict(residue):
    shape = residue.shape
    blocks = residue.reshape(shape[0] // 2, 2, shape[1] // 2, 2, shape[2] // 2, 2)
    return jnp.mean(blocks, axis=(1, 3, 5))


def prolong(coarse):
    return jnp.repeat(jnp.repeat(jnp.repeat(coarse, 2, 0), 2, 1), 2, 2)


def local_cycle(source, level):
    scale = 0.25 ** level
    parity = parity_of(source.shape)
    field = jnp.zeros_like(source)
    if level == LEVELS - 1:
        for number in range(CSWEEPS):
            field = full_sweep(field, source, scale, parity)
        return field
    for number in range(2):
        field = full_sweep(field, source, scale, parity)
    residue = source - scale * (centre * field - stencil_sum(jnp.pad(field, 1)))
    field = field + prolong(local_cycle(restrict(residue), level + 1))
    for number in range(2):
        field = full_sweep(field, source, scale, parity)
    return field


def reference(density):
    return local_cycle(density, 0)
```

```python
import itertools

import jax
import jax.numpy as jnp
from jax import lax
from jax.experimental import pallas as pl
from jax.experimental.pallas import tpu as pltpu
from jax.sharding import PartitionSpec as P

MESH = pl.DeviceIdType.MESH
F32 = jnp.float32
HIGHEST = lax.Precision.HIGHEST

NGX, NGY, NGZ = 8, 8, 4
BX, BY, BZ = 32, 16, 128
CSWEEPS = 4
BETA1 = 1.5
INV = 1.0 / (4.0 + 2.0 * BETA1)

D26 = [d for d in itertools.product((-1, 0, 1), repeat=3) if d != (0, 0, 0)]
D44 = [d for d in itertools.product((-1, 0, 1), (-2, -1, 0, 1, 2), (-1, 0, 1)) if d != (0, 0, 0)]
XY4 = [(-1, -1), (-1, 1), (1, -1), (1, 1)]
Z18 = [d for d in D26 if d[2] != 0]


def roll(x, shift, axis):
    size = x.shape[axis]
    shift = shift % size
    return x if shift == 0 else pltpu.roll(x, shift, axis)


def iota(shape, dim):
    return lax.broadcasted_iota(jnp.int32, shape, dim)


def both(cond, a, b):
    return jnp.where(cond, a, b)


def side(n):
    return 0 if n < 0 else 1


def kernel(
    f_hbm, out_hbm,
    fm, fh, vm, vh, mm, mh, s0, pe0m, pe0h, tmp0,
    g1, v1, m1, s1, pe1, tmp1,
    g2, v2, m2, s2, pe2, tmp2,
    fy0, fz0, vy0, vz0, fk1, fz1, vk1, vz1, ft2, vt2,
    fx_r, fy_r, fxy_r, fz_r, vx_r, vy_r, vxy_r, vz_r,
    f1x_r, f1y_r, f1xy_r, f1z_r, v1x_r, v1y_r, v1xy_r, v1z_r,
    f2_r, v2_r,
    t3, gy_r, gzb, gxb, g3, v3,
    io_sem, s_f0, r_f0, s_v0, r_v0, s_f1, r_f1, s_v1, r_v1, s_f2, r_f2, s_v2, r_v2, s_g, r_g,
):
    ix, iy, iz = lax.axis_index("gx"), lax.axis_index("gy"), lax.axis_index("gz")

    def there(n):
        nx, ny, nz = ix + n[0], iy + n[1], iz + n[2]
        return (nx >= 0) & (nx < NGX) & (ny >= 0) & (ny < NGY) & (nz >= 0) & (nz < NGZ)

    def at(n):
        return (
            jnp.clip(ix + n[0], 0, NGX - 1),
            jnp.clip(iy + n[1], 0, NGY - 1),
            jnp.clip(iz + n[2], 0, NGZ - 1),
        )

    def neg(n):
        return (-n[0], -n[1], -n[2])

    load = pltpu.make_async_copy(f_hbm, fm.at[pl.ds(4, BX), pl.ds(8, BY), :], io_sem.at[0])
    load.start()

    barrier = pltpu.get_barrier_semaphore()
    count = 0
    for d in D44:
        ok = there(d)
        count = count + ok.astype(jnp.int32)

        @pl.when(ok)
        def _(d=d):
            pl.semaphore_signal(barrier, inc=1, device_id=at(d), device_id_type=MESH)

    lines = []
    for k in range(1, NGY):
        lines.append((ix, lax.rem(iy + k, NGY), iz))
    for k in range(1, NGZ):
        lines.append((ix, iy, lax.rem(iz + k, NGZ)))
    for k in range(1, NGX):
        lines.append((lax.rem(ix + k, NGX), iy, iz))
    for peer in lines:
        pl.semaphore_signal(barrier, inc=1, device_id=peer, device_id_type=MESH)

    lane = iota((8, 128), 1)
    row = iota((8, 128), 0)

    def fill_masks(ref, rows, lanes_pos, lanes_ok, rows_pos, rows_ok):
        ok = rows_ok & lanes_ok
        par = (rows_pos + lanes_pos) & 1
        ref[0] = jnp.where(ok & (par == 0), 1.0, 0.0)
        ref[1] = jnp.where(ok & (par == 1), 1.0, 0.0)
        ref[2] = jnp.zeros((24, 128), F32)
        ref[3] = jnp.where(ok, 1.0, 0.0)

    r24, l24 = iota((24, 128), 0), iota((24, 128), 1)
    y0 = iy * BY + r24 - 4
    oky0 = (y0 >= 0) & (y0 < NGY * BY)
    z0 = iz * BZ + l24
    fill_masks(mm, 24, z0, z0 >= 0, y0, oky0)
    z0h = iz * BZ + l24 + jnp.where(l24 < 64, 128, -128)
    fill_masks(mh, 24, z0h, (z0h >= 0) & (z0h < NGZ * BZ) & ((l24 < 4) | (l24 >= 124)), y0, oky0)
    y1 = iy * 8 + r24 - 8
    z1 = iz * 64 + l24 - 6
    fill_masks(m1, 24, z1, (z1 >= 0) & (z1 < NGZ * 64) & (l24 < 76), y1, (y1 >= 0) & (y1 < NGY * 8))
    x2 = ix * 8 + r24 - 8
    z2 = iz * 32 + l24 - 7
    fill_masks(m2, 24, z2, (z2 >= 0) & (z2 < NGZ * 32) & (l24 < 46), x2, (x2 >= 0) & (x2 < NGX * 8))

    def pick(start, i, total, colour):
        pos = start + i
        return jnp.where((pos >= 0) & (pos < total), (pos + colour + 64) & 1, 2)

    def picked(start, i, total):
        pos = start + i
        return jnp.where((pos >= 0) & (pos < total), 3, 2)

    base0, base1, base2 = ix * BX - 4, ix * 16 - 6, iy * 4 - 7

    for ref in (vm, vh, v1, g1, v2, g2):
        n = ref.shape[0]

        @pl.loop(0, n)
        def _(i, ref=ref):
            ref[i] = jnp.zeros(ref.shape[1:], F32)

    @pl.loop(0, 40)
    def _(i):
        v3[i] = jnp.zeros((8, 128), F32)

    load.wait()

    def pack0(src, yp, zp):
        def ypack(t, c):
            yp[0, t] = jnp.concatenate([src[4 + 2 * t, 8:12, :], src[5 + 2 * t, 8:12, :]], axis=0)
            yp[1, t] = jnp.concatenate([src[4 + 2 * t, 20:24, :], src[5 + 2 * t, 20:24, :]], axis=0)
            return c

        lax.fori_loop(0, 16, ypack, 0, unroll=4)
        lane16 = iota((16, 128), 1)
        lo = jnp.zeros((16, 128), F32)
        hi = jnp.zeros((16, 128), F32)
        for x in range(BX):
            p = roll(src[4 + x, 8:24, :], 4 * x, 1)
            lo = jnp.where(lane16 // 4 == x, p, lo)
            hi = jnp.where(lane16 // 4 == (x - 1) % BX, p, hi)
        zp[0] = lo
        zp[1] = hi

    def copies0(src, yp, zp, xr, yr, xyr, zr, ss, rs, directions):
        out = []
        for d in directions:
            k = D26.index(d)
            dx, dy, dz = d
            nx, ny = -dx, -dy
            if dz == 0 and dy == 0:
                s = src.at[pl.ds(4 if dx < 0 else 32, 4), pl.ds(8, BY), :]
                t = xr.at[side(nx)]
            elif dz == 0 and dx == 0:
                s, t = yp.at[side(dy)], yr.at[side(ny)]
            elif dz == 0:
                s = yp.at[side(dy), pl.ds(0 if dx < 0 else 14, 2)]
                t = xyr.at[XY4.index((nx, ny))]
            else:
                slot = Z18.index(neg(d))
                if dy == 0:
                    s, t = zp.at[side(dz)], zr.at[slot]
                else:
                    rows = pl.ds(0 if dy < 0 else 8, 8)
                    s, t = zp.at[side(dz), rows], zr.at[slot, rows]
            out.append((d, pltpu.make_async_remote_copy(s, t, ss.at[k], rs.at[k], at(d), MESH)))
        return out

    def start(copies):
        for d, c in copies:
            @pl.when(there(d))
            def _(c=c):
                c.start()

    def arrive(copies):
        for d, c in copies:
            @pl.when(there(neg(d)))
            def _(c=c):
                c.wait_recv()

    def sent(copies):
        for d, c in copies:
            @pl.when(there(d))
            def _(c=c):
                c.wait_send()

    def unpack0(main, halo, xr, yr, xyr, zr):
        def faces(x, c):
            main[x, 8:24, :] = xr[0, x]
            main[36 + x, 8:24, :] = xr[1, x]
            return c

        lax.fori_loop(0, 4, faces, 0, unroll=True)

        def yfaces(t, c):
            for ny, rows in ((0, 4), (1, 24)):
                main[4 + 2 * t, rows : rows + 4, :] = yr[ny, t, 0:4, :]
                main[5 + 2 * t, rows : rows + 4, :] = yr[ny, t, 4:8, :]
            return c

        lax.fori_loop(0, 16, yfaces, 0, unroll=4)
        for k, (nx, ny) in enumerate(XY4):
            x0 = 0 if nx < 0 else 36
            rows = 4 if ny < 0 else 24
            for t in range(2):
                main[x0 + 2 * t, rows : rows + 4, :] = xyr[k, t, 0:4, :]
                main[x0 + 2 * t + 1, rows : rows + 4, :] = xyr[k, t, 4:8, :]
        for xe in range(40):
            nx, x = (-1, 28 + xe) if xe < 4 else ((0, xe - 4) if xe < 36 else (1, xe - 36))
            for ny, src, dst, num in ((-1, 8, 0, 8), (0, 0, 8, 16), (1, 0, 24, 8)):
                low = zr[Z18.index((nx, ny, -1)), src : src + num, :]
                high = zr[Z18.index((nx, ny, 1)), src : src + num, :]
                low = roll(low, 124 - 4 * ((x - 1) % BX), 1)
                high = roll(high, -4 * x, 1)
                halo[xe, dst : dst + num, :] = jnp.where(iota((num, 128), 1) < 64, high, low)

    ef0 = copies0(fm, fy0, fz0, fx_r, fy_r, fxy_r, fz_r, s_f0, r_f0, D26)
    ev0 = copies0(vm, vy0, vz0, vx_r, vy_r, vxy_r, vz_r, s_v0, r_v0, D26)

    pack0(fm, fy0, fz0)
    pl.semaphore_wait(barrier, count + len(lines))
    start(ef0)

    l24b = iota((24, 128), 1)

    def planes0(lo, hi, body, step=2):
        def run(i, c):
            body(lo + i * step)
            return c

        lax.fori_loop(0, (hi - lo) // step, run, 0)

    def shifted(c, h):
        lanes = iota(c.shape, 1)
        cr, hr = roll(c, 1, 1), roll(h, 1, 1)
        cl, hl = roll(c, -1, 1), roll(h, -1, 1)
        zm = jnp.where(lanes == 0, hr, cr) + jnp.where(lanes == 127, hl, cl)
        zh = jnp.where(lanes == 0, cr, hr) + jnp.where(lanes == 127, cl, hl)
        return BETA1 * zm, BETA1 * zh

    def half0(lo, hi, colour, last=False):
        def body(x):
            done = []
            for u in range(2):
                i = x + u
                sel = pick(base0, i, NGX * BX, colour)
                if last:
                    c, h = vm[i, 8:24, :], vh[i, 8:24, :]
                    zm, _ = shifted(c, h)
                    s = vm[i - 1, 8:24, :] + vm[i + 1, 8:24, :] + vm[i, 7:23, :] + vm[i, 9:25, :] + zm
                    m = mm[sel, 4:20, :] > 0.5
                    done.append((jnp.where(m, (fm[i, 8:24, :] + s) * INV, c),))
                    continue
                c, h = vm[i, 4:28, :], vh[i, 4:28, :]
                zm, zh = shifted(c, h)
                s = vm[i - 1, 4:28, :] + vm[i + 1, 4:28, :] + vm[i, 3:27, :] + vm[i, 5:29, :] + zm
                t = vh[i - 1, 4:28, :] + vh[i + 1, 4:28, :] + vh[i, 3:27, :] + vh[i, 5:29, :] + zh
                new = jnp.where(mm[sel] > 0.5, (fm[i, 4:28, :] + s) * INV, c)
                newh = jnp.where(mh[sel] > 0.5, (fh[i, 4:28, :] + t) * INV, h)
                done.append((new, newh))
            for u in range(2):
                if last:
                    vm[x + u, 8:24, :] = done[u][0]
                else:
                    vm[x + u, 4:28, :] = done[u][0]
                    vh[x + u, 4:28, :] = done[u][1]

        planes0(lo, hi, body)

    arrive(ef0)
    unpack0(fm, fh, fx_r, fy_r, fxy_r, fz_r)

    def first0(x):
        for u in range(2):
            i = x + u
            sel = pick(base0, i, NGX * BX, 0)
            vm[i, 4:28, :] = jnp.where(mm[sel] > 0.5, fm[i, 4:28, :] * INV, 0.0)
            vh[i, 4:28, :] = jnp.where(mh[sel] > 0.5, fh[i, 4:28, :] * INV, 0.0)

    planes0(0, 40, first0)
    half0(1, 39, 1)
    half0(2, 38, 0)
    half0(3, 37, 1)

    def resid0(x):
        total = None
        for u in range(2):
            i = x + u
            c, h = vm[i, 8:24, :], vh[i, 8:24, :]
            zm, _ = shifted(c, h)
            s = vm[i - 1, 8:24, :] + vm[i + 1, 8:24, :] + vm[i, 7:23, :] + vm[i, 9:25, :] + zm
            r = fm[i, 8:24, :] - ((4.0 + 2.0 * BETA1) * c - s)
            total = r if total is None else total + r
        s0[(x - 4) // 2] = total

    planes0(4, 36, resid0)

    kk, cc = iota((128, 128), 0), iota((128, 128), 1)
    r01 = jnp.where((kk // 2 == cc - 6) & (cc >= 6) & (cc < 70), 0.5, 0.0)
    rows = []
    for x in range(16):
        rows.append(s0[x, pl.ds(0, 8, stride=2), :] + s0[x, pl.ds(1, 8, stride=2), :])
    b1 = jnp.dot(jnp.concatenate(rows, axis=0), r01, precision=HIGHEST, preferred_element_type=F32)
    for x in range(16):
        g1[6 + x, 16:24, :] = b1[8 * x : 8 * x + 8]

    def pack1(src, pk, zp):
        lo = jnp.zeros((8, 128), F32)
        hi = jnp.zeros((8, 128), F32)
        for t in range(8):
            a, b = src[6 + 2 * t, 16:24, :], src[7 + 2 * t, 16:24, :]
            pk[t] = jnp.where(lane < 64, roll(a, -6, 1), roll(b, 58, 1))
            for x, p in ((2 * t, a), (2 * t + 1, b)):
                lo = jnp.where(lane // 6 == x, roll(p, 6 * x - 6, 1), lo)
                hi = jnp.where(lane // 6 == x, roll(p, 6 * x - 64, 1), hi)
        zp[0] = lo
        zp[1] = hi

    def copies1(pk, zp, xr, yr, xyr, zr, ss, rs):
        out = []
        for k, d in enumerate(D26):
            dx, dy, dz = d
            if dz == 0 and dx == 0:
                s, t = pk, yr.at[side(-dy)]
            elif dz == 0:
                s = pk.at[pl.ds(0 if dx < 0 else 5, 3)]
                t = xr.at[side(-dx)] if dy == 0 else xyr.at[XY4.index((-dx, -dy))]
            else:
                s, t = zp.at[side(dz)], zr.at[Z18.index(neg(d))]
            out.append((d, pltpu.make_async_remote_copy(s, t, ss.at[k], rs.at[k], at(d), MESH)))
        return out

    def unpack1(dst, xr, yr, xyr, zr):
        for xe in range(28):
            nx, x = (-1, 10 + xe) if xe < 6 else ((0, xe - 6) if xe < 22 else (1, xe - 22))
            for ny in (-1, 0, 1):
                rows = slice(16 + 8 * ny, 24 + 8 * ny)
                if nx == 0 and ny == 0:
                    mid = dst[xe, rows, :]
                else:
                    if nx == 0:
                        mid = yr[side(ny), x // 2]
                    else:
                        tile = x // 2 - 5 if nx < 0 else x // 2
                        mid = xr[side(nx), tile] if ny == 0 else xyr[XY4.index((nx, ny)), tile]
                    mid = roll(mid, 6 if x % 2 == 0 else -58, 1)
                low = roll(zr[Z18.index((nx, ny, -1))], -6 * x, 1)
                high = roll(zr[Z18.index((nx, ny, 1))], 70 - 6 * x, 1)
                dst[xe, rows, :] = jnp.where(lane < 6, low, jnp.where(lane < 70, mid, high))

    ef1 = copies1(fk1, fz1, f1x_r, f1y_r, f1xy_r, f1z_r, s_f1, r_f1)
    ev1 = copies1(vk1, vz1, v1x_r, v1y_r, v1xy_r, v1z_r, s_v1, r_v1)
    pack1(g1, fk1, fz1)
    start(ef1)

    def half(v, g, m, base, total, lo, hi, colour):
        def run(j, carry):
            x = lo + 2 * j
            done = []
            for u in range(2):
                i = x + u
                sel = pick(base, i, total, colour)
                c = v[i, 8:32, :]
                s = v[i - 1, 8:32, :] + v[i + 1, 8:32, :] + v[i, 7:31, :] + v[i, 9:33, :]
                s = s + BETA1 * (roll(c, 1, 1) + roll(c, -1, 1))
                done.append(jnp.where(m[sel] > 0.5, (g[i, 8:32, :] + s) * INV, c))
            for u in range(2):
                v[x + u, 8:32, :] = done[u]
            return carry

        lax.fori_loop(0, (hi - lo) // 2, run, 0)

    def first(v, g, m, base, total, lo, hi):
        def run(j, carry):
            for u in range(2):
                i = lo + 2 * j + u
                sel = pick(base, i, total, 0)
                v[i, 8:32, :] = jnp.where(m[sel] > 0.5, g[i, 8:32, :] * INV, 0.0)
            return carry

        lax.fori_loop(0, (hi - lo) // 2, run, 0)

    def residual(v, g, i):
        c = v[i, 16:24, :]
        s = v[i - 1, 16:24, :] + v[i + 1, 16:24, :] + v[i, 15:23, :] + v[i, 17:25, :]
        s = s + BETA1 * (roll(c, 1, 1) + roll(c, -1, 1))
        return g[i, 16:24, :] - ((4.0 + 2.0 * BETA1) * c - s)

    arrive(ef1)
    unpack1(g1, f1x_r, f1y_r, f1xy_r, f1z_r)
    lev1 = (v1, g1, m1, base1, NGX * 16)
    first(*lev1, 2, 26)
    half(*lev1, 3, 25, 1)
    half(*lev1, 4, 24, 0)
    half(*lev1, 5, 23, 1)
    for x in range(8):
        s1[8 * x : 8 * x + 8, :] = residual(v1, g1, 6 + 2 * x) + residual(v1, g1, 7 + 2 * x)

    r12 = jnp.where(((kk - 6) // 2 == cc - 7) & (kk >= 6) & (kk < 70) & (cc >= 7) & (cc < 39), 0.5, 0.0)
    rows = []
    for y in range(4):
        rows.append(s1[pl.ds(2 * y, 8, stride=8), :] + s1[pl.ds(2 * y + 1, 8, stride=8), :])
    b2 = jnp.dot(jnp.concatenate(rows, axis=0), r12, precision=HIGHEST, preferred_element_type=F32)
    for y in range(4):
        g2[7 + y, 16:24, :] = b2[8 * y : 8 * y + 8]

    def pack2(src, t):
        acc = jnp.zeros((8, 128), F32)
        for y in range(4):
            acc = jnp.where(lane // 32 == y, roll(src[7 + y, 16:24, :], 32 * y - 7, 1), acc)
        t[...] = acc

    def copies2(t, tr, ss, rs):
        out = []
        for k, d in enumerate(D44):
            out.append(
                (d, pltpu.make_async_remote_copy(t, tr.at[D44.index(neg(d))], ss.at[k], rs.at[k], at(d), MESH))
            )
        return out

    def unpack2(dst, own, tr, which):
        for ny in which:
            if ny == -2:
                ys = [(i, 1 + i) for i in range(3)]
            elif ny == 2:
                ys = [(15 + i, i) for i in range(3)]
            else:
                ys = [(7 + 4 * ny + i, i) for i in range(4)]
            for nx in (-1, 0, 1):
                rows = slice(16 + 8 * nx, 24 + 8 * nx)
                mid = own[...] if (nx, ny) == (0, 0) else tr[D44.index((nx, ny, 0))]
                low, high = tr[D44.index((nx, ny, -1))], tr[D44.index((nx, ny, 1))]
                for e, y in ys:
                    a = roll(low, -25 - 32 * y, 1)
                    b = roll(mid, 7 - 32 * y, 1)
                    c = roll(high, 39 - 32 * y, 1)
                    dst[e, rows, :] = jnp.where(lane < 7, a, jnp.where(lane < 39, b, c))

    ef2 = copies2(ft2, f2_r, s_f2, r_f2)
    ev2 = copies2(vt2, v2_r, s_v2, r_v2)
    pack2(g2, ft2)
    start(ef2)
    arrive([(d, c) for d, c in ef2 if abs(d[1]) < 2])
    unpack2(g2, ft2, f2_r, (-1, 0, 1))
    lev2 = (v2, g2, m2, base2, NGY * 4)
    first(*lev2, 3, 15)
    half(*lev2, 4, 14, 1)
    half(*lev2, 5, 13, 0)
    half(*lev2, 6, 12, 1)
    for y in range(2):
        s2[8 * y : 8 * y + 8, :] = residual(v2, g2, 7 + 2 * y) + residual(v2, g2, 8 + 2 * y)

    r23 = jnp.where(((kk - 7) // 2 == cc % 16) & (kk >= 7) & (kk < 39), 0.5, 0.0)
    a3 = s2[pl.ds(0, 8, stride=2), :] + s2[pl.ds(1, 8, stride=2), :]
    b3 = jnp.dot(a3, r23, precision=HIGHEST, preferred_element_type=F32)
    b3 = jnp.sum(jnp.where(lane // 16 == row, b3, 0.0), axis=0, keepdims=True)
    t3[...] = jnp.where(row == iy, b3, 0.0)

    egy, egz, egx = [], [], []
    for k in range(1, NGY):
        peer = (ix, lax.rem(iy + k, NGY), iz)
        egy.append(pltpu.make_async_remote_copy(t3, gy_r.at[k - 1], s_g.at[k - 1], r_g.at[k - 1], peer, MESH))
    for k in range(1, NGZ):
        peer = (ix, iy, lax.rem(iz + k, NGZ))
        n = 6 + k
        egz.append(pltpu.make_async_remote_copy(gzb.at[iz], gzb.at[iz], s_g.at[n], r_g.at[n], peer, MESH))
    for k in range(1, NGX):
        peer = (lax.rem(ix + k, NGX), iy, iz)
        n = 9 + k
        egx.append(pltpu.make_async_remote_copy(gzb, gxb.at[ix], s_g.at[n], r_g.at[n], peer, MESH))

    for c in egy:
        c.start()
    pack2(v2, vt2)
    pack1(v1, vk1, vz1)
    pack0(vm, vy0, vz0)
    arrive([(d, c) for d, c in ef2 if abs(d[1]) == 2])
    unpack2(g2, ft2, f2_r, (-2, 2))
    for c in egy:
        c.wait_recv()
    line = t3[...]
    for k in range(NGY - 1):
        line = line + gy_r[k]
    gzb[iz] = line
    for c in egz:
        c.start()
    for c in egz:
        c.wait_recv()
    for c in egx:
        c.start()
    start(ev2)
    start(ev1)
    start(ev0)
    gxb[ix] = gzb[...]
    for c in egx:
        c.wait_recv()

    for gx in range(NGX):
        for xl in range(4):
            acc = jnp.zeros((8, 128), F32)
            for gz in range(NGZ):
                acc = jnp.where((lane % 64) // 16 == gz, roll(gxb[gx, gz], (gz - xl) * 16, 1), acc)
            g3[4 * gx + xl] = acc

    zl = lane % 64
    w_lo = jnp.where(zl == 0, 0.0, BETA1)
    w_hi = jnp.where(zl == 63, 0.0, BETA1)
    y_edge = jnp.where(((row == 0) & (lane < 64)) | ((row == 7) & (lane >= 64)), 0.0, 1.0)
    par3 = (lane // 64 + lane) & 1
    colours3 = (par3 == 0, par3 == 1)

    def sum3(x):
        c = v3[x + 4]
        a = roll(c, 64, 1)
        w = jnp.where(lane < 64, roll(a, 1, 0), roll(a, -1, 0)) * y_edge
        s = v3[x + 3] + v3[x + 5] + (a + w)
        return c, s + (roll(c, 1, 1) * w_lo + roll(c, -1, 1) * w_hi)

    def half3(colour):
        def run(j, carry):
            done = []
            for u in range(4):
                x = 4 * j + u
                c, s = sum3(x)
                done.append(jnp.where(colours3[(u + colour) % 2], (g3[x] + s) * INV, c))
            for u in range(4):
                v3[4 * j + u + 4] = done[u]
            return carry

        lax.fori_loop(0, 8, run, 0)

    def first3(j, carry):
        for u in range(2):
            v3[2 * j + u + 4] = jnp.where(colours3[u], g3[2 * j + u] * INV, 0.0)
        return carry

    lax.fori_loop(0, 16, first3, 0)
    half3(1)
    half3(0)
    half3(1)

    def small(g, level):
        n = len(g)
        dz, dy = 2 ** (level - 3), 2 ** (level - 4)
        lo = jnp.where(zl < dz, 0.0, BETA1)
        hi = jnp.where(zl >= 64 - dz, 0.0, BETA1)
        ylo = jnp.where(row < dy, 0.0, 1.0)
        yhi = jnp.where(row >= 8 - dy, 0.0, 1.0)
        par = (row // dy + zl // dz) & 1
        colours = (par == 0, par == 1)

        def total(v, x):
            c = v[x]
            s = roll(c, dz, 1) * lo + roll(c, -dz, 1) * hi
            s = s + (roll(c, dy, 0) * ylo + roll(c, -dy, 0) * yhi)
            if x > 0:
                s = s + v[x - 1]
            if x < n - 1:
                s = s + v[x + 1]
            return s

        def sweep(v, colour):
            return [
                jnp.where(colours[(x + colour) % 2], (g[x] + total(v, x)) * INV, v[x]) for x in range(n)
            ]

        def black_from_red(v):
            return sweep(v, 1)

        v = [jnp.where(colours[x % 2], g[x] * INV, 0.0) for x in range(n)]
        v = sweep(v, 1)
        if level == 6:
            for _ in range(CSWEEPS - 1):
                v = sweep(sweep(v, 0), 1)
            return v
        v = sweep(sweep(v, 0), 1)
        r = [g[x] - ((4.0 + 2.0 * BETA1) * v[x] - total(v, x)) for x in range(n)]
        coarse = []
        for x in range(n // 2):
            t = r[2 * x] + r[2 * x + 1]
            t = t + jnp.where((row // dy) % 2 == 0, roll(t, -dy, 0), roll(t, dy, 0))
            t = t + jnp.where((zl // dz) % 2 == 0, roll(t, -dz, 1), roll(t, dz, 1))
            coarse.append(0.5 * t)
        e = small(coarse, level + 1)
        v = [v[x] + e[x // 2] for x in range(n)]
        for _ in range(2):
            v = sweep(sweep(v, 0), 1)
        return v

    def resid3(x):
        c, s = sum3(x)
        return g3[x] - ((4.0 + 2.0 * BETA1) * c - s)

    g4 = []
    for x in range(16):
        t = resid3(2 * x) + resid3(2 * x + 1)
        t = t + roll(t, 64, 1)
        t = t + jnp.where(lane % 2 == 0, roll(t, -1, 1), roll(t, 1, 1))
        g4.append(0.5 * t)
    e4 = small(g4, 4)
    for x in range(32):
        v3[4 + x] = v3[4 + x] + e4[x // 2]
    for _ in range(2):
        half3(0)
        half3(1)

    k2, c2 = iota((128, 256), 0), iota((128, 256), 1)
    cl = c2 % 128
    zc = iz * 16 + (cl + 1) // 2 - 4
    p32 = jnp.where((zc >= 0) & (zc < 64) & (cl < 46) & (k2 == (c2 // 128) * 64 + zc), 1.0, 0.0)
    e3 = v3[pl.ds(4 * ix, 12)].reshape(96, 128)
    u3 = jnp.dot(e3, p32, precision=HIGHEST, preferred_element_type=F32)
    for yl in range(2):
        tmp2[yl, 16:112, :] = u3[:, 128 * yl : 128 * yl + 128]
    for j in range(10):
        first_row = 16 + iy - 2 + j // 2
        e = tmp2[j % 2, pl.ds(first_row, 12, stride=8), :]
        pe2[j, pl.ds(0, 12, stride=2), :] = e
        pe2[j, pl.ds(1, 12, stride=2), :] = e
    arrive(ev2)
    unpack2(v2, vt2, v2_r, (-2, -1, 0, 1, 2))
    for i in range(18):
        sel = picked(base2, i, NGY * 4)
        v2[i, 8:32, :] = jnp.where(m2[sel] > 0.5, v2[i, 8:32, :] + pe2[(i + 1) // 2], 0.0)
    half(*lev2, 1, 17, 0)
    half(*lev2, 2, 16, 1)
    half(*lev2, 3, 15, 0)
    half(*lev2, 4, 14, 1)

    p21 = jnp.where((cc < 76) & (kk == 4 + cc // 2), 1.0, 0.0)
    u2 = jnp.dot(v2[3:15, 8:32, :].reshape(288, 128), p21, precision=HIGHEST, preferred_element_type=F32)
    tmp1[...] = u2
    for k in range(14):
        e = tmp1[pl.ds(5 + k, 12, stride=24), :]
        pe1[k, pl.ds(0, 12, stride=2), :] = e
        pe1[k, pl.ds(1, 12, stride=2), :] = e
    arrive(ev1)
    unpack1(v1, v1x_r, v1y_r, v1xy_r, v1z_r)
    for i in range(28):
        sel = picked(base1, i, NGX * 16)
        v1[i, 8:32, :] = jnp.where(m1[sel] > 0.5, v1[i, 8:32, :] + pe1[i // 2], 0.0)
    half(*lev1, 1, 27, 0)
    half(*lev1, 2, 26, 1)
    half(*lev1, 3, 25, 0)
    half(*lev1, 4, 24, 1)

    main_lane = 6 + cl // 2
    halo_lane = jnp.where(cl < 64, 70 + cl // 2, 6 + (cl - 128) // 2)
    used = (c2 < 128) | (cl < 4) | (cl >= 124)
    p10 = jnp.where(used & (k2 == jnp.where(c2 < 128, main_lane, halo_lane)), 1.0, 0.0)
    u1 = jnp.dot(v1[4:24, 14:30, :].reshape(320, 128), p10, precision=HIGHEST, preferred_element_type=F32)
    tmp0[...] = u1
    for k in range(20):
        for ref, cols in ((pe0m, slice(0, 128)), (pe0h, slice(128, 256))):
            e = tmp0[16 * k : 16 * k + 12, cols]
            ref[k, pl.ds(0, 12, stride=2), :] = e
            ref[k, pl.ds(1, 12, stride=2), :] = e
    arrive(ev0)
    sent(ev0)
    unpack0(vm, vh, vx_r, vy_r, vxy_r, vz_r)

    def add0(x):
        for u in range(2):
            i = x + u
            k = x // 2
            sel = picked(base0, i, NGX * BX)
            vm[i, 4:28, :] = jnp.where(mm[sel] > 0.5, vm[i, 4:28, :] + pe0m[k], 0.0)
            vh[i, 4:28, :] = jnp.where(mh[sel] > 0.5, vh[i, 4:28, :] + pe0h[k], 0.0)

    planes0(0, 40, add0)
    half0(1, 39, 0)
    half0(2, 38, 1)
    half0(3, 37, 0)
    half0(4, 36, 1, last=True)

    store = pltpu.make_async_copy(vm.at[pl.ds(4, BX), pl.ds(8, BY), :], out_hbm, io_sem.at[1])
    store.start()
    for e in (ef0, ef1, ef2, ev2, ev1):
        sent(e)
    for c in egy + egz + egx:
        c.wait_send()
    store.wait()


def on_device(density):
    def vmem(*shape):
        return pltpu.VMEM(shape, F32)

    level0 = [vmem(40, 32, 128)] * 4 + [vmem(4, 24, 128)] * 2
    level0 += [vmem(16, 16, 128), vmem(20, 24, 128), vmem(20, 24, 128), vmem(320, 256)]
    level1 = [vmem(28, 40, 128)] * 2 + [vmem(4, 24, 128), vmem(64, 128), vmem(14, 24, 128), vmem(288, 128)]
    level2 = [vmem(18, 40, 128)] * 2 + [vmem(4, 24, 128), vmem(16, 128), vmem(10, 24, 128), vmem(2, 128, 128)]
    packs = [vmem(2, 16, 8, 128), vmem(2, 16, 128)] * 2 + [vmem(8, 8, 128), vmem(2, 8, 128)] * 2
    packs += [vmem(8, 128)] * 2
    recv0 = [vmem(2, 4, 16, 128), vmem(2, 16, 8, 128), vmem(4, 2, 8, 128), vmem(18, 16, 128)] * 2
    recv1 = [vmem(2, 3, 8, 128), vmem(2, 8, 8, 128), vmem(4, 3, 8, 128), vmem(18, 8, 128)] * 2
    recv2 = [vmem(44, 8, 128)] * 2
    gather = [vmem(8, 128), vmem(7, 8, 128), vmem(4, 8, 128), vmem(8, 4, 8, 128), vmem(32, 8, 128), vmem(40, 8, 128)]
    dma = pltpu.SemaphoreType.DMA
    sems = [dma((2,))] + [dma((26,))] * 8 + [dma((44,))] * 4 + [dma((17,))] * 2
    return pl.pallas_call(
        kernel,
        out_shape=jax.ShapeDtypeStruct((BX, BY, BZ), F32),
        in_specs=[pl.BlockSpec(memory_space=pl.ANY)],
        out_specs=pl.BlockSpec(memory_space=pl.ANY),
        scratch_shapes=level0 + level1 + level2 + packs + recv0 + recv1 + recv2 + gather + sems,
        compiler_params=pltpu.CompilerParams(
            collective_id=0, has_side_effects=True, vmem_limit_bytes=48 * 1024 * 1024
        ),
    )(density)


def solution(mesh):
    spec = P("gx", "gy", "gz")
    return jax.shard_map(on_device, mesh=mesh, in_specs=(spec,), out_specs=spec, check_vma=False)
```

```python
import itertools

import jax
import jax.numpy as jnp
from jax import lax
from jax.experimental import pallas as pl
from jax.experimental.pallas import tpu as pltpu
from jax.sharding import PartitionSpec as P

MESH = pl.DeviceIdType.MESH
F32 = jnp.float32
BF16 = jnp.bfloat16

NGX, NGY, NGZ = 8, 8, 4
BX, BY, BZ = 32, 16, 128
CSWEEPS = 4
BETA1 = 1.5
CENTRE = 4.0 + 2.0 * BETA1
INV = 1.0 / CENTRE

D26 = [d for d in itertools.product((-1, 0, 1), repeat=3) if d != (0, 0, 0)]
D44 = [d for d in itertools.product((-1, 0, 1), (-2, -1, 0, 1, 2), (-1, 0, 1)) if d != (0, 0, 0)]
XY4 = [(-1, -1), (-1, 1), (1, -1), (1, 1)]
Z18 = [d for d in D26 if d[2] != 0]


def roll(x, shift, axis):
    size = x.shape[axis]
    shift = shift % size
    return x if shift == 0 else pltpu.roll(x, shift, axis)


def iota(shape, dim):
    return lax.broadcasted_iota(jnp.int32, shape, dim)


def side(n):
    return 0 if n < 0 else 1


def neg(n):
    return (-n[0], -n[1], -n[2])


def moved(x, matrix):
    hi = x.astype(BF16)
    rest = x - hi.astype(F32)
    mid = rest.astype(BF16)
    lo = (rest - mid.astype(F32)).astype(BF16)
    return (
        jnp.dot(lo, matrix, preferred_element_type=F32)
        + jnp.dot(mid, matrix, preferred_element_type=F32)
        + jnp.dot(hi, matrix, preferred_element_type=F32)
    )


def kernel(
    f_hbm, out_hbm,
    f0, p0, fr0, fb0, vr0, vb0, k0, s0, pe0, out,
    fr1, fb1, vr1, vb1, k1, s1, pe1, tmp1,
    fr2, fb2, vr2, vb2, k2, s2, pe2, tmp2,
    fy0, fz0, vy0, vz0, fk1, fz1, vk1, vz1, ft2, vt2,
    fx_r, fy_r, fxy_r, fz_r, vx_r, vy_r, vxy_r, vz_r,
    f1x_r, f1y_r, f1xy_r, f1z_r, v1x_r, v1y_r, v1xy_r, v1z_r,
    f2_r, v2_r,
    t3, gy_r, gzb, gxb, g3, v3,
    io_sem, s_f0, r_f0, s_v0, r_v0, s_f1, r_f1, s_v1, r_v1, s_f2, r_f2, s_v2, r_v2, s_g, r_g,
):
    ix, iy, iz = lax.axis_index("gx"), lax.axis_index("gy"), lax.axis_index("gz")

    def there(n):
        nx, ny, nz = ix + n[0], iy + n[1], iz + n[2]
        return (nx >= 0) & (nx < NGX) & (ny >= 0) & (ny < NGY) & (nz >= 0) & (nz < NGZ)

    def at(n):
        return (
            jnp.clip(ix + n[0], 0, NGX - 1),
            jnp.clip(iy + n[1], 0, NGY - 1),
            jnp.clip(iz + n[2], 0, NGZ - 1),
        )

    load = pltpu.make_async_copy(f_hbm, f0, io_sem.at[0])
    load.start()

    barrier = pltpu.get_barrier_semaphore()
    count = 0
    for d in D44:
        ok = there(d)
        count = count + ok.astype(jnp.int32)

        @pl.when(ok)
        def _(d=d):
            pl.semaphore_signal(barrier, inc=1, device_id=at(d), device_id_type=MESH)

    lines = []
    for k in range(1, NGY):
        lines.append((ix, lax.rem(iy + k, NGY), iz))
    for k in range(1, NGZ):
        lines.append((ix, iy, lax.rem(iz + k, NGZ)))
    for k in range(1, NGX):
        lines.append((lax.rem(ix + k, NGX), iy, iz))
    for peer in lines:
        pl.semaphore_signal(barrier, inc=1, device_id=peer, device_id_type=MESH)

    lane = iota((8, 128), 1)
    row = iota((8, 128), 0)
    lane16 = iota((16, 128), 1)
    r32, l32 = iota((32, 128), 0), iota((32, 128), 1)
    signed = jnp.where(l32 < 96, l32, l32 - 128)

    def fill(ref, halo, pairs, start_pairs, total_pairs, rows_at, total_rows):
        zp = start_pairs + signed
        ok = (signed >= -halo) & (signed < pairs + halo) & (zp >= 0) & (zp < total_pairs)
        ok = ok & (rows_at >= 0) & (rows_at < total_rows)
        ref[0] = jnp.zeros((32, 128), F32)
        ref[1] = jnp.where(ok, INV, 0.0)

    fill(k0, 2, 64, iz * 64, NGZ * 64, iy * BY + r32 - 8, NGY * BY)
    fill(k1, 3, 32, iz * 32, NGZ * 32, iy * 8 + r32 - 16, NGY * 8)
    fill(k2, 4, 16, iz * 16, NGZ * 16, ix * 8 + r32 - 16, NGX * 8)

    class Level:
        def __init__(self, fr, fb, vr, vb, k, first, main, rows, window, odd, start, total):
            self.fr, self.fb, self.vr, self.vb, self.k = fr, fb, vr, vb, k
            self.first, self.main, self.rows, self.window = first, main, rows, window
            self.odd, self.start, self.total = odd, start, total
            self.planes = main + 2 * first

        def coefficient(self, i, lo, hi):
            if self.first <= i < self.first + self.main:
                return self.k[1, lo:hi, :]
            pos = self.start + i
            return self.k[jnp.where((pos >= 0) & (pos < self.total), 1, 0), lo:hi, :]

        def even(self, i, lo, hi):
            return (iota((hi - lo, 128), 0) + (lo + i + self.odd)) % 2 == 0

    lev0 = Level(fr0, fb0, vr0, vb0, k0, 4, BX, (8, 24), (4, 28), 0, ix * BX - 4, NGX * BX)
    lev1 = Level(fr1, fb1, vr1, vb1, k1, 6, 16, (16, 24), (8, 32), 0, ix * 16 - 6, NGX * 16)
    lev2 = Level(fr2, fb2, vr2, vb2, k2, 7, 4, (16, 24), (8, 32), 1, iy * 4 - 7, NGY * 4)

    def around(level, src, i, lo, hi, red):
        c = src[i, lo:hi, :]
        up, down = roll(c, 1, 1), roll(c, -1, 1)
        even = level.even(i, lo, hi)
        z = jnp.where(even, up, down) if red else jnp.where(even, down, up)
        s = (src[i - 1, lo:hi, :] + src[i + 1, lo:hi, :]) + (
            src[i, lo - 1 : hi - 1, :] + src[i, lo + 1 : hi + 1, :]
        )
        return s + BETA1 * (c + z)

    def half(level, lo, hi, red, rows=None):
        dst, src = (level.vr, level.vb) if red else (level.vb, level.vr)
        source = level.fr if red else level.fb
        a, b = rows or level.window
        for i in range(lo, hi):
            s = source[i, a:b, :] + around(level, src, i, a, b, red)
            dst[i, a:b, :] = s * level.coefficient(i, a, b)

    def first_half(level, lo, hi):
        a, b = level.window
        for i in range(lo, hi):
            level.vr[i, a:b, :] = level.fr[i, a:b, :] * level.coefficient(i, a, b)

    def smooth_down(level):
        n, m = level.first, level.first + level.main
        first_half(level, n - 4, m + 4)
        half(level, n - 3, m + 3, False)
        half(level, n - 2, m + 2, True)
        half(level, n - 1, m + 1, False)

    def residual(level, i):
        a, b = level.rows
        vr, vb = level.vr[i, a:b, :], level.vb[i, a:b, :]
        red = level.fr[i, a:b, :] - (CENTRE * vr - around(level, level.vb, i, a, b, True))
        black = level.fb[i, a:b, :] - (CENTRE * vb - around(level, level.vr, i, a, b, False))
        return red + black

    def zero(ref):
        @pl.loop(0, ref.shape[0])
        def _(i):
            ref[i] = jnp.zeros(ref.shape[1:], F32)

    for ref in (vr0, vb0, vr1, vb1, vr2, vb2, pe0, pe1, pe2, v3, tmp2):
        zero(ref)

    def splitter(total, where):
        k, c = iota((256, total), 0), iota((256, total), 1)
        z = k % 128
        return z, (z + k // 128) % 2 == 0, c, where

    def split_rows(a, even):
        return jnp.concatenate([jnp.where(even, a, 0.0), jnp.where(even, 0.0, a)], axis=1)

    k256, c128 = iota((256, 128), 0), iota((256, 128), 1)
    z256 = k256 % 128
    red256 = (z256 + k256 // 128) % 2 == 0

    load.wait()

    to_pairs = jnp.where(c128 == z256 // 2 + jnp.where(red256, 0, 64), 1.0, 0.0).astype(BF16)
    for part in range(4):
        rows = []
        for x in range(8 * part, 8 * part + 8):
            rows.append(split_rows(f0[x], (iota((16, 128), 0) + x) % 2 == 0))
        p = moved(jnp.concatenate(rows, axis=0), to_pairs)
        for x in range(8):
            p0[8 * part + x] = p[16 * x : 16 * x + 16]

    def pack0(plane, yp, zp):
        lo = jnp.zeros((16, 128), F32)
        hi = jnp.zeros((16, 128), F32)
        slot = (lane16 % 64) // 2
        for x in range(BX):
            p = plane(x)
            half_tile = slice(4 * (x % 2), 4 * (x % 2) + 4)
            yp[0, x // 2, half_tile, :] = p[0:4]
            yp[1, x // 2, half_tile, :] = p[12:16]
            t = roll(p, 2 * x, 1)
            lo = jnp.where(slot == x, t, lo)
            hi = jnp.where(slot == (x - 1) % BX, roll(p, 64, 1) if x == 0 else t, hi)
        zp[0] = lo
        zp[1] = hi

    def copies0(xs, yp, zp, xr, yr, xyr, zr, ss, rs):
        out = []
        for k, d in enumerate(D26):
            dx, dy, dz = d
            if dz == 0 and dy == 0:
                s, t = xs(dx), xr.at[side(-dx)]
            elif dz == 0 and dx == 0:
                s, t = yp.at[side(dy)], yr.at[side(-dy)]
            elif dz == 0:
                s = yp.at[side(dy), pl.ds(0 if dx < 0 else 14, 2)]
                t = xyr.at[XY4.index((-dx, -dy))]
            else:
                slot = Z18.index(neg(d))
                if dy == 0:
                    s, t = zp.at[side(dz)], zr.at[slot]
                else:
                    rows = pl.ds(0 if dy < 0 else 8, 8)
                    s, t = zp.at[side(dz), rows], zr.at[slot, rows]
            out.append((d, pltpu.make_async_remote_copy(s, t, ss.at[k], rs.at[k], at(d), MESH)))
        return out

    def start(copies):
        for d, c in copies:
            @pl.when(there(d))
            def _(c=c):
                c.start()

    def arrive(copies):
        for d, c in copies:
            @pl.when(there(neg(d)))
            def _(c=c):
                c.wait_recv()

    def sent(copies):
        for d, c in copies:
            @pl.when(there(d))
            def _(c=c):
                c.wait_send()

    def unpack0(own, xr, yr, xyr, zr, put, colours):
        for nx in (-1, 0, 1):
            for ny, src, dst, num in ((-1, 8, 0, 8), (0, 0, 8, 16), (1, 0, 24, 8)):
                low = zr[Z18.index((nx, ny, -1)), src : src + num, :]
                high = zr[Z18.index((nx, ny, 1)), src : src + num, :]
                lanes = iota((num, 128), 1)
                mixed = [jnp.where(lanes < 64, high, low), jnp.where(lanes < 64, low, high)]
                xs = range(28, 32) if nx < 0 else (range(32) if nx == 0 else range(4))
                for x in xs:
                    if ny == 0:
                        p = own(x) if nx == 0 else xr[side(nx), x % 4]
                    else:
                        if nx == 0:
                            p = yr[side(ny), x // 2]
                        else:
                            p = xyr[XY4.index((nx, ny)), (x % 4) // 2]
                        if (x % 2 == 0) == (ny < 0):
                            p = roll(p, 4, 0)
                    for colour in range(colours):
                        if x == 0:
                            a = roll(high, 64 if colour == 0 else 0, 1)
                            b = roll(low, 0 if colour == 0 else 64, 1)
                            e = jnp.where(lanes < 96, a, b)
                        else:
                            e = roll(mixed[colour], (64 if colour == 0 else 0) - 2 * x, 1)
                        q = p if colour == 0 else roll(p, 64, 1)
                        i = 32 * nx + x + 4
                        put(colour, i, dst, num, jnp.where(lanes < 64, q, e))

    def clean(level):
        def put(colour, i, dst, num, value):
            ok = level.coefficient(i, dst, dst + num) > 0.0
            (level.fr if colour == 0 else level.fb)[i, dst : dst + num, :] = jnp.where(ok, value, 0.0)

        return put

    def corrected(level, add):
        def put(colour, i, dst, num, value):
            ok = level.coefficient(i, dst, dst + num) > 0.0
            level.vb[i, dst : dst + num, :] = jnp.where(ok, value + add(i, dst, num), 0.0)

        return put

    ef0 = copies0(
        lambda dx: p0.at[pl.ds(0 if dx < 0 else 28, 4)], fy0, fz0, fx_r, fy_r, fxy_r, fz_r, s_f0, r_f0
    )
    ev0 = copies0(
        lambda dx: vb0.at[pl.ds(4 if dx < 0 else 32, 4), pl.ds(8, BY), :],
        vy0, vz0, vx_r, vy_r, vxy_r, vz_r, s_v0, r_v0,
    )

    pack0(lambda x: p0[x], fy0, fz0)
    pl.semaphore_wait(barrier, count + len(lines))
    start(ef0)

    split1 = iota((256, 256), 1)
    k1i = iota((256, 256), 0)
    z1i = k1i % 128
    red1 = (z1i + k1i // 128) % 2 == 0
    packed = (split1 < 128) & (split1 % 64 == z1i // 2 + jnp.where(red1, 0, 32))
    apart = (split1 >= 128) & (split1 - 128 == z1i // 2 + jnp.where(red1, 0, 64))
    to_pairs1 = jnp.where((z1i < 64) & (packed | apart), 0.5, 0.0).astype(BF16)
    to_pairs2 = jnp.where(
        (z256 < 32) & (c128 % 32 == z256 // 2 + jnp.where(red256, 0, 16)), 0.5, 0.0
    ).astype(BF16)
    csign = jnp.where(c128 < 96, c128, c128 - 128)
    wanted = ((csign + 128) // 2 - 64) % 128 + 128 * ((csign + 128) % 2)
    from_pairs = jnp.where((k256 == wanted) & (csign >= -4) & (csign < 68), 1.0, 0.0).astype(BF16)
    to_cells = jnp.where(k256 == c128 // 2 + 128 * (c128 % 2), 1.0, 0.0).astype(BF16)

    arrive(ef0)
    unpack0(lambda x: p0[x], fx_r, fy_r, fxy_r, fz_r, clean(lev0), 2)
    smooth_down(lev0)
    for x in range(16):
        s0[x] = residual(lev0, 4 + 2 * x) + residual(lev0, 5 + 2 * x)

    rows = []
    for x in range(16):
        a = s0[x, pl.ds(0, 8, stride=2), :] + s0[x, pl.ds(1, 8, stride=2), :]
        rows.append(split_rows(a, (row + x) % 2 == 0))
    b1 = moved(jnp.concatenate(rows, axis=0), to_pairs1)

    def zpack1(plane, zp):
        lo = jnp.zeros((8, 128), F32)
        hi = jnp.zeros((8, 128), F32)
        for x in range(16):
            p = plane(x)
            here = (lane % 64) // 3 == x
            lo = jnp.where(here, roll(p, 3 * x, 1), lo)
            hi = jnp.where(here, roll(p, 3 * x - 29, 1), hi)
        zp[0] = lo
        zp[1] = hi

    def copies1(pk, zp, xr, yr, xyr, zr, ss, rs):
        out = []
        for k, d in enumerate(D26):
            dx, dy, dz = d
            if dz == 0 and dx == 0:
                s, t = pk, yr.at[side(-dy)]
            elif dz == 0:
                s = pk.at[pl.ds(0 if dx < 0 else 5, 3)]
                t = xr.at[side(-dx)] if dy == 0 else xyr.at[XY4.index((-dx, -dy))]
            else:
                s, t = zp.at[side(dz)], zr.at[Z18.index(neg(d))]
            out.append((d, pltpu.make_async_remote_copy(s, t, ss.at[k], rs.at[k], at(d), MESH)))
        return out

    def unpack1(pk, xr, yr, xyr, zr, put, colours):
        for xe in range(28):
            nx, x = (-1, 10 + xe) if xe < 6 else ((0, xe - 6) if xe < 22 else (1, xe - 22))
            for ny in (-1, 0, 1):
                if nx == 0:
                    mid = pk[x // 2] if ny == 0 else yr[side(ny), x // 2]
                else:
                    tile = x // 2 - 5 if nx < 0 else x // 2
                    mid = xr[side(nx), tile] if ny == 0 else xyr[XY4.index((nx, ny)), tile]
                low, high = zr[Z18.index((nx, ny, -1))], zr[Z18.index((nx, ny, 1))]
                for colour in range(colours):
                    a = roll(mid, -64 * (x % 2) - 32 * colour, 1)
                    b = roll(high, 32 - 3 * x - 64 * colour, 1)
                    c = roll(low, 125 - 3 * x - 64 * colour, 1)
                    put(colour, xe, 16 + 8 * ny, 8, jnp.where(lane < 32, a, jnp.where(lane < 64, b, c)))

    ef1 = copies1(fk1, fz1, f1x_r, f1y_r, f1xy_r, f1z_r, s_f1, r_f1)
    ev1 = copies1(vk1, vz1, v1x_r, v1y_r, v1xy_r, v1z_r, s_v1, r_v1)
    for t in range(8):
        fk1[t] = jnp.where(lane < 64, b1[16 * t : 16 * t + 8, 0:128], b1[16 * t + 8 : 16 * t + 16, 0:128])
    zpack1(lambda x: b1[8 * x : 8 * x + 8, 128:256], fz1)
    start(ef1)
    arrive(ef1)
    unpack1(fk1, f1x_r, f1y_r, f1xy_r, f1z_r, clean(lev1), 2)
    smooth_down(lev1)
    for x in range(8):
        s1[8 * x : 8 * x + 8, :] = residual(lev1, 6 + 2 * x) + residual(lev1, 7 + 2 * x)

    rows = []
    for y in range(4):
        a = s1[pl.ds(2 * y, 8, stride=8), :] + s1[pl.ds(2 * y + 1, 8, stride=8), :]
        rows.append(split_rows(a, (row + y) % 2 == 0))
    b2 = moved(jnp.concatenate(rows, axis=0), to_pairs2)

    def copies2(t, tr, ss, rs):
        out = []
        for k, d in enumerate(D44):
            dst = tr.at[D44.index(neg(d))]
            out.append((d, pltpu.make_async_remote_copy(t, dst, ss.at[k], rs.at[k], at(d), MESH)))
        return out

    def unpack2(own, tr, which, put, colours):
        part = lane % 32
        for ny in which:
            if ny == -2:
                ys = [(i, 1 + i) for i in range(3)]
            elif ny == 2:
                ys = [(15 + i, i) for i in range(3)]
            else:
                ys = [(7 + 4 * ny + i, i) for i in range(4)]
            for nx in (-1, 0, 1):
                mid = own[...] if (nx, ny) == (0, 0) else tr[D44.index((nx, ny, 0))]
                low, high = tr[D44.index((nx, ny, -1))], tr[D44.index((nx, ny, 1))]
                for colour in range(colours):
                    a = roll(mid, -16 * colour, 1)
                    b = roll(high, 16 - 16 * colour, 1)
                    c = roll(low, 112 - 16 * colour, 1)
                    mixed = jnp.where(part < 16, a, jnp.where(part < 24, b, c))
                    for e, y in ys:
                        put(colour, e, 16 + 8 * nx, 8, roll(mixed, -32 * y, 1))

    ef2 = copies2(ft2, f2_r, s_f2, r_f2)
    ev2 = copies2(vt2, v2_r, s_v2, r_v2)
    acc = b2[0:8]
    for y in range(1, 4):
        acc = jnp.where(lane // 32 == y, b2[8 * y : 8 * y + 8], acc)
    ft2[...] = acc
    start(ef2)
    arrive([(d, c) for d, c in ef2 if abs(d[1]) < 2])
    unpack2(ft2, f2_r, (-1, 0, 1), clean(lev2), 2)
    smooth_down(lev2)

    for y in range(2):
        s2[8 * y : 8 * y + 8, :] = residual(lev2, 7 + 2 * y) + residual(lev2, 8 + 2 * y)
    a3 = s2[pl.ds(0, 8, stride=2), :] + s2[pl.ds(1, 8, stride=2), :]
    a3 = jnp.where(lane < 16, 0.5 * a3, 0.0)
    a3 = pltpu.roll(a3, 0, 1, stride=16, stride_axis=0)
    a3 = jnp.sum(a3, axis=0, keepdims=True)
    t3[...] = jnp.where(row == iy, a3, 0.0)

    egy, egz, egx = [], [], []
    for k in range(1, NGY):
        peer = (ix, lax.rem(iy + k, NGY), iz)
        egy.append(pltpu.make_async_remote_copy(t3, gy_r.at[k - 1], s_g.at[k - 1], r_g.at[k - 1], peer, MESH))
    for k in range(1, NGZ):
        peer = (ix, iy, lax.rem(iz + k, NGZ))
        n = 6 + k
        egz.append(pltpu.make_async_remote_copy(gzb.at[iz], gzb.at[iz], s_g.at[n], r_g.at[n], peer, MESH))
    for k in range(1, NGX):
        peer = (lax.rem(ix + k, NGX), iy, iz)
        n = 9 + k
        egx.append(pltpu.make_async_remote_copy(gzb, gxb.at[ix], s_g.at[n], r_g.at[n], peer, MESH))

    for c in egy:
        c.start()
    acc = jnp.zeros((8, 128), F32)
    for y in range(4):
        acc = jnp.where(lane // 32 == y, roll(vb2[7 + y, 16:24, :], 32 * y, 1), acc)
    vt2[...] = acc
    for t in range(8):
        vk1[t] = jnp.where(lane < 64, vb1[6 + 2 * t, 16:24, :], roll(vb1[7 + 2 * t, 16:24, :], 64, 1))
    zpack1(lambda x: vb1[6 + x, 16:24, :], vz1)
    pack0(lambda x: vb0[4 + x, 8:24, :], vy0, vz0)
    arrive([(d, c) for d, c in ef2 if abs(d[1]) == 2])
    unpack2(ft2, f2_r, (-2, 2), clean(lev2), 2)
    for c in egy:
        c.wait_recv()
    line = t3[...]
    for k in range(NGY - 1):
        line = line + gy_r[k]
    gzb[iz] = line
    for c in egz:
        c.start()
    for c in egz:
        c.wait_recv()
    for c in egx:
        c.start()
    start(ev2)
    start(ev1)
    start(ev0)
    gxb[ix] = gzb[...]
    for c in egx:
        c.wait_recv()

    for gx in range(NGX):
        for xl in range(4):
            acc = jnp.zeros((8, 128), F32)
            for gz in range(NGZ):
                acc = jnp.where((lane % 64) // 16 == gz, roll(gxb[gx, gz], (gz - xl) * 16, 1), acc)
            g3[4 * gx + xl] = acc

    zl = lane % 64
    w_lo = jnp.where(zl == 0, 0.0, BETA1)
    w_hi = jnp.where(zl == 63, 0.0, BETA1)
    y_edge = jnp.where(((row == 0) & (lane < 64)) | ((row == 7) & (lane >= 64)), 0.0, 1.0)
    par3 = (lane // 64 + lane) & 1
    colours3 = (par3 == 0, par3 == 1)

    def sum3(x):
        c = v3[x + 4]
        a = roll(c, 64, 1)
        w = jnp.where(lane < 64, roll(a, 1, 0), roll(a, -1, 0)) * y_edge
        s = (v3[x + 3] + v3[x + 5]) + (a + w)
        return c, s + (roll(c, 1, 1) * w_lo + roll(c, -1, 1) * w_hi)

    def half3(colour):
        for j in range(4):
            done = []
            for x in range(8 * j, 8 * j + 8):
                c, s = sum3(x)
                done.append(jnp.where(colours3[(x + colour) % 2], (g3[x] + s) * INV, c))
            for u in range(8):
                v3[8 * j + u + 4] = done[u]

    for x in range(32):
        v3[x + 4] = jnp.where(colours3[x % 2], g3[x] * INV, 0.0)
    half3(1)
    half3(0)
    half3(1)

    def small(g, level):
        n = len(g)
        dz, dy = 2 ** (level - 3), 2 ** (level - 4)
        lo = jnp.where(zl < dz, 0.0, BETA1)
        hi = jnp.where(zl >= 64 - dz, 0.0, BETA1)
        ylo = jnp.where(row < dy, 0.0, 1.0)
        yhi = jnp.where(row >= 8 - dy, 0.0, 1.0)
        par = (row // dy + zl // dz) & 1
        colours = (par == 0, par == 1)

        def total(v, x):
            c = v[x]
            s = roll(c, dz, 1) * lo + roll(c, -dz, 1) * hi
            s = s + (roll(c, dy, 0) * ylo + roll(c, -dy, 0) * yhi)
            if x > 0:
                s = s + v[x - 1]
            if x < n - 1:
                s = s + v[x + 1]
            return s

        def sweep(v, colour):
            return [
                jnp.where(colours[(x + colour) % 2], (g[x] + total(v, x)) * INV, v[x]) for x in range(n)
            ]

        v = [jnp.where(colours[x % 2], g[x] * INV, 0.0) for x in range(n)]
        v = sweep(v, 1)
        if level == 6:
            for _ in range(CSWEEPS - 1):
                v = sweep(sweep(v, 0), 1)
            return v
        v = sweep(sweep(v, 0), 1)
        r = [g[x] - (CENTRE * v[x] - total(v, x)) for x in range(n)]
        coarse = []
        for x in range(n // 2):
            t = r[2 * x] + r[2 * x + 1]
            t = t + jnp.where((row // dy) % 2 == 0, roll(t, -dy, 0), roll(t, dy, 0))
            t = t + jnp.where((zl // dz) % 2 == 0, roll(t, -dz, 1), roll(t, dz, 1))
            coarse.append(0.5 * t)
        e = small(coarse, level + 1)
        v = [v[x] + e[x // 2] for x in range(n)]
        for _ in range(2):
            v = sweep(sweep(v, 0), 1)
        return v

    def resid3(x):
        c, s = sum3(x)
        return g3[x] - (CENTRE * c - s)

    g4 = []
    for x in range(16):
        t = resid3(2 * x) + resid3(2 * x + 1)
        t = t + roll(t, 64, 1)
        t = t + jnp.where(lane % 2 == 0, roll(t, -1, 1), roll(t, 1, 1))
        g4.append(0.5 * t)
    e4 = small(g4, 4)
    for x in range(32):
        v3[4 + x] = v3[4 + x] + e4[x // 2]
    for _ in range(2):
        half3(0)
        half3(1)

    for x in range(12):
        e = v3[4 * ix + x]
        for yl in range(2):
            tmp2[yl, 16 + 8 * x : 24 + 8 * x, :] = pltpu.roll(e, (128 - 16 * iz + 64 * yl) % 128, 1)
    for j in range(10):
        e = tmp2[j % 2, pl.ds(16 + iy - 2 + j // 2, 12, stride=8), :]
        pe2[j, pl.ds(8, 12, stride=2), :] = e
        pe2[j, pl.ds(9, 12, stride=2), :] = e
    arrive(ev2)
    sent(ev2)
    add2 = corrected(lev2, lambda i, dst, num: pe2[(i + 1) // 2, dst : dst + num, :])
    unpack2(vt2, v2_r, (-2, -1, 0, 1, 2), add2, 1)
    half(lev2, 1, 17, True)
    half(lev2, 2, 16, False)
    half(lev2, 3, 15, True)
    half(lev2, 4, 14, False)

    def cells(level, i, a, b):
        even = level.even(i, a, b)
        r, k = level.vr[i, a:b, :], level.vb[i, a:b, :]
        return jnp.concatenate([jnp.where(even, r, k), jnp.where(even, k, r)], axis=1)

    rows = [cells(lev2, i, 8, 32) for i in range(3, 15)]
    tmp1[...] = moved(jnp.concatenate(rows, axis=0), from_pairs)
    for k in range(14):
        e = tmp1[pl.ds(5 + k, 12, stride=24), :]
        pe1[k, pl.ds(8, 12, stride=2), :] = e
        pe1[k, pl.ds(9, 12, stride=2), :] = e
    arrive(ev1)
    sent(ev1)
    add1 = corrected(lev1, lambda i, dst, num: pe1[i // 2, dst : dst + num, :])
    unpack1(vk1, v1x_r, v1y_r, v1xy_r, v1z_r, add1, 1)
    half(lev1, 1, 27, True)
    half(lev1, 2, 26, False)
    half(lev1, 3, 25, True)
    half(lev1, 4, 24, False)

    rows = [cells(lev1, i, 14, 30) for i in range(4, 24)]
    u1 = moved(jnp.concatenate(rows, axis=0), from_pairs)
    for k in range(20):
        e = u1[16 * k : 16 * k + 12]
        pe0[k, pl.ds(4, 12, stride=2), :] = e
        pe0[k, pl.ds(5, 12, stride=2), :] = e
    arrive(ev0)
    sent(ev0)
    add0 = corrected(lev0, lambda i, dst, num: pe0[i // 2, dst : dst + num, :])
    unpack0(lambda x: vb0[4 + x, 8:24, :], vx_r, vy_r, vxy_r, vz_r, add0, 1)
    half(lev0, 1, 39, True)
    half(lev0, 2, 38, False)
    half(lev0, 3, 37, True)
    half(lev0, 4, 36, False, (8, 24))

    stores = []
    for part in range(4):
        rows = [cells(lev0, 4 + x, 8, 24) for x in range(8 * part, 8 * part + 8)]
        out[pl.ds(8 * part, 8)] = moved(jnp.concatenate(rows, axis=0), to_cells).reshape(8, 16, 128)
        here = pl.ds(8 * part, 8)
        stores.append(pltpu.make_async_copy(out.at[here], out_hbm.at[here], io_sem.at[1 + part]))
        stores[-1].start()
    for e in (ef0, ef1, ef2):
        sent(e)
    for c in egy + egz + egx:
        c.wait_send()
    for s in stores:
        s.wait()


def on_device(density):
    def vmem(*shape):
        return pltpu.VMEM(shape, F32)

    coef = vmem(2, 32, 128)
    level0 = [vmem(BX, BY, BZ)] * 2 + [vmem(40, 32, 128)] * 4 + [coef, vmem(16, 16, 128), vmem(20, 32, 128)]
    level0 += [vmem(BX, BY, BZ)]
    level1 = [vmem(28, 40, 128)] * 4 + [coef, vmem(64, 128), vmem(14, 32, 128), vmem(288, 128)]
    level2 = [vmem(18, 40, 128)] * 4 + [coef, vmem(16, 128), vmem(10, 32, 128), vmem(2, 128, 128)]
    packs = [vmem(2, 16, 8, 128), vmem(2, 16, 128)] * 2 + [vmem(8, 8, 128), vmem(2, 8, 128)] * 2
    packs += [vmem(8, 128)] * 2
    recv0 = [vmem(2, 4, 16, 128), vmem(2, 16, 8, 128), vmem(4, 2, 8, 128), vmem(18, 16, 128)] * 2
    recv1 = [vmem(2, 3, 8, 128), vmem(2, 8, 8, 128), vmem(4, 3, 8, 128), vmem(18, 8, 128)] * 2
    recv2 = [vmem(44, 8, 128)] * 2
    gather = [vmem(8, 128), vmem(7, 8, 128), vmem(4, 8, 128), vmem(8, 4, 8, 128), vmem(32, 8, 128), vmem(40, 8, 128)]
    dma = pltpu.SemaphoreType.DMA
    sems = [dma((5,))] + [dma((26,))] * 8 + [dma((44,))] * 4 + [dma((17,))] * 2
    return pl.pallas_call(
        kernel,
        out_shape=jax.ShapeDtypeStruct((BX, BY, BZ), F32),
        in_specs=[pl.BlockSpec(memory_space=pl.ANY)],
        out_specs=pl.BlockSpec(memory_space=pl.ANY),
        scratch_shapes=level0 + level1 + level2 + packs + recv0 + recv1 + recv2 + gather + sems,
        compiler_params=pltpu.CompilerParams(
            collective_id=0, has_side_effects=True, vmem_limit_bytes=48 * 1024 * 1024
        ),
    )(density)


def solution(mesh):
    spec = P("gx", "gy", "gz")
    return jax.shard_map(on_device, mesh=mesh, in_specs=(spec,), out_specs=spec, check_vma=False)
```

```python
import itertools

import jax
import jax.numpy as jnp
from jax import lax
from jax.experimental import pallas as pl
from jax.experimental.pallas import tpu as pltpu
from jax.sharding import PartitionSpec as P

MESH = pl.DeviceIdType.MESH
F32 = jnp.float32
BF16 = jnp.bfloat16

NGX, NGY, NGZ = 8, 8, 4
BX, BY, BZ = 32, 16, 128
CSWEEPS = 4
BETA1 = 1.5
CENTRE = 4.0 + 2.0 * BETA1
INV = 1.0 / CENTRE

D26 = [d for d in itertools.product((-1, 0, 1), repeat=3) if d != (0, 0, 0)]
D26.sort(key=lambda d: -sum(map(abs, d)))
D44 = D26 + [d for d in itertools.product((-1, 0, 1), (-2, 2), (-1, 0, 1))]
XY4 = [(-1, -1), (-1, 1), (1, -1), (1, 1)]
Z18 = [d for d in D26 if d[2] != 0]


def roll(x, shift, axis):
    size = x.shape[axis]
    shift = shift % size
    return x if shift == 0 else pltpu.roll(x, shift, axis)


def iota(shape, dim):
    return lax.broadcasted_iota(jnp.int32, shape, dim)


def side(n):
    return 0 if n < 0 else 1


def neg(n):
    return (-n[0], -n[1], -n[2])


def moved(x, matrix):
    hi = x.astype(BF16)
    rest = x - hi.astype(F32)
    mid = rest.astype(BF16)
    lo = (rest - mid.astype(F32)).astype(BF16)
    return (
        jnp.dot(lo, matrix, preferred_element_type=F32)
        + jnp.dot(mid, matrix, preferred_element_type=F32)
        + jnp.dot(hi, matrix, preferred_element_type=F32)
    )


def kernel(
    f_hbm, out,
    f0, p0, fr0, fb0, vr0, vb0, k0, s0, pe0,
    fr1, fb1, vr1, vb1, k1, s1, pe1, tmp1,
    fr2, fb2, vr2, vb2, k2, s2, pe2, tmp2,
    fy0, fz0, vy0, vz0, vx0, fk1, fz1, vk1, vz1, ft2, vt2,
    fx_r, fy_r, fxy_r, fz_r, vx_r, vy_r, vxy_r, vz_r,
    f1x_r, f1y_r, f1xy_r, f1z_r, v1x_r, v1y_r, v1xy_r, v1z_r,
    f2_r, v2_r,
    t3, gy_r, gzb, gxb, g3, v3,
    spare, tok, tok4, io_sem, s_all, r_f0, r_v0, r_f1, r_v1, r_f2, r_f2b, r_v2, r_gy, r_gz, r_gx,
):
    ix, iy, iz = lax.axis_index("gx"), lax.axis_index("gy"), lax.axis_index("gz")

    def there(n):
        nx, ny, nz = ix + n[0], iy + n[1], iz + n[2]
        return (nx >= 0) & (nx < NGX) & (ny >= 0) & (ny < NGY) & (nz >= 0) & (nz < NGZ)

    def at(n):
        return (
            jnp.clip(ix + n[0], 0, NGX - 1),
            jnp.clip(iy + n[1], 0, NGY - 1),
            jnp.clip(iz + n[2], 0, NGZ - 1),
        )

    load = pltpu.make_async_copy(f_hbm, f0, io_sem)
    load.start()

    barrier = pltpu.get_barrier_semaphore()
    count = 0
    for d in D26:
        ok = there(d)
        count = count + ok.astype(jnp.int32)

        @pl.when(ok)
        def _(d=d):
            pl.semaphore_signal(barrier, inc=1, device_id=at(d), device_id_type=MESH)

    def token(sem, reach):
        for d in ((-reach, 0, 0), (reach, 0, 0), (0, -reach, 0), (0, reach, 0)):
            @pl.when(there(d))
            def _(d=d):
                pl.semaphore_signal(sem, inc=1, device_id=at(d), device_id_type=MESH)

    lane = iota((8, 128), 1)
    row = iota((8, 128), 0)
    lane16 = iota((16, 128), 1)
    r32, l32 = iota((32, 128), 0), iota((32, 128), 1)
    signed = jnp.where(l32 < 96, l32, l32 - 128)

    class Level:
        def __init__(self, fr, fb, vr, vb, k, first, main, rows, window, odd, start, total):
            self.fr, self.fb, self.vr, self.vb, self.k = fr, fb, vr, vb, k
            self.first, self.main, self.rows, self.window = first, main, rows, window
            self.odd, self.start, self.total = odd, start, total
            self.planes = main + 2 * first

        def coefficient(self, i, lo, hi):
            if self.first <= i < self.first + self.main:
                return self.k[1, lo:hi, :]
            pos = self.start + i
            return self.k[jnp.where((pos >= 0) & (pos < self.total), 1, 0), lo:hi, :]

        def even(self, i, lo, hi):
            return (iota((hi - lo, 128), 0) + (lo + i + self.odd)) % 2 == 0

    lev0 = Level(fr0, fb0, vr0, vb0, k0, 4, BX, (8, 24), (4, 28), 0, ix * BX - 4, NGX * BX)
    lev1 = Level(fr1, fb1, vr1, vb1, k1, 6, 16, (16, 24), (8, 32), 0, ix * 16 - 6, NGX * 16)
    lev2 = Level(fr2, fb2, vr2, vb2, k2, 7, 4, (16, 24), (8, 32), 1, iy * 4 - 7, NGY * 4)

    def around(level, src, i, lo, hi, red):
        c = src[i, lo:hi, :]
        up, down = roll(c, 1, 1), roll(c, -1, 1)
        even = level.even(i, lo, hi)
        z = jnp.where(even, up, down) if red else jnp.where(even, down, up)
        s = (src[i - 1, lo:hi, :] + src[i + 1, lo:hi, :]) + (
            src[i, lo - 1 : hi - 1, :] + src[i, lo + 1 : hi + 1, :]
        )
        return s + BETA1 * (c + z)

    def half(level, lo, hi, red, rows=None):
        dst, src = (level.vr, level.vb) if red else (level.vb, level.vr)
        source = level.fr if red else level.fb
        a, b = rows or level.window
        for i in range(lo, hi):
            s = source[i, a:b, :] + around(level, src, i, a, b, red)
            dst[i, a:b, :] = s * level.coefficient(i, a, b)

    def first_half(level, lo, hi):
        a, b = level.window
        for i in range(lo, hi):
            level.vr[i, a:b, :] = level.fr[i, a:b, :] * level.coefficient(i, a, b)

    def smooth_down(level):
        n, m = level.first, level.first + level.main
        first_half(level, n - 4, m + 4)
        half(level, n - 3, m + 3, False)
        half(level, n - 2, m + 2, True)
        half(level, n - 1, m + 1, False)

    def residual(level, i):
        a, b = level.rows
        vr, vb = level.vr[i, a:b, :], level.vb[i, a:b, :]
        red = level.fr[i, a:b, :] - (CENTRE * vr - around(level, level.vb, i, a, b, True))
        black = level.fb[i, a:b, :] - (CENTRE * vb - around(level, level.vr, i, a, b, False))
        return red + black

    def split_rows(a, even):
        return jnp.concatenate([jnp.where(even, a, 0.0), jnp.where(even, 0.0, a)], axis=1)

    k256, c128 = iota((256, 128), 0), iota((256, 128), 1)
    z256 = k256 % 128
    red256 = (z256 + k256 // 128) % 2 == 0

    load.wait()

    kk2, cc2 = iota((256, 256), 0), iota((256, 256), 1)
    same = kk2 // 128 == cc2 // 128
    kk2, cc2 = kk2 % 128, cc2 % 128
    to_pairs = jnp.where(same & (cc2 == kk2 // 2 + 64 * (kk2 % 2)), 1.0, 0.0).astype(BF16)
    to_cells = jnp.where(same & (kk2 == cc2 // 2 + 64 * (cc2 % 2)), 1.0, 0.0).astype(BF16)
    for part in range(4):
        rows = []
        for x in range(8 * part, 8 * part + 8, 2):
            rows.append(jnp.concatenate([f0[x], f0[x + 1]], axis=1))
        p = moved(jnp.concatenate(rows, axis=0), to_pairs)
        for x in range(8):
            q = p[16 * (x // 2) : 16 * (x // 2) + 16, 128 * (x % 2) : 128 * (x % 2) + 128]
            p0[8 * part + x] = jnp.where((iota((16, 128), 0) + x) % 2 == 0, q, roll(q, 64, 1))

    def pack0(plane, yp, zp):
        lo = jnp.zeros((16, 128), F32)
        hi = jnp.zeros((16, 128), F32)
        slot = (lane16 % 64) // 2
        for x in range(BX):
            p = plane(x)
            half_tile = slice(4 * (x % 2), 4 * (x % 2) + 4)
            yp[0, x // 2, half_tile, :] = p[0:4]
            yp[1, x // 2, half_tile, :] = p[12:16]
            t = roll(p, 2 * x, 1)
            lo = jnp.where(slot == x, t, lo)
            hi = jnp.where(slot == (x - 1) % BX, roll(p, 64, 1) if x == 0 else t, hi)
        zp[0] = lo
        zp[1] = hi

    def copies0(xs, yp, zp, xr, yr, xyr, zr, ss, rs):
        out = []
        for d in D26:
            dx, dy, dz = d
            if dz == 0 and dy == 0:
                s, t = xs(dx), xr.at[side(-dx)]
            elif dz == 0 and dx == 0:
                s, t = yp.at[side(dy)], yr.at[side(-dy)]
            elif dz == 0:
                s = yp.at[side(dy), pl.ds(0 if dx < 0 else 14, 2)]
                t = xyr.at[XY4.index((-dx, -dy))]
            else:
                slot = Z18.index(neg(d))
                if dy == 0:
                    s, t = zp.at[side(dz)], zr.at[slot]
                else:
                    rows = pl.ds(0 if dy < 0 else 8, 8)
                    s, t = zp.at[side(dz), rows], zr.at[slot, rows]
            out.append((d, pltpu.make_async_remote_copy(s, t, ss, rs, at(d), MESH)))
        return out

    def start(copies):
        for d, c in copies:
            @pl.when(there(d))
            def _(c=c):
                c.start()

    near_x = jnp.where((ix > 0) & (ix < NGX - 1), 2, 1)
    near_z = jnp.where((iz > 0) & (iz < NGZ - 1), 2, 1)
    near_y = jnp.where((iy > 0) & (iy < NGY - 1), 2, 1)
    far_y = jnp.where((iy > 1) & (iy < NGY - 2), 2, 1)

    def units0(x, y, y2, z):
        return x * 8 + y * 16 + x * y * 2 + z * (2 + 2 * x + y + x * y)

    def units1(x, y, y2, z):
        return x * 3 + y * 8 + x * y * 3 + z * (1 + x) * (1 + y)

    def units2(x, y, y2, z):
        return (1 + x) * (1 + y) * (1 + z) - 1

    def units2b(x, y, y2, z):
        return (1 + x) * y2 * (1 + z)

    def wait_units(sem, n):
        pltpu.make_async_copy(spare.at[pl.ds(0, n)], spare.at[pl.ds(0, n)], sem).wait()

    def arrive(sem, units):
        for x, (y, y2), z in itertools.product((1, 2), ((1, 1), (2, 1), (2, 2)), (1, 2)):
            @pl.when((near_x == x) & (near_y == y) & (far_y == y2) & (near_z == z))
            def _(n=units(x, y, y2, z)):
                wait_units(sem, n)

    def unpack0(own, xr, yr, xyr, zr, put, colours):
        for nx in (-1, 0, 1):
            for ny, src, dst, num in ((-1, 8, 0, 8), (0, 0, 8, 16), (1, 0, 24, 8)):
                low = zr[Z18.index((nx, ny, -1)), src : src + num, :]
                high = zr[Z18.index((nx, ny, 1)), src : src + num, :]
                lanes = iota((num, 128), 1)
                mixed = [jnp.where(lanes < 64, high, low), jnp.where(lanes < 64, low, high)]
                xs = range(28, 32) if nx < 0 else (range(32) if nx == 0 else range(4))
                for x in xs:
                    if ny == 0:
                        p = own(x) if nx == 0 else xr[side(nx), x % 4]
                    else:
                        if nx == 0:
                            p = yr[side(ny), x // 2]
                        else:
                            p = xyr[XY4.index((nx, ny)), (x % 4) // 2]
                        if (x % 2 == 0) == (ny < 0):
                            p = roll(p, 4, 0)
                    for colour in range(colours):
                        if x == 0:
                            a = roll(high, 64 if colour == 0 else 0, 1)
                            b = roll(low, 0 if colour == 0 else 64, 1)
                            e = jnp.where(lanes < 96, a, b)
                        else:
                            e = roll(mixed[colour], (64 if colour == 0 else 0) - 2 * x, 1)
                        q = p if colour == 0 else roll(p, 64, 1)
                        i = 32 * nx + x + 4
                        put(colour, i, dst, num, jnp.where(lanes < 64, q, e))

    def clean(level):
        def put(colour, i, dst, num, value):
            ok = level.coefficient(i, dst, dst + num) > 0.0
            (level.fr if colour == 0 else level.fb)[i, dst : dst + num, :] = jnp.where(ok, value, 0.0)

        return put

    def corrected(level, add):
        def put(colour, i, dst, num, value):
            ok = level.coefficient(i, dst, dst + num) > 0.0
            level.vb[i, dst : dst + num, :] = jnp.where(ok, value + add(i, dst, num), 0.0)

        return put

    ef0 = copies0(
        lambda dx: p0.at[pl.ds(0 if dx < 0 else 28, 4)], fy0, fz0, fx_r, fy_r, fxy_r, fz_r, s_all, r_f0
    )
    ev0 = copies0(
        lambda dx: vx0.at[side(dx)],
        vy0, vz0, vx_r, vy_r, vxy_r, vz_r, s_all, r_v0,
    )

    pack0(lambda x: p0[x], fy0, fz0)
    pl.semaphore_wait(barrier, count)
    start(ef0)

    def fill(ref, halo, pairs, start_pairs, total_pairs, rows_at, total_rows):
        zp = start_pairs + signed
        ok = (signed >= -halo) & (signed < pairs + halo) & (zp >= 0) & (zp < total_pairs)
        ok = ok & (rows_at >= 0) & (rows_at < total_rows)
        ref[0] = jnp.zeros((32, 128), F32)
        ref[1] = jnp.where(ok, INV, 0.0)

    fill(k0, 2, 64, iz * 64, NGZ * 64, iy * BY + r32 - 8, NGY * BY)
    fill(k1, 3, 32, iz * 32, NGZ * 32, iy * 8 + r32 - 16, NGY * 8)
    fill(k2, 4, 16, iz * 16, NGZ * 16, ix * 8 + r32 - 16, NGX * 8)

    def zero(ref):
        @pl.loop(0, ref.shape[0])
        def _(i):
            ref[i] = jnp.zeros(ref.shape[1:], F32)

    for ref in (vr0, vb0, vr1, vb1, vr2, vb2, pe0, pe1, pe2, v3, tmp2):
        zero(ref)

    split1 = iota((256, 256), 1)
    k1i = iota((256, 256), 0)
    z1i = k1i % 128
    red1 = (z1i + k1i // 128) % 2 == 0
    packed = (split1 < 128) & (split1 % 64 == z1i // 2 + jnp.where(red1, 0, 32))
    apart = (split1 >= 128) & (split1 - 128 == z1i // 2 + jnp.where(red1, 0, 64))
    to_pairs1 = jnp.where((z1i < 64) & (packed | apart), 0.5, 0.0).astype(BF16)
    to_pairs2 = jnp.where(
        (z256 < 32) & (c128 % 32 == z256 // 2 + jnp.where(red256, 0, 16)), 0.5, 0.0
    ).astype(BF16)
    csign = jnp.where(cc2 < 96, cc2, cc2 - 128)
    wanted = ((csign + 128) // 2 - 64 + 64 * (csign % 2)) % 128
    from_pairs = jnp.where(same & (kk2 == wanted) & (csign >= -4) & (csign < 68), 1.0, 0.0).astype(BF16)

    arrive(r_f0, units0)
    token(tok, 2)
    unpack0(lambda x: p0[x], fx_r, fy_r, fxy_r, fz_r, clean(lev0), 2)
    smooth_down(lev0)
    for x in range(16):
        s0[x] = residual(lev0, 4 + 2 * x) + residual(lev0, 5 + 2 * x)

    rows = []
    for x in range(16):
        a = s0[x, pl.ds(0, 8, stride=2), :] + s0[x, pl.ds(1, 8, stride=2), :]
        rows.append(split_rows(a, (row + x) % 2 == 0))
    b1 = moved(jnp.concatenate(rows, axis=0), to_pairs1)

    def zpack1(plane, zp):
        lo = jnp.zeros((8, 128), F32)
        hi = jnp.zeros((8, 128), F32)
        for x in range(16):
            p = plane(x)
            here = (lane % 64) // 3 == x
            lo = jnp.where(here, roll(p, 3 * x, 1), lo)
            hi = jnp.where(here, roll(p, 3 * x - 29, 1), hi)
        zp[0] = lo
        zp[1] = hi

    def copies1(pk, zp, xr, yr, xyr, zr, ss, rs):
        out = []
        for d in D26:
            dx, dy, dz = d
            if dz == 0 and dx == 0:
                s, t = pk, yr.at[side(-dy)]
            elif dz == 0:
                s = pk.at[pl.ds(0 if dx < 0 else 5, 3)]
                t = xr.at[side(-dx)] if dy == 0 else xyr.at[XY4.index((-dx, -dy))]
            else:
                s, t = zp.at[side(dz)], zr.at[Z18.index(neg(d))]
            out.append((d, pltpu.make_async_remote_copy(s, t, ss, rs, at(d), MESH)))
        return out

    def unpack1(pk, xr, yr, xyr, zr, put, colours):
        for xe in range(28):
            nx, x = (-1, 10 + xe) if xe < 6 else ((0, xe - 6) if xe < 22 else (1, xe - 22))
            for ny in (-1, 0, 1):
                if nx == 0:
                    mid = pk[x // 2] if ny == 0 else yr[side(ny), x // 2]
                else:
                    tile = x // 2 - 5 if nx < 0 else x // 2
                    mid = xr[side(nx), tile] if ny == 0 else xyr[XY4.index((nx, ny)), tile]
                low, high = zr[Z18.index((nx, ny, -1))], zr[Z18.index((nx, ny, 1))]
                for colour in range(colours):
                    a = roll(mid, -64 * (x % 2) - 32 * colour, 1)
                    b = roll(high, 32 - 3 * x - 64 * colour, 1)
                    c = roll(low, 125 - 3 * x - 64 * colour, 1)
                    put(colour, xe, 16 + 8 * ny, 8, jnp.where(lane < 32, a, jnp.where(lane < 64, b, c)))

    ef1 = copies1(fk1, fz1, f1x_r, f1y_r, f1xy_r, f1z_r, s_all, r_f1)
    ev1 = copies1(vk1, vz1, v1x_r, v1y_r, v1xy_r, v1z_r, s_all, r_v1)
    for t in range(8):
        fk1[t] = jnp.where(lane < 64, b1[16 * t : 16 * t + 8, 0:128], b1[16 * t + 8 : 16 * t + 16, 0:128])
    zpack1(lambda x: b1[8 * x : 8 * x + 8, 128:256], fz1)
    start(ef1)
    arrive(r_f1, units1)
    pl.semaphore_wait(tok, jnp.where((ix > 1) & (ix < NGX - 2), 2, 1) + far_y)
    token(tok4, 4)
    unpack1(fk1, f1x_r, f1y_r, f1xy_r, f1z_r, clean(lev1), 2)
    smooth_down(lev1)
    for x in range(8):
        s1[8 * x : 8 * x + 8, :] = residual(lev1, 6 + 2 * x) + residual(lev1, 7 + 2 * x)

    rows = []
    for y in range(4):
        a = s1[pl.ds(2 * y, 8, stride=8), :] + s1[pl.ds(2 * y + 1, 8, stride=8), :]
        rows.append(split_rows(a, (row + y) % 2 == 0))
    b2 = moved(jnp.concatenate(rows, axis=0), to_pairs2)

    def copies2(t, tr, ss, rs, directions):
        out = []
        for d in directions:
            dst = tr.at[D44.index(neg(d))]
            out.append((d, pltpu.make_async_remote_copy(t, dst, ss, rs, at(d), MESH)))
        return out

    def unpack2(own, tr, which, put, colours):
        part = lane % 32
        for ny in which:
            if ny == -2:
                ys = [(i, 1 + i) for i in range(3)]
            elif ny == 2:
                ys = [(15 + i, i) for i in range(3)]
            else:
                ys = [(7 + 4 * ny + i, i) for i in range(4)]
            for nx in (-1, 0, 1):
                mid = own[...] if (nx, ny) == (0, 0) else tr[D44.index((nx, ny, 0))]
                low, high = tr[D44.index((nx, ny, -1))], tr[D44.index((nx, ny, 1))]
                for colour in range(colours):
                    a = roll(mid, -16 * colour, 1)
                    b = roll(high, 16 - 16 * colour, 1)
                    c = roll(low, 112 - 16 * colour, 1)
                    mixed = jnp.where(part < 16, a, jnp.where(part < 24, b, c))
                    for e, y in ys:
                        put(colour, e, 16 + 8 * nx, 8, roll(mixed, -32 * y, 1))

    ef2 = copies2(ft2, f2_r, s_all, r_f2, D26)
    ef2b = copies2(ft2, f2_r, s_all, r_f2b, D44[26:])
    ev2 = copies2(vt2, v2_r, s_all, r_v2, D44)
    acc = b2[0:8]
    for y in range(1, 4):
        acc = jnp.where(lane // 32 == y, b2[8 * y : 8 * y + 8], acc)
    ft2[...] = acc
    start(ef2)
    arrive(r_f2, units2)
    unpack2(ft2, f2_r, (-1, 0, 1), clean(lev2), 2)
    smooth_down(lev2)

    for y in range(2):
        s2[8 * y : 8 * y + 8, :] = residual(lev2, 7 + 2 * y) + residual(lev2, 8 + 2 * y)
    a3 = s2[pl.ds(0, 8, stride=2), :] + s2[pl.ds(1, 8, stride=2), :]
    a3 = jnp.where(lane < 16, 0.5 * a3, 0.0)
    a3 = pltpu.roll(a3, 0, 1, stride=16, stride_axis=0)
    a3 = jnp.sum(a3, axis=0, keepdims=True)
    t3[...] = jnp.where(row == iy, a3, 0.0)

    egy, egz, egx = [], [], []
    for k in range(1, NGY):
        peer = (ix, lax.rem(iy + k, NGY), iz)
        egy.append(pltpu.make_async_remote_copy(t3, gy_r.at[k - 1], s_all, r_gy, peer, MESH))
    for k in range(1, NGZ):
        peer = (ix, iy, lax.rem(iz + k, NGZ))
        egz.append(pltpu.make_async_remote_copy(gzb.at[iz], gzb.at[iz], s_all, r_gz, peer, MESH))
    for k in range(1, NGX):
        peer = (lax.rem(ix + k, NGX), iy, iz)
        egx.append(pltpu.make_async_remote_copy(gzb, gxb.at[ix], s_all, r_gx, peer, MESH))

    pl.semaphore_wait(tok4, 2)
    for c in egy:
        c.start()
    start(ef2b)
    acc = jnp.zeros((8, 128), F32)
    for y in range(4):
        acc = jnp.where(lane // 32 == y, roll(vb2[7 + y, 16:24, :], 32 * y, 1), acc)
    vt2[...] = acc
    for t in range(8):
        vk1[t] = jnp.where(lane < 64, vb1[6 + 2 * t, 16:24, :], roll(vb1[7 + 2 * t, 16:24, :], 64, 1))
    zpack1(lambda x: vb1[6 + x, 16:24, :], vz1)
    pack0(lambda x: vb0[4 + x, 8:24, :], vy0, vz0)
    for x in range(4):
        vx0[0, x] = vb0[4 + x, 8:24, :]
        vx0[1, x] = vb0[32 + x, 8:24, :]
    arrive(r_f2b, units2b)
    unpack2(ft2, f2_r, (-2, 2), clean(lev2), 2)
    wait_units(r_gy, 7)
    line = t3[...]
    for k in range(NGY - 1):
        line = line + gy_r[k]
    gzb[iz] = line
    for c in egz:
        c.start()
    wait_units(r_gz, 3)
    for c in egx:
        c.start()
    start(ev2)
    start(ev1)
    start(ev0)
    gxb[ix] = gzb[...]
    wait_units(r_gx, 28)

    for gx in range(NGX):
        for xl in range(4):
            acc = jnp.zeros((8, 128), F32)
            for gz in range(NGZ):
                acc = jnp.where((lane % 64) // 16 == gz, roll(gxb[gx, gz], (gz - xl) * 16, 1), acc)
            g3[4 * gx + xl] = acc

    zl = lane % 64
    w_lo = jnp.where(zl == 0, 0.0, BETA1)
    w_hi = jnp.where(zl == 63, 0.0, BETA1)
    y_edge = jnp.where(((row == 0) & (lane < 64)) | ((row == 7) & (lane >= 64)), 0.0, 1.0)
    par3 = (lane // 64 + lane) & 1
    colours3 = (par3 == 0, par3 == 1)

    def sum3(x):
        c = v3[x + 4]
        a = roll(c, 64, 1)
        w = jnp.where(lane < 64, roll(a, 1, 0), roll(a, -1, 0)) * y_edge
        s = (v3[x + 3] + v3[x + 5]) + (a + w)
        return c, s + (roll(c, 1, 1) * w_lo + roll(c, -1, 1) * w_hi)

    def half3(colour):
        for j in range(4):
            done = []
            for x in range(8 * j, 8 * j + 8):
                c, s = sum3(x)
                done.append(jnp.where(colours3[(x + colour) % 2], (g3[x] + s) * INV, c))
            for u in range(8):
                v3[8 * j + u + 4] = done[u]

    for x in range(32):
        v3[x + 4] = jnp.where(colours3[x % 2], g3[x] * INV, 0.0)
    half3(1)
    half3(0)
    half3(1)

    def small(g, level):
        n = len(g)
        dz, dy = 2 ** (level - 3), 2 ** (level - 4)
        lo = jnp.where(zl < dz, 0.0, BETA1)
        hi = jnp.where(zl >= 64 - dz, 0.0, BETA1)
        ylo = jnp.where(row < dy, 0.0, 1.0)
        yhi = jnp.where(row >= 8 - dy, 0.0, 1.0)
        par = (row // dy + zl // dz) & 1
        colours = (par == 0, par == 1)

        def total(v, x):
            c = v[x]
            s = roll(c, dz, 1) * lo + roll(c, -dz, 1) * hi
            s = s + (roll(c, dy, 0) * ylo + roll(c, -dy, 0) * yhi)
            if x > 0:
                s = s + v[x - 1]
            if x < n - 1:
                s = s + v[x + 1]
            return s

        def sweep(v, colour):
            return [
                jnp.where(colours[(x + colour) % 2], (g[x] + total(v, x)) * INV, v[x]) for x in range(n)
            ]

        v = [jnp.where(colours[x % 2], g[x] * INV, 0.0) for x in range(n)]
        v = sweep(v, 1)
        if level == 6:
            for _ in range(CSWEEPS - 1):
                v = sweep(sweep(v, 0), 1)
            return v
        v = sweep(sweep(v, 0), 1)
        r = [g[x] - (CENTRE * v[x] - total(v, x)) for x in range(n)]
        coarse = []
        for x in range(n // 2):
            t = r[2 * x] + r[2 * x + 1]
            t = t + jnp.where((row // dy) % 2 == 0, roll(t, -dy, 0), roll(t, dy, 0))
            t = t + jnp.where((zl // dz) % 2 == 0, roll(t, -dz, 1), roll(t, dz, 1))
            coarse.append(0.5 * t)
        e = small(coarse, level + 1)
        v = [v[x] + e[x // 2] for x in range(n)]
        for _ in range(2):
            v = sweep(sweep(v, 0), 1)
        return v

    def resid3(x):
        c, s = sum3(x)
        return g3[x] - (CENTRE * c - s)

    g4 = []
    for x in range(16):
        t = resid3(2 * x) + resid3(2 * x + 1)
        t = t + roll(t, 64, 1)
        t = t + jnp.where(lane % 2 == 0, roll(t, -1, 1), roll(t, 1, 1))
        g4.append(0.5 * t)
    e4 = small(g4, 4)
    for x in range(32):
        v3[4 + x] = v3[4 + x] + e4[x // 2]
    for _ in range(2):
        half3(0)
        half3(1)

    for x in range(12):
        e = v3[4 * ix + x]
        for yl in range(2):
            tmp2[yl, 16 + 8 * x : 24 + 8 * x, :] = pltpu.roll(e, (128 - 16 * iz + 64 * yl) % 128, 1)
    for j in range(10):
        e = tmp2[j % 2, pl.ds(16 + iy - 2 + j // 2, 12, stride=8), :]
        pe2[j, pl.ds(8, 12, stride=2), :] = e
        pe2[j, pl.ds(9, 12, stride=2), :] = e
    arrive(r_v2, lambda *c: units2(*c) + units2b(*c))
    add2 = corrected(lev2, lambda i, dst, num: pe2[(i + 1) // 2, dst : dst + num, :])
    unpack2(vt2, v2_r, (-2, -1, 0, 1, 2), add2, 1)
    half(lev2, 1, 17, True)
    half(lev2, 2, 16, False)
    half(lev2, 3, 15, True)
    half(lev2, 4, 14, False)

    def cells(level, i, a, b):
        even = level.even(i, a, b)
        r, k = level.vr[i, a:b, :], level.vb[i, a:b, :]
        first, second = jnp.where(even, r, k), roll(jnp.where(even, k, r), 64, 1)
        lanes = iota((b - a, 128), 1)
        if level is lev0:
            return jnp.where(lanes < 64, first, second)
        return jnp.where((lanes < 40) | (lanes >= 104), first, second)

    def merged(level, planes, a, b, matrix):
        rows = []
        for i in range(0, len(planes), 2):
            rows.append(jnp.concatenate([cells(level, j, a, b) for j in planes[i : i + 2]], axis=1))
        u = moved(jnp.concatenate(rows, axis=0), matrix)
        n = b - a
        return [u[n * (i // 2) : n * (i // 2) + n, 128 * (i % 2) : 128 * (i % 2) + 128] for i in range(len(planes))]

    for i, e in enumerate(merged(lev2, range(3, 15), 8, 32, from_pairs)):
        tmp1[24 * i : 24 * i + 24, :] = e
    for k in range(14):
        e = tmp1[pl.ds(5 + k, 12, stride=24), :]
        pe1[k, pl.ds(8, 12, stride=2), :] = e
        pe1[k, pl.ds(9, 12, stride=2), :] = e
    arrive(r_v1, units1)
    add1 = corrected(lev1, lambda i, dst, num: pe1[i // 2, dst : dst + num, :])
    unpack1(vk1, v1x_r, v1y_r, v1xy_r, v1z_r, add1, 1)
    half(lev1, 1, 27, True)
    half(lev1, 2, 26, False)
    half(lev1, 3, 25, True)
    half(lev1, 4, 24, False)

    for k, e in enumerate(merged(lev1, range(4, 24), 14, 30, from_pairs)):
        e = e[0:12]
        pe0[k, pl.ds(4, 12, stride=2), :] = e
        pe0[k, pl.ds(5, 12, stride=2), :] = e
    arrive(r_v0, units0)
    add0 = corrected(lev0, lambda i, dst, num: pe0[i // 2, dst : dst + num, :])
    unpack0(lambda x: vb0[4 + x, 8:24, :], vx_r, vy_r, vxy_r, vz_r, add0, 1)
    half(lev0, 1, 39, True)
    half(lev0, 2, 38, False)
    half(lev0, 3, 37, True)
    half(lev0, 4, 36, False, (8, 24))

    for part in range(4):
        planes = range(4 + 8 * part, 12 + 8 * part)
        for x, e in enumerate(merged(lev0, planes, 8, 24, to_cells)):
            out[8 * part + x] = e
    arrive(s_all, lambda *c: 2 * (units0(*c) + units1(*c) + units2(*c) + units2b(*c)) + 38)


def on_device(density):
    def vmem(*shape):
        return pltpu.VMEM(shape, F32)

    coef = vmem(2, 32, 128)
    level0 = [vmem(BX, BY, BZ)] * 2 + [vmem(40, 32, 128)] * 4 + [coef, vmem(16, 16, 128), vmem(20, 32, 128)]
    level1 = [vmem(28, 40, 128)] * 4 + [coef, vmem(64, 128), vmem(14, 32, 128), vmem(288, 128)]
    level2 = [vmem(18, 40, 128)] * 4 + [coef, vmem(16, 128), vmem(10, 32, 128), vmem(2, 128, 128)]
    packs = [vmem(2, 16, 8, 128), vmem(2, 16, 128)] * 2 + [vmem(2, 4, 16, 128)] + [vmem(8, 8, 128), vmem(2, 8, 128)] * 2
    packs += [vmem(8, 128)] * 2
    recv0 = [vmem(2, 4, 16, 128), vmem(2, 16, 8, 128), vmem(4, 2, 8, 128), vmem(18, 16, 128)] * 2
    recv1 = [vmem(2, 3, 8, 128), vmem(2, 8, 8, 128), vmem(4, 3, 8, 128), vmem(18, 8, 128)] * 2
    recv2 = [vmem(44, 8, 128)] * 2
    gather = [vmem(8, 128), vmem(7, 8, 128), vmem(4, 8, 128), vmem(8, 4, 8, 128), vmem(32, 8, 128), vmem(40, 8, 128)]
    dma = pltpu.SemaphoreType.DMA
    token = pltpu.SemaphoreType.REGULAR
    sems = [vmem(400, 8, 128), token, token] + [dma] * 12
    return pl.pallas_call(
        kernel,
        out_shape=jax.ShapeDtypeStruct((BX, BY, BZ), F32),
        in_specs=[pl.BlockSpec(memory_space=pltpu.HBM)],
        out_specs=pl.BlockSpec(memory_space=pltpu.VMEM),
        scratch_shapes=level0 + level1 + level2 + packs + recv0 + recv1 + recv2 + gather + sems,
        compiler_params=pltpu.CompilerParams(
            collective_id=0, has_side_effects=True, vmem_limit_bytes=48 * 1024 * 1024
        ),
    )(density)


def solution(mesh):
    spec = P("gx", "gy", "gz")
    return jax.shard_map(on_device, mesh=mesh, in_specs=(spec,), out_specs=spec, check_vma=False)
```

```python
import itertools

import jax
import jax.numpy as jnp
from jax import lax
from jax.experimental import pallas as pl
from jax.experimental.pallas import tpu as pltpu
from jax.sharding import PartitionSpec as P

MESH = pl.DeviceIdType.MESH
F32 = jnp.float32
BF16 = jnp.bfloat16

NGX, NGY, NGZ = 8, 8, 4
BX, BY, BZ = 32, 16, 128
CSWEEPS = 4
BETA1 = 1.5
CENTRE = 4.0 + 2.0 * BETA1
INV = 1.0 / CENTRE

D26 = [d for d in itertools.product((-1, 0, 1), repeat=3) if d != (0, 0, 0)]
D26.sort(key=lambda d: -sum(map(abs, d)))
D44 = D26 + [d for d in itertools.product((-1, 0, 1), (-2, 2), (-1, 0, 1))]
XY4 = [(-1, -1), (-1, 1), (1, -1), (1, 1)]
Z18 = [d for d in D26 if d[2] != 0]


def roll(x, shift, axis):
    size = x.shape[axis]
    shift = shift % size
    return x if shift == 0 else pltpu.roll(x, shift, axis)


def iota(shape, dim):
    return lax.broadcasted_iota(jnp.int32, shape, dim)


def side(n):
    return 0 if n < 0 else 1


def neg(n):
    return (-n[0], -n[1], -n[2])


def moved(x, matrix):
    hi = x.astype(BF16)
    rest = x - hi.astype(F32)
    mid = rest.astype(BF16)
    lo = (rest - mid.astype(F32)).astype(BF16)
    return (
        jnp.dot(lo, matrix, preferred_element_type=F32)
        + jnp.dot(mid, matrix, preferred_element_type=F32)
        + jnp.dot(hi, matrix, preferred_element_type=F32)
    )


def kernel(
    f_hbm, out,
    f0, p0, fr0, fb0, vr0, vb0, k0, s0, pe0,
    fr1, fb1, vr1, vb1, k1, s1, pe1, tmp1,
    fr2, fb2, vr2, vb2, k2, s2, pe2, tmp2,
    fy0, fz0, vy0, vz0, vx0, fk1, fz1, vk1, vz1, ft2, vt2,
    fx_r, fy_r, fxy_r, fz_r, vx_r, vy_r, vxy_r, vz_r,
    f1x_r, f1y_r, f1xy_r, f1z_r, v1x_r, v1y_r, v1xy_r, v1z_r,
    f2_r, v2_r,
    t3, gy_r, gzb, gxb, g3, v3,
    spare, tok, tok4, io_sem, s_all, r_f0, r_v0, r_f1, r_v1, r_f2, r_f2b, r_v2, r_gy, r_gz, r_gx,
):
    ix, iy, iz = lax.axis_index("gx"), lax.axis_index("gy"), lax.axis_index("gz")

    def there(n):
        nx, ny, nz = ix + n[0], iy + n[1], iz + n[2]
        return (nx >= 0) & (nx < NGX) & (ny >= 0) & (ny < NGY) & (nz >= 0) & (nz < NGZ)

    def at(n):
        return (
            jnp.clip(ix + n[0], 0, NGX - 1),
            jnp.clip(iy + n[1], 0, NGY - 1),
            jnp.clip(iz + n[2], 0, NGZ - 1),
        )

    load = pltpu.make_async_copy(f_hbm, f0, io_sem)
    load.start()

    barrier = pltpu.get_barrier_semaphore()
    count = 0
    for d in D26:
        ok = there(d)
        count = count + ok.astype(jnp.int32)

        @pl.when(ok)
        def _(d=d):
            pl.semaphore_signal(barrier, inc=1, device_id=at(d), device_id_type=MESH)

    def token(sem, reach):
        for d in ((-reach, 0, 0), (reach, 0, 0), (0, -reach, 0), (0, reach, 0)):
            @pl.when(there(d))
            def _(d=d):
                pl.semaphore_signal(sem, inc=1, device_id=at(d), device_id_type=MESH)

    lane = iota((8, 128), 1)
    row = iota((8, 128), 0)
    lane16 = iota((16, 128), 1)
    r32, l32 = iota((32, 128), 0), iota((32, 128), 1)
    signed = jnp.where(l32 < 96, l32, l32 - 128)

    class Level:
        def __init__(self, fr, fb, vr, vb, k, first, main, rows, window, odd, start, total):
            self.fr, self.fb, self.vr, self.vb, self.k = fr, fb, vr, vb, k
            self.first, self.main, self.rows, self.window = first, main, rows, window
            self.odd, self.start, self.total = odd, start, total
            self.planes = main + 2 * first

        def coefficient(self, i, lo, hi):
            if self.first <= i < self.first + self.main:
                return self.k[1, lo:hi, :]
            pos = self.start + i
            return self.k[jnp.where((pos >= 0) & (pos < self.total), 1, 0), lo:hi, :]

        def even(self, i, lo, hi):
            return (iota((hi - lo, 128), 0) + (lo + i + self.odd)) % 2 == 0

    lev0 = Level(fr0, fb0, vr0, vb0, k0, 4, BX, (8, 24), (4, 28), 0, ix * BX - 4, NGX * BX)
    lev1 = Level(fr1, fb1, vr1, vb1, k1, 6, 16, (16, 24), (8, 32), 0, ix * 16 - 6, NGX * 16)
    lev2 = Level(fr2, fb2, vr2, vb2, k2, 7, 4, (16, 24), (8, 32), 1, iy * 4 - 7, NGY * 4)

    def around(level, src, i, lo, hi, red):
        c = src[i, lo:hi, :]
        up, down = roll(c, 1, 1), roll(c, -1, 1)
        even = level.even(i, lo, hi)
        z = jnp.where(even, up, down) if red else jnp.where(even, down, up)
        s = (src[i - 1, lo:hi, :] + src[i + 1, lo:hi, :]) + (
            src[i, lo - 1 : hi - 1, :] + src[i, lo + 1 : hi + 1, :]
        )
        return s + BETA1 * (c + z)

    def half(level, lo, hi, red, rows=None):
        dst, src = (level.vr, level.vb) if red else (level.vb, level.vr)
        source = level.fr if red else level.fb
        a, b = rows or level.window
        for i in range(lo, hi):
            s = source[i, a:b, :] + around(level, src, i, a, b, red)
            dst[i, a:b, :] = s * level.coefficient(i, a, b)

    def first_half(level, lo, hi):
        a, b = level.window
        for i in range(lo, hi):
            level.vr[i, a:b, :] = level.fr[i, a:b, :] * level.coefficient(i, a, b)

    def smooth_down(level):
        n, m = level.first, level.first + level.main
        first_half(level, n - 4, m + 4)
        half(level, n - 3, m + 3, False)
        half(level, n - 2, m + 2, True)
        half(level, n - 1, m + 1, False)

    def residual(level, i):
        a, b = level.rows
        vr, vb = level.vr[i, a:b, :], level.vb[i, a:b, :]
        red = level.fr[i, a:b, :] - (CENTRE * vr - around(level, level.vb, i, a, b, True))
        black = level.fb[i, a:b, :] - (CENTRE * vb - around(level, level.vr, i, a, b, False))
        return red + black

    def split_rows(a, even):
        return jnp.concatenate([jnp.where(even, a, 0.0), jnp.where(even, 0.0, a)], axis=1)

    k256, c128 = iota((256, 128), 0), iota((256, 128), 1)
    z256 = k256 % 128
    red256 = (z256 + k256 // 128) % 2 == 0

    load.wait()

    kk2, cc2 = iota((256, 256), 0), iota((256, 256), 1)
    same = kk2 // 128 == cc2 // 128
    kk2, cc2 = kk2 % 128, cc2 % 128
    to_pairs = jnp.where(same & (cc2 == kk2 // 2 + 64 * (kk2 % 2)), 1.0, 0.0).astype(BF16)
    to_cells = jnp.where(same & (kk2 == cc2 // 2 + 64 * (cc2 % 2)), 1.0, 0.0).astype(BF16)
    for part in range(4):
        rows = []
        for x in range(8 * part, 8 * part + 8, 2):
            rows.append(jnp.concatenate([f0[x], f0[x + 1]], axis=1))
        p = moved(jnp.concatenate(rows, axis=0), to_pairs)
        for x in range(8):
            q = p[16 * (x // 2) : 16 * (x // 2) + 16, 128 * (x % 2) : 128 * (x % 2) + 128]
            p0[8 * part + x] = jnp.where((iota((16, 128), 0) + x) % 2 == 0, q, roll(q, 64, 1))

    def pack0(plane, yp, zp):
        lo = jnp.zeros((16, 128), F32)
        hi = jnp.zeros((16, 128), F32)
        slot = (lane16 % 64) // 2
        for x in range(BX):
            p = plane(x)
            half_tile = slice(4 * (x % 2), 4 * (x % 2) + 4)
            yp[0, x // 2, half_tile, :] = p[0:4]
            yp[1, x // 2, half_tile, :] = p[12:16]
            t = roll(p, 2 * x, 1)
            lo = jnp.where(slot == x, t, lo)
            hi = jnp.where(slot == (x - 1) % BX, roll(p, 64, 1) if x == 0 else t, hi)
        zp[0] = lo
        zp[1] = hi

    def copies0(xs, yp, zp, xr, yr, xyr, zr, ss, rs):
        out = []
        for d in D26:
            dx, dy, dz = d
            if dz == 0 and dy == 0:
                s, t = xs(dx), xr.at[side(-dx)]
            elif dz == 0 and dx == 0:
                s, t = yp.at[side(dy)], yr.at[side(-dy)]
            elif dz == 0:
                s = yp.at[side(dy), pl.ds(0 if dx < 0 else 14, 2)]
                t = xyr.at[XY4.index((-dx, -dy))]
            else:
                slot = Z18.index(neg(d))
                if dy == 0:
                    s, t = zp.at[side(dz)], zr.at[slot]
                else:
                    rows = pl.ds(0 if dy < 0 else 8, 8)
                    s, t = zp.at[side(dz), rows], zr.at[slot, rows]
            out.append((d, pltpu.make_async_remote_copy(s, t, ss, rs, at(d), MESH)))
        return out

    def start(copies):
        for d, c in copies:
            @pl.when(there(d))
            def _(c=c):
                c.start()

    near_x = jnp.where((ix > 0) & (ix < NGX - 1), 2, 1)
    near_z = jnp.where((iz > 0) & (iz < NGZ - 1), 2, 1)
    near_y = jnp.where((iy > 0) & (iy < NGY - 1), 2, 1)
    far_y = jnp.where((iy > 1) & (iy < NGY - 2), 2, 1)

    def units0(x, y, y2, z):
        return x * 8 + y * 16 + x * y * 2 + z * (2 + 2 * x + y + x * y)

    def units1(x, y, y2, z):
        return x * 3 + y * 8 + x * y * 3 + z * (1 + x) * (1 + y)

    def units2(x, y, y2, z):
        return (1 + x) * (1 + y) * (1 + z) - 1

    def units2b(x, y, y2, z):
        return (1 + x) * y2 * (1 + z)

    def wait_units(sem, n):
        pltpu.make_async_copy(spare.at[pl.ds(0, n)], spare.at[pl.ds(0, n)], sem).wait()

    def arrive(sem, units):
        for x, (y, y2), z in itertools.product((1, 2), ((1, 1), (2, 1), (2, 2)), (1, 2)):
            @pl.when((near_x == x) & (near_y == y) & (far_y == y2) & (near_z == z))
            def _(n=units(x, y, y2, z)):
                wait_units(sem, n)

    def unpack0(own, xr, yr, xyr, zr, put, colours):
        for nx in (-1, 0, 1):
            for ny, src, dst, num in ((-1, 8, 0, 8), (0, 0, 8, 16), (1, 0, 24, 8)):
                low = zr[Z18.index((nx, ny, -1)), src : src + num, :]
                high = zr[Z18.index((nx, ny, 1)), src : src + num, :]
                lanes = iota((num, 128), 1)
                mixed = [jnp.where(lanes < 64, high, low), jnp.where(lanes < 64, low, high)]
                xs = range(28, 32) if nx < 0 else (range(32) if nx == 0 else range(4))
                for x in xs:
                    if ny == 0:
                        p = own(x) if nx == 0 else xr[side(nx), x % 4]
                    else:
                        if nx == 0:
                            p = yr[side(ny), x // 2]
                        else:
                            p = xyr[XY4.index((nx, ny)), (x % 4) // 2]
                        if (x % 2 == 0) == (ny < 0):
                            p = roll(p, 4, 0)
                    for colour in range(colours):
                        if x == 0:
                            a = roll(high, 64 if colour == 0 else 0, 1)
                            b = roll(low, 0 if colour == 0 else 64, 1)
                            e = jnp.where(lanes < 96, a, b)
                        else:
                            e = roll(mixed[colour], (64 if colour == 0 else 0) - 2 * x, 1)
                        q = p if colour == 0 else roll(p, 64, 1)
                        i = 32 * nx + x + 4
                        put(colour, i, dst, num, jnp.where(lanes < 64, q, e))

    def clean(level):
        def put(colour, i, dst, num, value):
            ok = level.coefficient(i, dst, dst + num) > 0.0
            (level.fr if colour == 0 else level.fb)[i, dst : dst + num, :] = jnp.where(ok, value, 0.0)

        return put

    def corrected(level, add):
        def put(colour, i, dst, num, value):
            ok = level.coefficient(i, dst, dst + num) > 0.0
            level.vb[i, dst : dst + num, :] = jnp.where(ok, value + add(i, dst, num), 0.0)

        return put

    ef0 = copies0(
        lambda dx: p0.at[pl.ds(0 if dx < 0 else 28, 4)], fy0, fz0, fx_r, fy_r, fxy_r, fz_r, s_all, r_f0
    )
    ev0 = copies0(
        lambda dx: vx0.at[side(dx)],
        vy0, vz0, vx_r, vy_r, vxy_r, vz_r, s_all, r_v0,
    )

    pack0(lambda x: p0[x], fy0, fz0)
    pl.semaphore_wait(barrier, count)
    start(ef0)

    def fill(ref, halo, pairs, start_pairs, total_pairs, rows_at, total_rows):
        zp = start_pairs + signed
        ok = (signed >= -halo) & (signed < pairs + halo) & (zp >= 0) & (zp < total_pairs)
        ok = ok & (rows_at >= 0) & (rows_at < total_rows)
        ref[0] = jnp.zeros((32, 128), F32)
        ref[1] = jnp.where(ok, INV, 0.0)

    fill(k0, 2, 64, iz * 64, NGZ * 64, iy * BY + r32 - 8, NGY * BY)
    fill(k1, 3, 32, iz * 32, NGZ * 32, iy * 8 + r32 - 16, NGY * 8)
    fill(k2, 4, 16, iz * 16, NGZ * 16, ix * 8 + r32 - 16, NGX * 8)

    def zero(ref):
        @pl.loop(0, ref.shape[0])
        def _(i):
            ref[i] = jnp.zeros(ref.shape[1:], F32)

    for ref in (vr0, vb0, vr1, vb1, vr2, vb2, pe0, pe1, pe2, v3, tmp2):
        zero(ref)

    split1 = iota((256, 256), 1)
    k1i = iota((256, 256), 0)
    z1i = k1i % 128
    red1 = (z1i + k1i // 128) % 2 == 0
    packed = (split1 < 128) & (split1 % 64 == z1i // 2 + jnp.where(red1, 0, 32))
    apart = (split1 >= 128) & (split1 - 128 == z1i // 2 + jnp.where(red1, 0, 64))
    to_pairs1 = jnp.where((z1i < 64) & (packed | apart), 0.5, 0.0).astype(BF16)
    to_pairs2 = jnp.where(
        (z256 < 32) & (c128 % 32 == z256 // 2 + jnp.where(red256, 0, 16)), 0.5, 0.0
    ).astype(BF16)
    csign = jnp.where(cc2 < 96, cc2, cc2 - 128)
    wanted = ((csign + 128) // 2 - 64 + 64 * (csign % 2)) % 128
    from_pairs = jnp.where(same & (kk2 == wanted) & (csign >= -4) & (csign < 68), 1.0, 0.0).astype(BF16)

    arrive(r_f0, units0)
    token(tok, 2)
    unpack0(lambda x: p0[x], fx_r, fy_r, fxy_r, fz_r, clean(lev0), 2)
    smooth_down(lev0)
    for x in range(16):
        s0[x] = residual(lev0, 4 + 2 * x) + residual(lev0, 5 + 2 * x)

    rows = []
    for x in range(16):
        a = s0[x, pl.ds(0, 8, stride=2), :] + s0[x, pl.ds(1, 8, stride=2), :]
        rows.append(split_rows(a, (row + x) % 2 == 0))
    b1 = moved(jnp.concatenate(rows, axis=0), to_pairs1)

    def zpack1(plane, zp):
        lo = jnp.zeros((8, 128), F32)
        hi = jnp.zeros((8, 128), F32)
        for x in range(16):
            p = plane(x)
            here = (lane % 64) // 3 == x
            lo = jnp.where(here, roll(p, 3 * x, 1), lo)
            hi = jnp.where(here, roll(p, 3 * x - 29, 1), hi)
        zp[0] = lo
        zp[1] = hi

    def copies1(pk, zp, xr, yr, xyr, zr, ss, rs):
        out = []
        for d in D26:
            dx, dy, dz = d
            if dz == 0 and dx == 0:
                s, t = pk, yr.at[side(-dy)]
            elif dz == 0:
                s = pk.at[pl.ds(0 if dx < 0 else 5, 3)]
                t = xr.at[side(-dx)] if dy == 0 else xyr.at[XY4.index((-dx, -dy))]
            else:
                s, t = zp.at[side(dz)], zr.at[Z18.index(neg(d))]
            out.append((d, pltpu.make_async_remote_copy(s, t, ss, rs, at(d), MESH)))
        return out

    def unpack1(pk, xr, yr, xyr, zr, put, colours):
        for xe in range(28):
            nx, x = (-1, 10 + xe) if xe < 6 else ((0, xe - 6) if xe < 22 else (1, xe - 22))
            for ny in (-1, 0, 1):
                if nx == 0:
                    mid = pk[x // 2] if ny == 0 else yr[side(ny), x // 2]
                else:
                    tile = x // 2 - 5 if nx < 0 else x // 2
                    mid = xr[side(nx), tile] if ny == 0 else xyr[XY4.index((nx, ny)), tile]
                low, high = zr[Z18.index((nx, ny, -1))], zr[Z18.index((nx, ny, 1))]
                for colour in range(colours):
                    a = roll(mid, -64 * (x % 2) - 32 * colour, 1)
                    b = roll(high, 32 - 3 * x - 64 * colour, 1)
                    c = roll(low, 125 - 3 * x - 64 * colour, 1)
                    put(colour, xe, 16 + 8 * ny, 8, jnp.where(lane < 32, a, jnp.where(lane < 64, b, c)))

    ef1 = copies1(fk1, fz1, f1x_r, f1y_r, f1xy_r, f1z_r, s_all, r_f1)
    ev1 = copies1(vk1, vz1, v1x_r, v1y_r, v1xy_r, v1z_r, s_all, r_v1)
    for t in range(8):
        fk1[t] = jnp.where(lane < 64, b1[16 * t : 16 * t + 8, 0:128], b1[16 * t + 8 : 16 * t + 16, 0:128])
    zpack1(lambda x: b1[8 * x : 8 * x + 8, 128:256], fz1)
    start(ef1)
    arrive(r_f1, units1)
    pl.semaphore_wait(tok, jnp.where((ix > 1) & (ix < NGX - 2), 2, 1) + far_y)
    token(tok4, 4)
    unpack1(fk1, f1x_r, f1y_r, f1xy_r, f1z_r, clean(lev1), 2)
    smooth_down(lev1)
    for x in range(8):
        s1[8 * x : 8 * x + 8, :] = residual(lev1, 6 + 2 * x) + residual(lev1, 7 + 2 * x)

    rows = []
    for y in range(4):
        a = s1[pl.ds(2 * y, 8, stride=8), :] + s1[pl.ds(2 * y + 1, 8, stride=8), :]
        rows.append(split_rows(a, (row + y) % 2 == 0))
    b2 = moved(jnp.concatenate(rows, axis=0), to_pairs2)

    def copies2(t, tr, ss, rs, directions):
        out = []
        for d in directions:
            dst = tr.at[D44.index(neg(d))]
            out.append((d, pltpu.make_async_remote_copy(t, dst, ss, rs, at(d), MESH)))
        return out

    def unpack2(own, tr, which, put, colours):
        part = lane % 32
        for ny in which:
            if ny == -2:
                ys = [(i, 1 + i) for i in range(3)]
            elif ny == 2:
                ys = [(15 + i, i) for i in range(3)]
            else:
                ys = [(7 + 4 * ny + i, i) for i in range(4)]
            for nx in (-1, 0, 1):
                mid = own[...] if (nx, ny) == (0, 0) else tr[D44.index((nx, ny, 0))]
                low, high = tr[D44.index((nx, ny, -1))], tr[D44.index((nx, ny, 1))]
                for colour in range(colours):
                    a = roll(mid, -16 * colour, 1)
                    b = roll(high, 16 - 16 * colour, 1)
                    c = roll(low, 112 - 16 * colour, 1)
                    mixed = jnp.where(part < 16, a, jnp.where(part < 24, b, c))
                    for e, y in ys:
                        put(colour, e, 16 + 8 * nx, 8, roll(mixed, -32 * y, 1))

    ef2 = copies2(ft2, f2_r, s_all, r_f2, D26)
    ef2b = copies2(ft2, f2_r, s_all, r_f2b, D44[26:])
    ev2 = copies2(vt2, v2_r, s_all, r_v2, D44)
    acc = b2[0:8]
    for y in range(1, 4):
        acc = jnp.where(lane // 32 == y, b2[8 * y : 8 * y + 8], acc)
    ft2[...] = acc
    start(ef2)
    arrive(r_f2, units2)
    unpack2(ft2, f2_r, (-1, 0, 1), clean(lev2), 2)
    smooth_down(lev2)

    for y in range(2):
        s2[8 * y : 8 * y + 8, :] = residual(lev2, 7 + 2 * y) + residual(lev2, 8 + 2 * y)
    a3 = s2[pl.ds(0, 8, stride=2), :] + s2[pl.ds(1, 8, stride=2), :]
    a3 = jnp.where(lane < 16, 0.5 * a3, 0.0)
    a3 = pltpu.roll(a3, 0, 1, stride=16, stride_axis=0)
    a3 = jnp.sum(a3, axis=0, keepdims=True)
    t3[...] = jnp.where(row == iy, a3, 0.0)

    egy, egz, egx = [], [], []
    for k in (4, 3, 5, 2, 6, 1, 7):
        peer = (ix, lax.rem(iy + k, NGY), iz)
        egy.append(pltpu.make_async_remote_copy(t3, gy_r.at[k - 1], s_all, r_gy, peer, MESH))
    for k in (2, 1, 3):
        peer = (ix, iy, lax.rem(iz + k, NGZ))
        egz.append(pltpu.make_async_remote_copy(gzb.at[iz], gzb.at[iz], s_all, r_gz, peer, MESH))
    for k in (4, 3, 5, 2, 6, 1, 7):
        peer = (lax.rem(ix + k, NGX), iy, iz)
        egx.append(pltpu.make_async_remote_copy(gzb, gxb.at[ix], s_all, r_gx, peer, MESH))

    pl.semaphore_wait(tok4, 2)
    for c in egy:
        c.start()
    start(ef2b)
    acc = jnp.zeros((8, 128), F32)
    for y in range(4):
        acc = jnp.where(lane // 32 == y, roll(vb2[7 + y, 16:24, :], 32 * y, 1), acc)
    vt2[...] = acc
    for t in range(8):
        vk1[t] = jnp.where(lane < 64, vb1[6 + 2 * t, 16:24, :], roll(vb1[7 + 2 * t, 16:24, :], 64, 1))
    zpack1(lambda x: vb1[6 + x, 16:24, :], vz1)
    pack0(lambda x: vb0[4 + x, 8:24, :], vy0, vz0)
    for x in range(4):
        vx0[0, x] = vb0[4 + x, 8:24, :]
        vx0[1, x] = vb0[32 + x, 8:24, :]
    wait_units(r_gy, 7)
    line = t3[...]
    for k in range(NGY - 1):
        line = line + gy_r[k]
    gzb[iz] = line
    for c in egz:
        c.start()
    wait_units(r_gz, 3)
    for c in egx:
        c.start()
    start(ev2)
    start(ev1)
    start(ev0)
    gxb[ix] = gzb[...]
    arrive(r_f2b, units2b)
    unpack2(ft2, f2_r, (-2, 2), clean(lev2), 2)
    wait_units(r_gx, 28)

    for gx in range(NGX):
        for xl in range(4):
            acc = jnp.zeros((8, 128), F32)
            for gz in range(NGZ):
                acc = jnp.where((lane % 64) // 16 == gz, roll(gxb[gx, gz], (gz - xl) * 16, 1), acc)
            g3[4 * gx + xl] = acc

    zl = lane % 64
    w_lo = jnp.where(zl == 0, 0.0, BETA1)
    w_hi = jnp.where(zl == 63, 0.0, BETA1)
    y_edge = jnp.where(((row == 0) & (lane < 64)) | ((row == 7) & (lane >= 64)), 0.0, 1.0)
    par3 = (lane // 64 + lane) & 1
    colours3 = (par3 == 0, par3 == 1)

    def sum3(x):
        c = v3[x + 4]
        a = roll(c, 64, 1)
        w = jnp.where(lane < 64, roll(a, 1, 0), roll(a, -1, 0)) * y_edge
        s = (v3[x + 3] + v3[x + 5]) + (a + w)
        return c, s + (roll(c, 1, 1) * w_lo + roll(c, -1, 1) * w_hi)

    def half3(colour):
        for j in range(4):
            done = []
            for x in range(8 * j, 8 * j + 8):
                c, s = sum3(x)
                done.append(jnp.where(colours3[(x + colour) % 2], (g3[x] + s) * INV, c))
            for u in range(8):
                v3[8 * j + u + 4] = done[u]

    for x in range(32):
        v3[x + 4] = jnp.where(colours3[x % 2], g3[x] * INV, 0.0)
    half3(1)
    half3(0)
    half3(1)

    def small(g, level):
        n = len(g)
        dz, dy = 2 ** (level - 3), 2 ** (level - 4)
        lo = jnp.where(zl < dz, 0.0, BETA1)
        hi = jnp.where(zl >= 64 - dz, 0.0, BETA1)
        ylo = jnp.where(row < dy, 0.0, 1.0)
        yhi = jnp.where(row >= 8 - dy, 0.0, 1.0)
        par = (row // dy + zl // dz) & 1
        colours = (par == 0, par == 1)

        def beside(c, lo, hi, ylo, yhi):
            z = roll(c, dz, 1) * lo + roll(c, -dz, 1) * hi
            return z + (roll(c, dy, 0) * ylo + roll(c, -dy, 0) * yhi)

        def fixed(v, x):
            s = g[x]
            if x > 0:
                s = s + v[x - 1]
            if x < n - 1:
                s = s + v[x + 1]
            return s

        weights = [[jnp.where(c, w * INV, 0.0) for w in (lo, hi, ylo, yhi)] for c in colours]

        def sweep(v, colour):
            out = []
            for x in range(n):
                c = (x + colour) % 2
                base = jnp.where(colours[c], fixed(v, x) * INV, v[x])
                out.append(base + beside(v[x], *weights[c]))
            return out

        v = [jnp.where(colours[x % 2], g[x] * INV, 0.0) for x in range(n)]
        v = sweep(v, 1)
        if level == 6:
            for _ in range(CSWEEPS - 1):
                v = sweep(sweep(v, 0), 1)
            return v
        v = sweep(sweep(v, 0), 1)
        r = [(fixed(v, x) - CENTRE * v[x]) + beside(v[x], lo, hi, ylo, yhi) for x in range(n)]
        coarse = []
        for x in range(n // 2):
            t = r[2 * x] + r[2 * x + 1]
            t = t + jnp.where((row // dy) % 2 == 0, roll(t, -dy, 0), roll(t, dy, 0))
            t = t + jnp.where((zl // dz) % 2 == 0, roll(t, -dz, 1), roll(t, dz, 1))
            coarse.append(0.5 * t)
        e = small(coarse, level + 1)
        v = [v[x] + e[x // 2] for x in range(n)]
        for _ in range(2):
            v = sweep(sweep(v, 0), 1)
        return v

    def resid3(x):
        c, s = sum3(x)
        return g3[x] - (CENTRE * c - s)

    g4 = []
    for x in range(16):
        t = resid3(2 * x) + resid3(2 * x + 1)
        t = t + roll(t, 64, 1)
        t = t + jnp.where(lane % 2 == 0, roll(t, -1, 1), roll(t, 1, 1))
        g4.append(0.5 * t)
    e4 = small(g4, 4)
    for x in range(32):
        v3[4 + x] = v3[4 + x] + e4[x // 2]
    for _ in range(2):
        half3(0)
        half3(1)

    for x in range(12):
        e = v3[4 * ix + x]
        for yl in range(2):
            tmp2[yl, 16 + 8 * x : 24 + 8 * x, :] = pltpu.roll(e, (128 - 16 * iz + 64 * yl) % 128, 1)
    for j in range(10):
        e = tmp2[j % 2, pl.ds(16 + iy - 2 + j // 2, 12, stride=8), :]
        pe2[j, pl.ds(8, 12, stride=2), :] = e
        pe2[j, pl.ds(9, 12, stride=2), :] = e
    arrive(r_v2, lambda *c: units2(*c) + units2b(*c))
    add2 = corrected(lev2, lambda i, dst, num: pe2[(i + 1) // 2, dst : dst + num, :])
    unpack2(vt2, v2_r, (-2, -1, 0, 1, 2), add2, 1)
    half(lev2, 1, 17, True)
    half(lev2, 2, 16, False)
    half(lev2, 3, 15, True)
    half(lev2, 4, 14, False)

    def cells(level, i, a, b):
        even = level.even(i, a, b)
        r, k = level.vr[i, a:b, :], level.vb[i, a:b, :]
        first, second = jnp.where(even, r, k), roll(jnp.where(even, k, r), 64, 1)
        lanes = iota((b - a, 128), 1)
        if level is lev0:
            return jnp.where(lanes < 64, first, second)
        return jnp.where((lanes < 40) | (lanes >= 104), first, second)

    def merged(level, planes, a, b, matrix):
        rows = []
        for i in range(0, len(planes), 2):
            rows.append(jnp.concatenate([cells(level, j, a, b) for j in planes[i : i + 2]], axis=1))
        u = moved(jnp.concatenate(rows, axis=0), matrix)
        n = b - a
        return [u[n * (i // 2) : n * (i // 2) + n, 128 * (i % 2) : 128 * (i % 2) + 128] for i in range(len(planes))]

    for i, e in enumerate(merged(lev2, range(3, 15), 8, 32, from_pairs)):
        tmp1[24 * i : 24 * i + 24, :] = e
    for k in range(14):
        e = tmp1[pl.ds(5 + k, 12, stride=24), :]
        pe1[k, pl.ds(8, 12, stride=2), :] = e
        pe1[k, pl.ds(9, 12, stride=2), :] = e
    arrive(r_v1, units1)
    add1 = corrected(lev1, lambda i, dst, num: pe1[i // 2, dst : dst + num, :])
    unpack1(vk1, v1x_r, v1y_r, v1xy_r, v1z_r, add1, 1)
    half(lev1, 1, 27, True)
    half(lev1, 2, 26, False)
    half(lev1, 3, 25, True)
    half(lev1, 4, 24, False)

    for k, e in enumerate(merged(lev1, range(4, 24), 14, 30, from_pairs)):
        e = e[0:12]
        pe0[k, pl.ds(4, 12, stride=2), :] = e
        pe0[k, pl.ds(5, 12, stride=2), :] = e
    arrive(r_v0, units0)
    add0 = corrected(lev0, lambda i, dst, num: pe0[i // 2, dst : dst + num, :])
    unpack0(lambda x: vb0[4 + x, 8:24, :], vx_r, vy_r, vxy_r, vz_r, add0, 1)
    half(lev0, 1, 39, True)
    half(lev0, 2, 38, False)
    half(lev0, 3, 37, True)
    half(lev0, 4, 36, False, (8, 24))

    for part in range(4):
        planes = range(4 + 8 * part, 12 + 8 * part)
        for x, e in enumerate(merged(lev0, planes, 8, 24, to_cells)):
            out[8 * part + x] = e
    arrive(s_all, lambda *c: 2 * (units0(*c) + units1(*c) + units2(*c) + units2b(*c)) + 38)


def on_device(density):
    def vmem(*shape):
        return pltpu.VMEM(shape, F32)

    coef = vmem(2, 32, 128)
    level0 = [vmem(BX, BY, BZ)] * 2 + [vmem(40, 32, 128)] * 4 + [coef, vmem(16, 16, 128), vmem(20, 32, 128)]
    level1 = [vmem(28, 40, 128)] * 4 + [coef, vmem(64, 128), vmem(14, 32, 128), vmem(288, 128)]
    level2 = [vmem(18, 40, 128)] * 4 + [coef, vmem(16, 128), vmem(10, 32, 128), vmem(2, 128, 128)]
    packs = [vmem(2, 16, 8, 128), vmem(2, 16, 128)] * 2 + [vmem(2, 4, 16, 128)] + [vmem(8, 8, 128), vmem(2, 8, 128)] * 2
    packs += [vmem(8, 128)] * 2
    recv0 = [vmem(2, 4, 16, 128), vmem(2, 16, 8, 128), vmem(4, 2, 8, 128), vmem(18, 16, 128)] * 2
    recv1 = [vmem(2, 3, 8, 128), vmem(2, 8, 8, 128), vmem(4, 3, 8, 128), vmem(18, 8, 128)] * 2
    recv2 = [vmem(44, 8, 128)] * 2
    gather = [vmem(8, 128), vmem(7, 8, 128), vmem(4, 8, 128), vmem(8, 4, 8, 128), vmem(32, 8, 128), vmem(40, 8, 128)]
    dma = pltpu.SemaphoreType.DMA
    token = pltpu.SemaphoreType.REGULAR
    sems = [vmem(400, 8, 128), token, token] + [dma] * 12
    return pl.pallas_call(
        kernel,
        out_shape=jax.ShapeDtypeStruct((BX, BY, BZ), F32),
        in_specs=[pl.BlockSpec(memory_space=pltpu.HBM)],
        out_specs=pl.BlockSpec(memory_space=pltpu.VMEM),
        scratch_shapes=level0 + level1 + level2 + packs + recv0 + recv1 + recv2 + gather + sems,
        compiler_params=pltpu.CompilerParams(
            collective_id=0, has_side_effects=True, vmem_limit_bytes=48 * 1024 * 1024
        ),
    )(pltpu.with_memory_space_constraint(density, pltpu.HBM))


def solution(mesh):
    spec = P("gx", "gy", "gz")
    return jax.shard_map(on_device, mesh=mesh, in_specs=(spec,), out_specs=spec, check_vma=False)
```

```python
import itertools

import jax
import jax.numpy as jnp
from jax import lax
from jax.experimental import pallas as pl
from jax.experimental.pallas import tpu as pltpu
from jax.sharding import PartitionSpec as P

MESH = pl.DeviceIdType.MESH
F32 = jnp.float32
BF16 = jnp.bfloat16

NGX, NGY, NGZ = 8, 8, 4
BX, BY, BZ = 32, 16, 128
CSWEEPS = 4
BETA1 = 1.5
CENTRE = 4.0 + 2.0 * BETA1
INV = 1.0 / CENTRE

D26 = [d for d in itertools.product((-1, 0, 1), repeat=3) if d != (0, 0, 0)]
D26.sort(key=lambda d: -sum(map(abs, d)))
D44 = D26 + [d for d in itertools.product((-1, 0, 1), (-2, 2), (-1, 0, 1))]
XY4 = [(-1, -1), (-1, 1), (1, -1), (1, 1)]
Z18 = [d for d in D26 if d[2] != 0]


def roll(x, shift, axis):
    size = x.shape[axis]
    shift = shift % size
    return x if shift == 0 else pltpu.roll(x, shift, axis)


def iota(shape, dim):
    return lax.broadcasted_iota(jnp.int32, shape, dim)


def side(n):
    return 0 if n < 0 else 1


def neg(n):
    return (-n[0], -n[1], -n[2])


def moved(x, matrix):
    hi = x.astype(BF16)
    rest = x - hi.astype(F32)
    mid = rest.astype(BF16)
    lo = (rest - mid.astype(F32)).astype(BF16)
    return (
        jnp.dot(lo, matrix, preferred_element_type=F32)
        + jnp.dot(mid, matrix, preferred_element_type=F32)
        + jnp.dot(hi, matrix, preferred_element_type=F32)
    )


def kernel(
    f_hbm, out,
    f0, p0, fr0, fb0, vr0, vb0, rest0, k0, s0, pe0,
    fr1, fb1, vr1, vb1, rest1, k1, s1, pe1, tmp1,
    fr2, fb2, vr2, vb2, rest2, k2, s2, pe2, tmp2,
    fy0, fz0, vy0, vz0, vx0, fk1, fz1, vk1, vz1, ft2, vt2,
    fx_r, fy_r, fxy_r, fz_r, vx_r, vy_r, vxy_r, vz_r,
    f1x_r, f1y_r, f1xy_r, f1z_r, v1x_r, v1y_r, v1xy_r, v1z_r,
    f2_r, v2_r,
    t3, gy_r, gzb, gxb, g3, v3,
    spare, tok, tok4, io_sem, s_all, r_f0, r_v0, r_f1, r_v1, r_f2, r_f2b, r_v2, r_gy, r_gz, r_gx,
):
    ix, iy, iz = lax.axis_index("gx"), lax.axis_index("gy"), lax.axis_index("gz")

    def there(n):
        nx, ny, nz = ix + n[0], iy + n[1], iz + n[2]
        return (nx >= 0) & (nx < NGX) & (ny >= 0) & (ny < NGY) & (nz >= 0) & (nz < NGZ)

    def at(n):
        return (
            jnp.clip(ix + n[0], 0, NGX - 1),
            jnp.clip(iy + n[1], 0, NGY - 1),
            jnp.clip(iz + n[2], 0, NGZ - 1),
        )

    load = pltpu.make_async_copy(f_hbm, f0, io_sem)
    load.start()

    barrier = pltpu.get_barrier_semaphore()
    count = 0
    for d in D26:
        ok = there(d)
        count = count + ok.astype(jnp.int32)

        @pl.when(ok)
        def _(d=d):
            pl.semaphore_signal(barrier, inc=1, device_id=at(d), device_id_type=MESH)

    def token(sem, reach):
        for d in ((-reach, 0, 0), (reach, 0, 0), (0, -reach, 0), (0, reach, 0)):
            @pl.when(there(d))
            def _(d=d):
                pl.semaphore_signal(sem, inc=1, device_id=at(d), device_id_type=MESH)

    lane = iota((8, 128), 1)
    row = iota((8, 128), 0)
    lane16 = iota((16, 128), 1)
    r32, l32 = iota((32, 128), 0), iota((32, 128), 1)
    signed = jnp.where(l32 < 96, l32, l32 - 128)

    class Level:
        def __init__(self, fr, fb, vr, vb, rest, k, first, main, rows, window, odd, start, total):
            self.fr, self.fb, self.vr, self.vb, self.rest, self.k = fr, fb, vr, vb, rest, k
            self.first, self.main, self.rows, self.window = first, main, rows, window
            self.odd, self.start, self.total = odd, start, total
            self.planes = main + 2 * first

        def coefficient(self, i, lo, hi):
            if self.first <= i < self.first + self.main:
                return self.k[1, lo:hi, :]
            pos = self.start + i
            return self.k[jnp.where((pos >= 0) & (pos < self.total), 1, 0), lo:hi, :]

        def even(self, i, lo, hi):
            return (iota((hi - lo, 128), 0) + (lo + i + self.odd)) % 2 == 0

    lev0 = Level(fr0, fb0, vr0, vb0, rest0, k0, 4, BX, (8, 24), (4, 28), 0, ix * BX - 4, NGX * BX)
    lev1 = Level(fr1, fb1, vr1, vb1, rest1, k1, 6, 16, (16, 24), (8, 32), 0, ix * 16 - 6, NGX * 16)
    lev2 = Level(fr2, fb2, vr2, vb2, rest2, k2, 7, 4, (16, 24), (8, 32), 1, iy * 4 - 7, NGY * 4)

    def around(level, src, i, lo, hi, red):
        c0, c1 = src[i, lo:hi, :], src[i + 1, lo:hi, :]
        even = level.even(i, lo, hi)
        first, second = (c0, c1) if red else (c1, c0)
        up = roll(jnp.where(even, first, second), 1, 1)
        down = roll(jnp.where(even, second, first), -1, 1)
        z0, z1 = jnp.where(even, up, down), jnp.where(even, down, up)
        if not red:
            z0, z1 = z1, z0

        def plane(j, other, c, z):
            s = (other + src[j, lo - 1 : hi - 1, :]) + src[j, lo + 1 : hi + 1, :]
            return s + BETA1 * (c + z)

        return (
            plane(i, src[i - 1, lo:hi, :] + c1, c0, z0),
            plane(i + 1, c0 + src[i + 2, lo:hi, :], c1, z1),
        )

    def half(level, lo, hi, red, rows=None, keep=False):
        dst, src = (level.vr, level.vb) if red else (level.vb, level.vr)
        source = level.fr if red else level.fb
        a, b = rows or level.window
        for i in range(lo, hi, 2):
            for j, s in enumerate(around(level, src, i, a, b, red)):
                s = source[i + j, a:b, :] + s
                v = s * level.coefficient(i + j, a, b)
                dst[i + j, a:b, :] = v
                if keep and level.first <= i + j < level.first + level.main:
                    level.rest[i + j, a:b, :] = s - CENTRE * v

    def first_half(level, lo, hi):
        a, b = level.window
        for i in range(lo, hi):
            level.vr[i, a:b, :] = level.fr[i, a:b, :] * level.coefficient(i, a, b)

    def smooth_down(level):
        n, m = level.first, level.first + level.main
        first_half(level, n - 4, m + 4)
        half(level, n - 3, m + 3, False)
        half(level, n - 2, m + 2, True)
        half(level, n - 1, m + 1, False, keep=True)

    def residual(level, i):
        a, b = level.rows
        total = level.rest[i, a:b, :] + level.rest[i + 1, a:b, :]
        for j, s in enumerate(around(level, level.vb, i, a, b, True)):
            total = total + (level.fr[i + j, a:b, :] - (CENTRE * level.vr[i + j, a:b, :] - s))
        return total

    def split_rows(a, even):
        return jnp.concatenate([jnp.where(even, a, 0.0), jnp.where(even, 0.0, a)], axis=1)

    k256, c128 = iota((256, 128), 0), iota((256, 128), 1)
    z256 = k256 % 128
    red256 = (z256 + k256 // 128) % 2 == 0

    load.wait()

    kk2, cc2 = iota((256, 256), 0), iota((256, 256), 1)
    same = kk2 // 128 == cc2 // 128
    kk2, cc2 = kk2 % 128, cc2 % 128
    to_pairs = jnp.where(same & (cc2 == kk2 // 2 + 64 * (kk2 % 2)), 1.0, 0.0).astype(BF16)
    to_cells = jnp.where(same & (kk2 == cc2 // 2 + 64 * (cc2 % 2)), 1.0, 0.0).astype(BF16)
    for part in range(4):
        rows = []
        for x in range(8 * part, 8 * part + 8, 2):
            rows.append(jnp.concatenate([f0[x], f0[x + 1]], axis=1))
        p = moved(jnp.concatenate(rows, axis=0), to_pairs)
        for x in range(8):
            q = p[16 * (x // 2) : 16 * (x // 2) + 16, 128 * (x % 2) : 128 * (x % 2) + 128]
            p0[8 * part + x] = jnp.where((iota((16, 128), 0) + x) % 2 == 0, q, roll(q, 64, 1))

    def pack0(plane, yp, zp):
        lo = jnp.zeros((16, 128), F32)
        hi = jnp.zeros((16, 128), F32)
        slot = (lane16 % 64) // 2
        for x in range(BX):
            p = plane(x)
            half_tile = slice(4 * (x % 2), 4 * (x % 2) + 4)
            yp[0, x // 2, half_tile, :] = p[0:4]
            yp[1, x // 2, half_tile, :] = p[12:16]
            t = roll(p, 2 * x, 1)
            lo = jnp.where(slot == x, t, lo)
            hi = jnp.where(slot == (x - 1) % BX, t, hi)
        zp[0] = lo
        zp[1] = hi

    def copies0(xs, yp, zp, xr, yr, xyr, zr, ss, rs):
        out = []
        for d in D26:
            dx, dy, dz = d
            if dz == 0 and dy == 0:
                s, t = xs(dx), xr.at[side(-dx)]
            elif dz == 0 and dx == 0:
                s, t = yp.at[side(dy)], yr.at[side(-dy)]
            elif dz == 0:
                s = yp.at[side(dy), pl.ds(0 if dx < 0 else 14, 2)]
                t = xyr.at[XY4.index((-dx, -dy))]
            else:
                slot = Z18.index(neg(d))
                if dy == 0:
                    s, t = zp.at[side(dz)], zr.at[slot]
                else:
                    rows = pl.ds(0 if dy < 0 else 8, 8)
                    s, t = zp.at[side(dz), rows], zr.at[slot, rows]
            out.append((d, pltpu.make_async_remote_copy(s, t, ss, rs, at(d), MESH)))
        return out

    def start(copies):
        for d, c in copies:
            @pl.when(there(d))
            def _(c=c):
                c.start()

    near_x = jnp.where((ix > 0) & (ix < NGX - 1), 2, 1)
    near_z = jnp.where((iz > 0) & (iz < NGZ - 1), 2, 1)
    near_y = jnp.where((iy > 0) & (iy < NGY - 1), 2, 1)
    far_y = jnp.where((iy > 1) & (iy < NGY - 2), 2, 1)

    def units0(x, y, y2, z):
        return x * 8 + y * 16 + x * y * 2 + z * (2 + 2 * x + y + x * y)

    def units1(x, y, y2, z):
        return x * 3 + y * 8 + x * y * 3 + z * (1 + x) * (1 + y)

    def units2(x, y, y2, z):
        return (1 + x) * (1 + y) * (1 + z) - 1

    def units2b(x, y, y2, z):
        return (1 + x) * y2 * (1 + z)

    def wait_units(sem, n):
        pltpu.make_async_copy(spare.at[pl.ds(0, n)], spare.at[pl.ds(0, n)], sem).wait()

    def arrive(sem, units):
        for x, (y, y2), z in itertools.product((1, 2), ((1, 1), (2, 1), (2, 2)), (1, 2)):
            @pl.when((near_x == x) & (near_y == y) & (far_y == y2) & (near_z == z))
            def _(n=units(x, y, y2, z)):
                wait_units(sem, n)

    def unpack0(own, xr, yr, xyr, zr, put, colours):
        for nx in (-1, 0, 1):
            for ny, src, dst, num in ((-1, 8, 0, 8), (0, 0, 8, 16), (1, 0, 24, 8)):
                low = zr[Z18.index((nx, ny, -1)), src : src + num, :]
                high = zr[Z18.index((nx, ny, 1)), src : src + num, :]
                lanes = iota((num, 128), 1)
                xs = range(28, 32) if nx < 0 else (range(32) if nx == 0 else range(4))
                for x in xs:
                    if ny == 0:
                        p = own(x) if nx == 0 else xr[side(nx), x % 4]
                    else:
                        if nx == 0:
                            p = yr[side(ny), x // 2]
                        else:
                            p = xyr[XY4.index((nx, ny)), (x % 4) // 2]
                        if (x % 2 == 0) == (ny < 0):
                            p = roll(p, 4, 0)
                    e = roll(jnp.where((lanes % 64) // 2 == x, high, low), 64 - 2 * x, 1)
                    i = 32 * nx + x + 4
                    put(0, i, dst, num, jnp.where(lanes < 64, p, e))
                    if colours == 2:
                        put(1, i, dst, num, roll(jnp.where(lanes < 64, e, p), 64, 1))

    def clean(level):
        def put(colour, i, dst, num, value):
            ok = level.coefficient(i, dst, dst + num) > 0.0
            (level.fr if colour == 0 else level.fb)[i, dst : dst + num, :] = jnp.where(ok, value, 0.0)

        return put

    def corrected(level, add):
        def put(colour, i, dst, num, value):
            ok = level.coefficient(i, dst, dst + num) > 0.0
            level.vb[i, dst : dst + num, :] = jnp.where(ok, value + add(i, dst, num), 0.0)

        return put

    ef0 = copies0(
        lambda dx: p0.at[pl.ds(0 if dx < 0 else 28, 4)], fy0, fz0, fx_r, fy_r, fxy_r, fz_r, s_all, r_f0
    )
    ev0 = copies0(
        lambda dx: vx0.at[side(dx)],
        vy0, vz0, vx_r, vy_r, vxy_r, vz_r, s_all, r_v0,
    )

    pack0(lambda x: p0[x], fy0, fz0)
    pl.semaphore_wait(barrier, count)
    start(ef0)

    def fill(ref, halo, pairs, start_pairs, total_pairs, rows_at, total_rows):
        zp = start_pairs + signed
        ok = (signed >= -halo) & (signed < pairs + halo) & (zp >= 0) & (zp < total_pairs)
        ok = ok & (rows_at >= 0) & (rows_at < total_rows)
        ref[0] = jnp.zeros((32, 128), F32)
        ref[1] = jnp.where(ok, INV, 0.0)

    fill(k0, 2, 64, iz * 64, NGZ * 64, iy * BY + r32 - 8, NGY * BY)
    fill(k1, 3, 32, iz * 32, NGZ * 32, iy * 8 + r32 - 16, NGY * 8)
    fill(k2, 4, 16, iz * 16, NGZ * 16, ix * 8 + r32 - 16, NGX * 8)

    def zero(ref):
        @pl.loop(0, ref.shape[0])
        def _(i):
            ref[i] = jnp.zeros(ref.shape[1:], F32)

    for ref in (vr0, vb0, vr1, vb1, vr2, vb2, pe0, pe1, pe2, v3, tmp2):
        zero(ref)

    to_pairs1 = jnp.where(
        (z256 < 64) & (c128 % 32 == z256 // 2) & ((c128 < 64) == red256), 0.5, 0.0
    ).astype(BF16)
    to_pairs2 = jnp.where(
        (z256 < 32) & (c128 % 32 == z256 // 2 + jnp.where(red256, 0, 16)), 0.5, 0.0
    ).astype(BF16)
    csign = jnp.where(cc2 < 96, cc2, cc2 - 128)
    wanted = ((csign + 128) // 2 - 64 + 64 * (csign % 2)) % 128
    from_pairs = jnp.where(same & (kk2 == wanted) & (csign >= -4) & (csign < 68), 1.0, 0.0).astype(BF16)

    arrive(r_f0, units0)
    token(tok, 2)
    unpack0(lambda x: p0[x], fx_r, fy_r, fxy_r, fz_r, clean(lev0), 2)
    smooth_down(lev0)
    for x in range(16):
        s0[x] = residual(lev0, 4 + 2 * x)

    rows = []
    for x in range(16):
        a = s0[x, pl.ds(0, 8, stride=2), :] + s0[x, pl.ds(1, 8, stride=2), :]
        rows.append(split_rows(a, (row + x) % 2 == 0))
    b1 = moved(jnp.concatenate(rows, axis=0), to_pairs1)

    def zpack1(plane, zp):
        lo = jnp.zeros((8, 128), F32)
        hi = jnp.zeros((8, 128), F32)
        for x in range(16):
            p = plane(x)
            lo = jnp.where((lane % 64) // 3 == x, roll(p, 3 * x, 1), lo)
            hi = jnp.where(((lane + 35) % 64) // 3 == x, roll(p, 3 * x + 64, 1), hi)
        zp[0] = lo
        zp[1] = hi

    def copies1(pk, zp, xr, yr, xyr, zr, ss, rs):
        out = []
        for d in D26:
            dx, dy, dz = d
            if dz == 0 and dx == 0:
                s, t = pk, yr.at[side(-dy)]
            elif dz == 0:
                s = pk.at[pl.ds(0 if dx < 0 else 5, 3)]
                t = xr.at[side(-dx)] if dy == 0 else xyr.at[XY4.index((-dx, -dy))]
            else:
                s, t = zp.at[side(dz)], zr.at[Z18.index(neg(d))]
            out.append((d, pltpu.make_async_remote_copy(s, t, ss, rs, at(d), MESH)))
        return out

    def unpack1(pk, xr, yr, xyr, zr, put, colours):
        for xe in range(28):
            nx, x = (-1, 10 + xe) if xe < 6 else ((0, xe - 6) if xe < 22 else (1, xe - 22))
            for ny in (-1, 0, 1):
                if nx == 0:
                    mid = pk[x // 2] if ny == 0 else yr[side(ny), x // 2]
                else:
                    tile = x // 2 - 5 if nx < 0 else x // 2
                    mid = xr[side(nx), tile] if ny == 0 else xyr[XY4.index((nx, ny)), tile]
                low, high = zr[Z18.index((nx, ny, -1))], zr[Z18.index((nx, ny, 1))]
                at_x = 32 * (x % 2)
                e = roll(jnp.where((lane % 64) // 3 == x, high, low), at_x + 32 - 3 * x, 1)
                for colour in range(colours):
                    first = at_x + 64 * colour
                    value = jnp.where((lane >= first) & (lane < first + 32), mid, e)
                    put(colour, xe, 16 + 8 * ny, 8, roll(value, -first, 1))

    ef1 = copies1(fk1, fz1, f1x_r, f1y_r, f1xy_r, f1z_r, s_all, r_f1)
    ev1 = copies1(vk1, vz1, v1x_r, v1y_r, v1xy_r, v1z_r, s_all, r_v1)
    for t in range(8):
        fk1[t] = jnp.where(lane % 64 < 32, b1[16 * t : 16 * t + 8], b1[16 * t + 8 : 16 * t + 16])
    zpack1(lambda x: b1[8 * x : 8 * x + 8], fz1)
    start(ef1)
    arrive(r_f1, units1)
    pl.semaphore_wait(tok, jnp.where((ix > 1) & (ix < NGX - 2), 2, 1) + far_y)
    token(tok4, 4)
    unpack1(fk1, f1x_r, f1y_r, f1xy_r, f1z_r, clean(lev1), 2)
    smooth_down(lev1)
    for x in range(8):
        s1[8 * x : 8 * x + 8, :] = residual(lev1, 6 + 2 * x)

    rows = []
    for y in range(4):
        a = s1[pl.ds(2 * y, 8, stride=8), :] + s1[pl.ds(2 * y + 1, 8, stride=8), :]
        rows.append(split_rows(a, (row + y) % 2 == 0))
    b2 = moved(jnp.concatenate(rows, axis=0), to_pairs2)

    def copies2(t, tr, ss, rs, directions):
        out = []
        for d in directions:
            dst = tr.at[D44.index(neg(d))]
            out.append((d, pltpu.make_async_remote_copy(t, dst, ss, rs, at(d), MESH)))
        return out

    def unpack2(own, tr, which, put, colours):
        part = lane % 32
        for ny in which:
            if ny == -2:
                ys = [(i, 1 + i) for i in range(3)]
            elif ny == 2:
                ys = [(15 + i, i) for i in range(3)]
            else:
                ys = [(7 + 4 * ny + i, i) for i in range(4)]
            for nx in (-1, 0, 1):
                mid = own[...] if (nx, ny) == (0, 0) else tr[D44.index((nx, ny, 0))]
                low, high = tr[D44.index((nx, ny, -1))], tr[D44.index((nx, ny, 1))]
                for colour in range(colours):
                    a = roll(mid, -16 * colour, 1)
                    b = roll(high, 16 - 16 * colour, 1)
                    c = roll(low, 112 - 16 * colour, 1)
                    mixed = jnp.where(part < 16, a, jnp.where(part < 24, b, c))
                    for e, y in ys:
                        put(colour, e, 16 + 8 * nx, 8, roll(mixed, -32 * y, 1))

    ef2 = copies2(ft2, f2_r, s_all, r_f2, D26)
    ef2b = copies2(ft2, f2_r, s_all, r_f2b, D44[26:])
    ev2 = copies2(vt2, v2_r, s_all, r_v2, D44)
    acc = b2[0:8]
    for y in range(1, 4):
        acc = jnp.where(lane // 32 == y, b2[8 * y : 8 * y + 8], acc)
    ft2[...] = acc
    start(ef2)
    arrive(r_f2, units2)
    unpack2(ft2, f2_r, (-1, 0, 1), clean(lev2), 2)
    smooth_down(lev2)

    for y in range(2):
        s2[8 * y : 8 * y + 8, :] = residual(lev2, 7 + 2 * y)
    a3 = s2[pl.ds(0, 8, stride=2), :] + s2[pl.ds(1, 8, stride=2), :]
    a3 = jnp.where(lane < 16, 0.5 * a3, 0.0)
    a3 = pltpu.roll(a3, 0, 1, stride=16, stride_axis=0)
    a3 = jnp.sum(a3, axis=0, keepdims=True)
    t3[...] = jnp.where(row == iy, a3, 0.0)

    egy, egz, egx = [], [], []
    for k in (4, 3, 5, 2, 6, 1, 7):
        peer = (ix, lax.rem(iy + k, NGY), iz)
        egy.append(pltpu.make_async_remote_copy(t3, gy_r.at[k - 1], s_all, r_gy, peer, MESH))
    for k in (2, 1, 3):
        peer = (ix, iy, lax.rem(iz + k, NGZ))
        egz.append(pltpu.make_async_remote_copy(gzb.at[iz], gzb.at[iz], s_all, r_gz, peer, MESH))
    for k in (4, 3, 5, 2, 6, 1, 7):
        peer = (lax.rem(ix + k, NGX), iy, iz)
        egx.append(pltpu.make_async_remote_copy(gzb, gxb.at[ix], s_all, r_gx, peer, MESH))

    pl.semaphore_wait(tok4, 2)
    for c in egy:
        c.start()
    start(ef2b)
    acc = jnp.zeros((8, 128), F32)
    for y in range(4):
        acc = jnp.where(lane // 32 == y, roll(vb2[7 + y, 16:24, :], 32 * y, 1), acc)
    vt2[...] = acc
    for t in range(8):
        vk1[t] = jnp.where(lane % 64 < 32, vb1[6 + 2 * t, 16:24, :], roll(vb1[7 + 2 * t, 16:24, :], 32, 1))
    zpack1(lambda x: vb1[6 + x, 16:24, :], vz1)
    pack0(lambda x: vb0[4 + x, 8:24, :], vy0, vz0)
    for x in range(4):
        vx0[0, x] = vb0[4 + x, 8:24, :]
        vx0[1, x] = vb0[32 + x, 8:24, :]
    wait_units(r_gy, 7)
    line = t3[...]
    for k in range(NGY - 1):
        line = line + gy_r[k]
    gzb[iz] = line
    for c in egz:
        c.start()
    wait_units(r_gz, 3)
    for c in egx:
        c.start()
    start(ev2)
    start(ev1)
    start(ev0)
    gxb[ix] = gzb[...]
    arrive(r_f2b, units2b)
    unpack2(ft2, f2_r, (-2, 2), clean(lev2), 2)
    wait_units(r_gx, 28)

    for gx in range(NGX):
        for xl in range(4):
            acc = jnp.zeros((8, 128), F32)
            for gz in range(NGZ):
                acc = jnp.where((lane % 64) // 16 == gz, roll(gxb[gx, gz], (gz - xl) * 16, 1), acc)
            g3[4 * gx + xl] = acc

    zl = lane % 64
    w_lo = jnp.where(zl == 0, 0.0, BETA1)
    w_hi = jnp.where(zl == 63, 0.0, BETA1)
    y_edge = jnp.where(((row == 0) & (lane < 64)) | ((row == 7) & (lane >= 64)), 0.0, 1.0)
    par3 = (lane // 64 + lane) & 1
    colours3 = (par3 == 0, par3 == 1)

    def sum3(x):
        c = v3[x + 4]
        a = roll(c, 64, 1)
        w = jnp.where(lane < 64, roll(a, 1, 0), roll(a, -1, 0)) * y_edge
        s = (v3[x + 3] + v3[x + 5]) + (a + w)
        return c, s + (roll(c, 1, 1) * w_lo + roll(c, -1, 1) * w_hi)

    def half3(colour):
        for j in range(4):
            done = []
            for x in range(8 * j, 8 * j + 8):
                c, s = sum3(x)
                done.append(jnp.where(colours3[(x + colour) % 2], (g3[x] + s) * INV, c))
            for u in range(8):
                v3[8 * j + u + 4] = done[u]

    for x in range(32):
        v3[x + 4] = jnp.where(colours3[x % 2], g3[x] * INV, 0.0)
    half3(1)
    half3(0)
    half3(1)

    def small(g, level):
        n = len(g)
        dz, dy = 2 ** (level - 3), 2 ** (level - 4)
        lo = jnp.where(zl < dz, 0.0, BETA1)
        hi = jnp.where(zl >= 64 - dz, 0.0, BETA1)
        ylo = jnp.where(row < dy, 0.0, 1.0)
        yhi = jnp.where(row >= 8 - dy, 0.0, 1.0)
        par = (row // dy + zl // dz) & 1
        colours = (par == 0, par == 1)

        def beside(c, lo, hi, ylo, yhi):
            z = roll(c, dz, 1) * lo + roll(c, -dz, 1) * hi
            return z + (roll(c, dy, 0) * ylo + roll(c, -dy, 0) * yhi)

        def fixed(v, x):
            s = g[x]
            if x > 0:
                s = s + v[x - 1]
            if x < n - 1:
                s = s + v[x + 1]
            return s

        weights = [[jnp.where(c, w * INV, 0.0) for w in (lo, hi, ylo, yhi)] for c in colours]

        def sweep(v, colour):
            out = []
            for x in range(n):
                c = (x + colour) % 2
                base = jnp.where(colours[c], fixed(v, x) * INV, v[x])
                out.append(base + beside(v[x], *weights[c]))
            return out

        v = [jnp.where(colours[x % 2], g[x] * INV, 0.0) for x in range(n)]
        v = sweep(v, 1)
        if level == 6:
            for _ in range(CSWEEPS - 1):
                v = sweep(sweep(v, 0), 1)
            return v
        v = sweep(sweep(v, 0), 1)
        r = [(fixed(v, x) - CENTRE * v[x]) + beside(v[x], lo, hi, ylo, yhi) for x in range(n)]
        coarse = []
        for x in range(n // 2):
            t = r[2 * x] + r[2 * x + 1]
            t = t + jnp.where((row // dy) % 2 == 0, roll(t, -dy, 0), roll(t, dy, 0))
            t = t + jnp.where((zl // dz) % 2 == 0, roll(t, -dz, 1), roll(t, dz, 1))
            coarse.append(0.5 * t)
        e = small(coarse, level + 1)
        v = [v[x] + e[x // 2] for x in range(n)]
        for _ in range(2):
            v = sweep(sweep(v, 0), 1)
        return v

    def resid3(x):
        c, s = sum3(x)
        return g3[x] - (CENTRE * c - s)

    g4 = []
    for x in range(16):
        t = resid3(2 * x) + resid3(2 * x + 1)
        t = t + roll(t, 64, 1)
        t = t + jnp.where(lane % 2 == 0, roll(t, -1, 1), roll(t, 1, 1))
        g4.append(0.5 * t)
    e4 = small(g4, 4)
    for x in range(32):
        v3[4 + x] = v3[4 + x] + e4[x // 2]
    for _ in range(2):
        half3(0)
        half3(1)

    for x in range(12):
        e = v3[4 * ix + x]
        for yl in range(2):
            tmp2[yl, 16 + 8 * x : 24 + 8 * x, :] = pltpu.roll(e, (128 - 16 * iz + 64 * yl) % 128, 1)
    for j in range(10):
        e = tmp2[j % 2, pl.ds(16 + iy - 2 + j // 2, 12, stride=8), :]
        pe2[j, pl.ds(8, 12, stride=2), :] = e
        pe2[j, pl.ds(9, 12, stride=2), :] = e
    arrive(r_v2, lambda *c: units2(*c) + units2b(*c))
    add2 = corrected(lev2, lambda i, dst, num: pe2[(i + 1) // 2, dst : dst + num, :])
    unpack2(vt2, v2_r, (-2, -1, 0, 1, 2), add2, 1)
    half(lev2, 1, 17, True)
    half(lev2, 2, 16, False)
    half(lev2, 3, 15, True)
    half(lev2, 4, 14, False)

    def cells(level, i, a, b):
        even = level.even(i, a, b)
        r, k = level.vr[i, a:b, :], level.vb[i, a:b, :]
        first, second = jnp.where(even, r, k), roll(jnp.where(even, k, r), 64, 1)
        lanes = iota((b - a, 128), 1)
        if level is lev0:
            return jnp.where(lanes < 64, first, second)
        return jnp.where((lanes < 40) | (lanes >= 104), first, second)

    def merged(level, planes, a, b, matrix):
        rows = []
        for i in range(0, len(planes), 2):
            rows.append(jnp.concatenate([cells(level, j, a, b) for j in planes[i : i + 2]], axis=1))
        u = moved(jnp.concatenate(rows, axis=0), matrix)
        n = b - a
        return [u[n * (i // 2) : n * (i // 2) + n, 128 * (i % 2) : 128 * (i % 2) + 128] for i in range(len(planes))]

    for i, e in enumerate(merged(lev2, range(3, 15), 8, 32, from_pairs)):
        tmp1[24 * i : 24 * i + 24, :] = e
    for k in range(14):
        e = tmp1[pl.ds(5 + k, 12, stride=24), :]
        pe1[k, pl.ds(8, 12, stride=2), :] = e
        pe1[k, pl.ds(9, 12, stride=2), :] = e
    arrive(r_v1, units1)
    add1 = corrected(lev1, lambda i, dst, num: pe1[i // 2, dst : dst + num, :])
    unpack1(vk1, v1x_r, v1y_r, v1xy_r, v1z_r, add1, 1)
    half(lev1, 1, 27, True)
    half(lev1, 2, 26, False)
    half(lev1, 3, 25, True)
    half(lev1, 4, 24, False)

    for k, e in enumerate(merged(lev1, range(4, 24), 14, 30, from_pairs)):
        e = e[0:12]
        pe0[k, pl.ds(4, 12, stride=2), :] = e
        pe0[k, pl.ds(5, 12, stride=2), :] = e
    arrive(r_v0, units0)
    add0 = corrected(lev0, lambda i, dst, num: pe0[i // 2, dst : dst + num, :])
    unpack0(lambda x: vb0[4 + x, 8:24, :], vx_r, vy_r, vxy_r, vz_r, add0, 1)
    half(lev0, 1, 39, True)
    half(lev0, 2, 38, False)
    half(lev0, 3, 37, True)
    half(lev0, 4, 36, False, (8, 24))

    for part in range(4):
        planes = range(4 + 8 * part, 12 + 8 * part)
        for x, e in enumerate(merged(lev0, planes, 8, 24, to_cells)):
            out[8 * part + x] = e
    arrive(s_all, lambda *c: 2 * (units0(*c) + units1(*c) + units2(*c) + units2b(*c)) + 38)


def on_device(density):
    def vmem(*shape):
        return pltpu.VMEM(shape, F32)

    coef = vmem(2, 32, 128)
    level0 = [vmem(BX, BY, BZ)] * 2 + [vmem(40, 32, 128)] * 5 + [coef, vmem(16, 16, 128), vmem(20, 32, 128)]
    level1 = [vmem(28, 40, 128)] * 5 + [coef, vmem(64, 128), vmem(14, 32, 128), vmem(288, 128)]
    level2 = [vmem(18, 40, 128)] * 5 + [coef, vmem(16, 128), vmem(10, 32, 128), vmem(2, 128, 128)]
    packs = [vmem(2, 16, 8, 128), vmem(2, 16, 128)] * 2 + [vmem(2, 4, 16, 128)] + [vmem(8, 8, 128), vmem(2, 8, 128)] * 2
    packs += [vmem(8, 128)] * 2
    recv0 = [vmem(2, 4, 16, 128), vmem(2, 16, 8, 128), vmem(4, 2, 8, 128), vmem(18, 16, 128)] * 2
    recv1 = [vmem(2, 3, 8, 128), vmem(2, 8, 8, 128), vmem(4, 3, 8, 128), vmem(18, 8, 128)] * 2
    recv2 = [vmem(44, 8, 128)] * 2
    gather = [vmem(8, 128), vmem(7, 8, 128), vmem(4, 8, 128), vmem(8, 4, 8, 128), vmem(32, 8, 128), vmem(40, 8, 128)]
    dma = pltpu.SemaphoreType.DMA
    token = pltpu.SemaphoreType.REGULAR
    sems = [vmem(400, 8, 128), token, token] + [dma] * 12
    return pl.pallas_call(
        kernel,
        out_shape=jax.ShapeDtypeStruct((BX, BY, BZ), F32),
        in_specs=[pl.BlockSpec(memory_space=pltpu.HBM)],
        out_specs=pl.BlockSpec(memory_space=pltpu.VMEM),
        scratch_shapes=level0 + level1 + level2 + packs + recv0 + recv1 + recv2 + gather + sems,
        compiler_params=pltpu.CompilerParams(
            collective_id=0, has_side_effects=True, vmem_limit_bytes=48 * 1024 * 1024
        ),
    )(pltpu.with_memory_space_constraint(density, pltpu.HBM))


def solution(mesh):
    spec = P("gx", "gy", "gz")
    return jax.shard_map(on_device, mesh=mesh, in_specs=(spec,), out_specs=spec, check_vma=False)
```

```python
import itertools

import jax
import jax.numpy as jnp
from jax import lax
from jax.experimental import pallas as pl
from jax.experimental.pallas import tpu as pltpu
from jax.sharding import PartitionSpec as P

MESH = pl.DeviceIdType.MESH
F32 = jnp.float32
BF16 = jnp.bfloat16

NGX, NGY, NGZ = 8, 8, 4
BX, BY, BZ = 32, 16, 128
CSWEEPS = 4
BETA1 = 1.5
CENTRE = 4.0 + 2.0 * BETA1
INV = 1.0 / CENTRE

D26 = [d for d in itertools.product((-1, 0, 1), repeat=3) if d != (0, 0, 0)]
D26.sort(key=lambda d: -sum(map(abs, d)))
D44 = D26 + [d for d in itertools.product((-1, 0, 1), (-2, 2), (-1, 0, 1))]
XY4 = [(-1, -1), (-1, 1), (1, -1), (1, 1)]
Z18 = [d for d in D26 if d[2] != 0]


def roll(x, shift, axis):
    size = x.shape[axis]
    shift = shift % size
    return x if shift == 0 else pltpu.roll(x, shift, axis)


def iota(shape, dim):
    return lax.broadcasted_iota(jnp.int32, shape, dim)


def side(n):
    return 0 if n < 0 else 1


def neg(n):
    return (-n[0], -n[1], -n[2])


def moved(x, matrix):
    hi = x.astype(BF16)
    rest = x - hi.astype(F32)
    mid = rest.astype(BF16)
    lo = (rest - mid.astype(F32)).astype(BF16)
    return (
        jnp.dot(lo, matrix, preferred_element_type=F32)
        + jnp.dot(mid, matrix, preferred_element_type=F32)
        + jnp.dot(hi, matrix, preferred_element_type=F32)
    )


def kernel(
    f_hbm, out,
    f0, p0, turned, fr0, fb0, vr0, vb0, rest0, k0, s0, pe0,
    fr1, fb1, vr1, vb1, rest1, k1, s1, pe1, tmp1,
    fr2, fb2, vr2, vb2, rest2, k2, s2, pe2, tmp2,
    fy0, fz0, vy0, vz0, vx0, fk1, fz1, vk1, vz1, ft2, vt2,
    fx_r, fy_r, fxy_r, fz_r, vx_r, vy_r, vxy_r, vz_r,
    f1x_r, f1y_r, f1xy_r, f1z_r, v1x_r, v1y_r, v1xy_r, v1z_r,
    f2_r, v2_r,
    t3, gy_r, gzb, gxb, g3, v3,
    spare, tok, tok4, io_sem, s_all, r_f0, r_v0, r_f1, r_v1, r_f2, r_f2b, r_v2, r_gy, r_gz, r_gx,
):
    ix, iy, iz = lax.axis_index("gx"), lax.axis_index("gy"), lax.axis_index("gz")

    def there(n):
        nx, ny, nz = ix + n[0], iy + n[1], iz + n[2]
        return (nx >= 0) & (nx < NGX) & (ny >= 0) & (ny < NGY) & (nz >= 0) & (nz < NGZ)

    def at(n):
        return (
            jnp.clip(ix + n[0], 0, NGX - 1),
            jnp.clip(iy + n[1], 0, NGY - 1),
            jnp.clip(iz + n[2], 0, NGZ - 1),
        )

    load = pltpu.make_async_copy(f_hbm, f0, io_sem)
    load.start()

    barrier = pltpu.get_barrier_semaphore()
    count = 0
    for d in D26:
        ok = there(d)
        count = count + ok.astype(jnp.int32)

        @pl.when(ok)
        def _(d=d):
            pl.semaphore_signal(barrier, inc=1, device_id=at(d), device_id_type=MESH)

    def token(sem, reach):
        for d in ((-reach, 0, 0), (reach, 0, 0), (0, -reach, 0), (0, reach, 0)):
            @pl.when(there(d))
            def _(d=d):
                pl.semaphore_signal(sem, inc=1, device_id=at(d), device_id_type=MESH)

    lane = iota((8, 128), 1)
    row = iota((8, 128), 0)
    lane16 = iota((16, 128), 1)
    r32, l32 = iota((32, 128), 0), iota((32, 128), 1)
    signed = jnp.where(l32 < 96, l32, l32 - 128)

    class Level:
        def __init__(self, fr, fb, vr, vb, rest, k, first, main, rows, window, odd, start, total):
            self.fr, self.fb, self.vr, self.vb, self.rest, self.k = fr, fb, vr, vb, rest, k
            self.first, self.main, self.rows, self.window = first, main, rows, window
            self.odd, self.start, self.total = odd, start, total
            self.planes = main + 2 * first

        def coefficient(self, i, lo, hi):
            if self.first <= i < self.first + self.main:
                return self.k[1, lo:hi, :]
            pos = self.start + i
            return self.k[jnp.where((pos >= 0) & (pos < self.total), 1, 0), lo:hi, :]

        def even(self, i, lo, hi):
            return (iota((hi - lo, 128), 0) + (lo + i + self.odd)) % 2 == 0

    lev0 = Level(fr0, fb0, vr0, vb0, rest0, k0, 4, BX, (8, 24), (4, 28), 0, ix * BX - 4, NGX * BX)
    lev1 = Level(fr1, fb1, vr1, vb1, rest1, k1, 6, 16, (16, 24), (8, 32), 0, ix * 16 - 6, NGX * 16)
    lev2 = Level(fr2, fb2, vr2, vb2, rest2, k2, 7, 4, (16, 24), (8, 32), 1, iy * 4 - 7, NGY * 4)

    def around(level, src, i, lo, hi, red):
        c0, c1 = src[i, lo:hi, :], src[i + 1, lo:hi, :]
        even = level.even(i, lo, hi)
        first, second = (c0, c1) if red else (c1, c0)
        up = roll(jnp.where(even, first, second), 1, 1)
        down = roll(jnp.where(even, second, first), -1, 1)
        z0, z1 = jnp.where(even, up, down), jnp.where(even, down, up)
        if not red:
            z0, z1 = z1, z0

        def plane(j, other, c, z):
            s = (other + src[j, lo - 1 : hi - 1, :]) + src[j, lo + 1 : hi + 1, :]
            return s + BETA1 * (c + z)

        return (
            plane(i, src[i - 1, lo:hi, :] + c1, c0, z0),
            plane(i + 1, c0 + src[i + 2, lo:hi, :], c1, z1),
        )

    def half(level, lo, hi, red, rows=None, keep=False):
        dst, src = (level.vr, level.vb) if red else (level.vb, level.vr)
        source = level.fr if red else level.fb
        a, b = rows or level.window
        for i in range(lo, hi, 2):
            for j, s in enumerate(around(level, src, i, a, b, red)):
                s = source[i + j, a:b, :] + s
                v = s * level.coefficient(i + j, a, b)
                dst[i + j, a:b, :] = v
                if keep and level.first <= i + j < level.first + level.main:
                    level.rest[i + j, a:b, :] = s - CENTRE * v

    def first_half(level, lo, hi):
        a, b = level.window
        for i in range(lo, hi):
            level.vr[i, a:b, :] = level.fr[i, a:b, :] * level.coefficient(i, a, b)

    def smooth_down(level):
        n, m = level.first, level.first + level.main
        first_half(level, n - 4, m + 4)
        half(level, n - 3, m + 3, False)
        half(level, n - 2, m + 2, True)
        half(level, n - 1, m + 1, False, keep=True)

    def residual(level, i):
        a, b = level.rows
        total = level.rest[i, a:b, :] + level.rest[i + 1, a:b, :]
        for j, s in enumerate(around(level, level.vb, i, a, b, True)):
            total = total + (level.fr[i + j, a:b, :] - (CENTRE * level.vr[i + j, a:b, :] - s))
        return total

    def split_rows(a, even):
        return jnp.concatenate([jnp.where(even, a, 0.0), jnp.where(even, 0.0, a)], axis=1)

    k256, c128 = iota((256, 128), 0), iota((256, 128), 1)
    z256 = k256 % 128
    red256 = (z256 + k256 // 128) % 2 == 0

    load.wait()

    kk2, cc2 = iota((256, 256), 0), iota((256, 256), 1)
    same = kk2 // 128 == cc2 // 128
    kk2, cc2 = kk2 % 128, cc2 % 128
    to_pairs = jnp.where(same & (cc2 == kk2 // 2 + 64 * (kk2 % 2)), 1.0, 0.0).astype(BF16)
    to_cells = jnp.where(same & (kk2 == cc2 // 2 + 64 * (cc2 % 2)), 1.0, 0.0).astype(BF16)
    for part in range(4):
        rows = []
        for x in range(8 * part, 8 * part + 8, 2):
            rows.append(jnp.concatenate([f0[x], f0[x + 1]], axis=1))
        p = moved(jnp.concatenate(rows, axis=0), to_pairs)
        for x in range(8):
            q = p[16 * (x // 2) : 16 * (x // 2) + 16, 128 * (x % 2) : 128 * (x % 2) + 128]
            p0[8 * part + x] = jnp.where((iota((16, 128), 0) + x) % 2 == 0, q, roll(q, 64, 1))

    def pack0(plane, yp, zp):
        lo = jnp.zeros((16, 128), F32)
        hi = jnp.zeros((16, 128), F32)
        slot = (lane16 % 64) // 2
        for x in range(BX):
            p = plane(x)
            half_tile = slice(4 * (x % 2), 4 * (x % 2) + 4)
            yp[0, x // 2, half_tile, :] = p[0:4]
            yp[1, x // 2, half_tile, :] = p[12:16]
            t = roll(p, 2 * x, 1)
            lo = jnp.where(slot == x, t, lo)
            hi = jnp.where(slot == (x - 1) % BX, t, hi)
        zp[0] = lo
        zp[1] = hi

    def copies0(xs, yp, zp, xr, yr, xyr, zr, ss, rs):
        out = []
        for d in D26:
            dx, dy, dz = d
            if dz == 0 and dy == 0:
                s, t = xs(dx), xr.at[side(-dx)]
            elif dz == 0 and dx == 0:
                s, t = yp.at[side(dy)], yr.at[side(-dy)]
            elif dz == 0:
                s = yp.at[side(dy), pl.ds(0 if dx < 0 else 14, 2)]
                t = xyr.at[XY4.index((-dx, -dy))]
            else:
                slot = Z18.index(neg(d))
                if dy == 0:
                    s, t = zp.at[side(dz)], zr.at[slot]
                else:
                    rows = pl.ds(0 if dy < 0 else 8, 8)
                    s, t = zp.at[side(dz), rows], zr.at[slot, rows]
            out.append((d, pltpu.make_async_remote_copy(s, t, ss, rs, at(d), MESH)))
        return out

    def start(copies):
        for d, c in copies:
            @pl.when(there(d))
            def _(c=c):
                c.start()

    near_x = jnp.where((ix > 0) & (ix < NGX - 1), 2, 1)
    near_z = jnp.where((iz > 0) & (iz < NGZ - 1), 2, 1)
    near_y = jnp.where((iy > 0) & (iy < NGY - 1), 2, 1)
    far_y = jnp.where((iy > 1) & (iy < NGY - 2), 2, 1)

    def units0(x, y, y2, z):
        return x * 8 + y * 16 + x * y * 2 + z * (2 + 2 * x + y + x * y)

    def units1(x, y, y2, z):
        return x * 3 + y * 8 + x * y * 3 + z * (1 + x) * (1 + y)

    def units2(x, y, y2, z):
        return (1 + x) * (1 + y) * (1 + z) - 1

    def units2b(x, y, y2, z):
        return (1 + x) * y2 * (1 + z)

    def wait_units(sem, n):
        pltpu.make_async_copy(spare.at[pl.ds(0, n)], spare.at[pl.ds(0, n)], sem).wait()

    def arrive(sem, units):
        for x, (y, y2), z in itertools.product((1, 2), ((1, 1), (2, 1), (2, 2)), (1, 2)):
            @pl.when((near_x == x) & (near_y == y) & (far_y == y2) & (near_z == z))
            def _(n=units(x, y, y2, z)):
                wait_units(sem, n)

    def unpack0(own, xr, yr, xyr, zr, put, colours):
        for nx in (-1, 0, 1):
            for ny, src, dst, num in ((-1, 8, 0, 8), (0, 0, 8, 16), (1, 0, 24, 8)):
                low = zr[Z18.index((nx, ny, -1)), src : src + num, :]
                high = zr[Z18.index((nx, ny, 1)), src : src + num, :]
                lanes = iota((num, 128), 1)
                xs = range(28, 32) if nx < 0 else (range(32) if nx == 0 else range(4))
                for x in xs:
                    if ny == 0:
                        p = own(x) if nx == 0 else xr[side(nx), x % 4]
                    elif nx == 0:
                        p = yr[side(ny), x // 2]
                    else:
                        p = xyr[XY4.index((nx, ny)), (x % 4) // 2]
                    if ny != 0 and (x % 2 == 0) == (ny < 0):
                        p = roll(p, 4, 0)
                    mixed = jnp.where((lanes % 64) // 2 == x, high, low)
                    i = 32 * nx + x + 4
                    put(0, i, dst, num, jnp.where(lanes < 64, p, roll(mixed, 64 - 2 * x, 1)))
                    if colours == 2:
                        q = turned[x] if nx == 0 and ny == 0 else roll(p, 64, 1)
                        put(1, i, dst, num, jnp.where(lanes < 64, q, roll(mixed, -2 * x, 1)))

    def clean(level):
        def put(colour, i, dst, num, value):
            ok = level.coefficient(i, dst, dst + num) > 0.0
            (level.fr if colour == 0 else level.fb)[i, dst : dst + num, :] = jnp.where(ok, value, 0.0)

        return put

    def corrected(level, add):
        def put(colour, i, dst, num, value):
            ok = level.coefficient(i, dst, dst + num) > 0.0
            level.vb[i, dst : dst + num, :] = jnp.where(ok, value + add(i, dst, num), 0.0)

        return put

    ef0 = copies0(
        lambda dx: p0.at[pl.ds(0 if dx < 0 else 28, 4)], fy0, fz0, fx_r, fy_r, fxy_r, fz_r, s_all, r_f0
    )
    ev0 = copies0(
        lambda dx: vx0.at[side(dx)],
        vy0, vz0, vx_r, vy_r, vxy_r, vz_r, s_all, r_v0,
    )

    pack0(lambda x: p0[x], fy0, fz0)
    pl.semaphore_wait(barrier, count)
    start(ef0)

    def fill(ref, halo, pairs, start_pairs, total_pairs, rows_at, total_rows):
        zp = start_pairs + signed
        ok = (signed >= -halo) & (signed < pairs + halo) & (zp >= 0) & (zp < total_pairs)
        ok = ok & (rows_at >= 0) & (rows_at < total_rows)
        ref[0] = jnp.zeros((32, 128), F32)
        ref[1] = jnp.where(ok, INV, 0.0)

    fill(k0, 2, 64, iz * 64, NGZ * 64, iy * BY + r32 - 8, NGY * BY)
    fill(k1, 3, 32, iz * 32, NGZ * 32, iy * 8 + r32 - 16, NGY * 8)
    fill(k2, 4, 16, iz * 16, NGZ * 16, ix * 8 + r32 - 16, NGX * 8)

    def zero(ref):
        @pl.loop(0, ref.shape[0])
        def _(i):
            ref[i] = jnp.zeros(ref.shape[1:], F32)

    for ref in (vr0, vb0, vr1, vb1, vr2, vb2, pe0, pe1, pe2, v3, tmp2):
        zero(ref)

    to_pairs1 = jnp.where(
        (z256 < 64) & (c128 % 32 == z256 // 2) & ((c128 < 64) == red256), 0.5, 0.0
    ).astype(BF16)
    to_pairs2 = jnp.where(
        (z256 < 32) & (c128 % 32 == z256 // 2 + jnp.where(red256, 0, 16)), 0.5, 0.0
    ).astype(BF16)
    csign = jnp.where(cc2 < 96, cc2, cc2 - 128)
    wanted = ((csign + 128) // 2 - 64 + 64 * (csign % 2)) % 128
    from_pairs = jnp.where(same & (kk2 == wanted) & (csign >= -4) & (csign < 68), 1.0, 0.0).astype(BF16)

    for x in range(BX):
        turned[x] = roll(p0[x], 64, 1)

    arrive(r_f0, units0)
    token(tok, 2)
    unpack0(lambda x: p0[x], fx_r, fy_r, fxy_r, fz_r, clean(lev0), 2)
    smooth_down(lev0)
    for x in range(16):
        s0[x] = residual(lev0, 4 + 2 * x)

    rows = []
    for x in range(16):
        a = s0[x, pl.ds(0, 8, stride=2), :] + s0[x, pl.ds(1, 8, stride=2), :]
        rows.append(split_rows(a, (row + x) % 2 == 0))
    b1 = moved(jnp.concatenate(rows, axis=0), to_pairs1)

    def zpack1(plane, zp):
        lo = jnp.zeros((8, 128), F32)
        hi = jnp.zeros((8, 128), F32)
        for x in range(16):
            p = plane(x)
            lo = jnp.where((lane % 64) // 3 == x, roll(p, 3 * x, 1), lo)
            hi = jnp.where(((lane + 35) % 64) // 3 == x, roll(p, 3 * x + 64, 1), hi)
        zp[0] = lo
        zp[1] = hi

    def copies1(pk, zp, xr, yr, xyr, zr, ss, rs):
        out = []
        for d in D26:
            dx, dy, dz = d
            if dz == 0 and dx == 0:
                s, t = pk, yr.at[side(-dy)]
            elif dz == 0:
                s = pk.at[pl.ds(0 if dx < 0 else 5, 3)]
                t = xr.at[side(-dx)] if dy == 0 else xyr.at[XY4.index((-dx, -dy))]
            else:
                s, t = zp.at[side(dz)], zr.at[Z18.index(neg(d))]
            out.append((d, pltpu.make_async_remote_copy(s, t, ss, rs, at(d), MESH)))
        return out

    def unpack1(pk, xr, yr, xyr, zr, put, colours):
        for xe in range(28):
            nx, x = (-1, 10 + xe) if xe < 6 else ((0, xe - 6) if xe < 22 else (1, xe - 22))
            for ny in (-1, 0, 1):
                if nx == 0:
                    mid = pk[x // 2] if ny == 0 else yr[side(ny), x // 2]
                else:
                    tile = x // 2 - 5 if nx < 0 else x // 2
                    mid = xr[side(nx), tile] if ny == 0 else xyr[XY4.index((nx, ny)), tile]
                low, high = zr[Z18.index((nx, ny, -1))], zr[Z18.index((nx, ny, 1))]
                mixed = jnp.where((lane % 64) // 3 == x, high, low)
                for colour in range(colours):
                    a = roll(mid, -32 * (x % 2) - 64 * colour, 1)
                    b = roll(mixed, 32 - 3 * x - 64 * colour, 1)
                    put(colour, xe, 16 + 8 * ny, 8, jnp.where(lane < 32, a, b))

    ef1 = copies1(fk1, fz1, f1x_r, f1y_r, f1xy_r, f1z_r, s_all, r_f1)
    ev1 = copies1(vk1, vz1, v1x_r, v1y_r, v1xy_r, v1z_r, s_all, r_v1)
    for t in range(8):
        fk1[t] = jnp.where(lane % 64 < 32, b1[16 * t : 16 * t + 8], b1[16 * t + 8 : 16 * t + 16])
    zpack1(lambda x: b1[8 * x : 8 * x + 8], fz1)
    start(ef1)
    arrive(r_f1, units1)
    pl.semaphore_wait(tok, jnp.where((ix > 1) & (ix < NGX - 2), 2, 1) + far_y)
    token(tok4, 4)
    unpack1(fk1, f1x_r, f1y_r, f1xy_r, f1z_r, clean(lev1), 2)
    smooth_down(lev1)
    for x in range(8):
        s1[8 * x : 8 * x + 8, :] = residual(lev1, 6 + 2 * x)

    rows = []
    for y in range(4):
        a = s1[pl.ds(2 * y, 8, stride=8), :] + s1[pl.ds(2 * y + 1, 8, stride=8), :]
        rows.append(split_rows(a, (row + y) % 2 == 0))
    b2 = moved(jnp.concatenate(rows, axis=0), to_pairs2)

    def copies2(t, tr, ss, rs, directions):
        out = []
        for d in directions:
            dst = tr.at[D44.index(neg(d))]
            out.append((d, pltpu.make_async_remote_copy(t, dst, ss, rs, at(d), MESH)))
        return out

    def unpack2(own, tr, which, put, colours):
        part = lane % 32
        for ny in which:
            if ny == -2:
                ys = [(i, 1 + i) for i in range(3)]
            elif ny == 2:
                ys = [(15 + i, i) for i in range(3)]
            else:
                ys = [(7 + 4 * ny + i, i) for i in range(4)]
            for nx in (-1, 0, 1):
                mid = own[...] if (nx, ny) == (0, 0) else tr[D44.index((nx, ny, 0))]
                low, high = tr[D44.index((nx, ny, -1))], tr[D44.index((nx, ny, 1))]
                for colour in range(colours):
                    a = roll(mid, -16 * colour, 1)
                    b = roll(high, 16 - 16 * colour, 1)
                    c = roll(low, 112 - 16 * colour, 1)
                    mixed = jnp.where(part < 16, a, jnp.where(part < 24, b, c))
                    for e, y in ys:
                        put(colour, e, 16 + 8 * nx, 8, roll(mixed, -32 * y, 1))

    ef2 = copies2(ft2, f2_r, s_all, r_f2, D26)
    ef2b = copies2(ft2, f2_r, s_all, r_f2b, D44[26:])
    ev2 = copies2(vt2, v2_r, s_all, r_v2, D44)
    acc = b2[0:8]
    for y in range(1, 4):
        acc = jnp.where(lane // 32 == y, b2[8 * y : 8 * y + 8], acc)
    ft2[...] = acc
    start(ef2)
    arrive(r_f2, units2)
    unpack2(ft2, f2_r, (-1, 0, 1), clean(lev2), 2)
    smooth_down(lev2)

    for y in range(2):
        s2[8 * y : 8 * y + 8, :] = residual(lev2, 7 + 2 * y)
    a3 = s2[pl.ds(0, 8, stride=2), :] + s2[pl.ds(1, 8, stride=2), :]
    a3 = jnp.where(lane < 16, 0.5 * a3, 0.0)
    a3 = pltpu.roll(a3, 0, 1, stride=16, stride_axis=0)
    a3 = jnp.sum(a3, axis=0, keepdims=True)
    t3[...] = jnp.where(row == iy, a3, 0.0)

    egy, egz, egx = [], [], []
    for k in (4, 3, 5, 2, 6, 1, 7):
        peer = (ix, lax.rem(iy + k, NGY), iz)
        egy.append(pltpu.make_async_remote_copy(t3, gy_r.at[k - 1], s_all, r_gy, peer, MESH))
    for k in (2, 1, 3):
        peer = (ix, iy, lax.rem(iz + k, NGZ))
        egz.append(pltpu.make_async_remote_copy(gzb.at[iz], gzb.at[iz], s_all, r_gz, peer, MESH))
    for k in (4, 3, 5, 2, 6, 1, 7):
        peer = (lax.rem(ix + k, NGX), iy, iz)
        egx.append(pltpu.make_async_remote_copy(gzb, gxb.at[ix], s_all, r_gx, peer, MESH))

    pl.semaphore_wait(tok4, 2)
    for c in egy:
        c.start()
    start(ef2b)
    acc = jnp.zeros((8, 128), F32)
    for y in range(4):
        acc = jnp.where(lane // 32 == y, roll(vb2[7 + y, 16:24, :], 32 * y, 1), acc)
    vt2[...] = acc
    for t in range(8):
        vk1[t] = jnp.where(lane % 64 < 32, vb1[6 + 2 * t, 16:24, :], roll(vb1[7 + 2 * t, 16:24, :], 32, 1))
    zpack1(lambda x: vb1[6 + x, 16:24, :], vz1)
    pack0(lambda x: vb0[4 + x, 8:24, :], vy0, vz0)
    for x in range(4):
        vx0[0, x] = vb0[4 + x, 8:24, :]
        vx0[1, x] = vb0[32 + x, 8:24, :]
    wait_units(r_gy, 7)
    line = t3[...]
    for k in range(NGY - 1):
        line = line + gy_r[k]
    gzb[iz] = line
    for c in egz:
        c.start()
    wait_units(r_gz, 3)
    for c in egx:
        c.start()
    start(ev2)
    start(ev1)
    start(ev0)
    gxb[ix] = gzb[...]
    arrive(r_f2b, units2b)
    unpack2(ft2, f2_r, (-2, 2), clean(lev2), 2)
    wait_units(r_gx, 28)

    for gx in range(NGX):
        for xl in range(4):
            acc = jnp.zeros((8, 128), F32)
            for gz in range(NGZ):
                acc = jnp.where((lane % 64) // 16 == gz, roll(gxb[gx, gz], (gz - xl) * 16, 1), acc)
            g3[4 * gx + xl] = acc

    zl = lane % 64
    w_lo = jnp.where(zl == 0, 0.0, BETA1)
    w_hi = jnp.where(zl == 63, 0.0, BETA1)
    y_edge = jnp.where(((row == 0) & (lane < 64)) | ((row == 7) & (lane >= 64)), 0.0, 1.0)
    par3 = (lane // 64 + lane) & 1
    colours3 = (par3 == 0, par3 == 1)

    def sum3(x):
        c = v3[x + 4]
        a = roll(c, 64, 1)
        w = jnp.where(lane < 64, roll(a, 1, 0), roll(a, -1, 0)) * y_edge
        s = (v3[x + 3] + v3[x + 5]) + (a + w)
        return c, s + (roll(c, 1, 1) * w_lo + roll(c, -1, 1) * w_hi)

    def half3(colour):
        for j in range(4):
            done = []
            for x in range(8 * j, 8 * j + 8):
                c, s = sum3(x)
                done.append(jnp.where(colours3[(x + colour) % 2], (g3[x] + s) * INV, c))
            for u in range(8):
                v3[8 * j + u + 4] = done[u]

    for x in range(32):
        v3[x + 4] = jnp.where(colours3[x % 2], g3[x] * INV, 0.0)
    half3(1)
    half3(0)
    half3(1)

    def small(g, level):
        n = len(g)
        dz, dy = 2 ** (level - 3), 2 ** (level - 4)
        lo = jnp.where(zl < dz, 0.0, BETA1)
        hi = jnp.where(zl >= 64 - dz, 0.0, BETA1)
        ylo = jnp.where(row < dy, 0.0, 1.0)
        yhi = jnp.where(row >= 8 - dy, 0.0, 1.0)
        par = (row // dy + zl // dz) & 1
        colours = (par == 0, par == 1)

        def beside(c, lo, hi, ylo, yhi):
            z = roll(c, dz, 1) * lo + roll(c, -dz, 1) * hi
            return z + (roll(c, dy, 0) * ylo + roll(c, -dy, 0) * yhi)

        def fixed(v, x):
            s = g[x]
            if x > 0:
                s = s + v[x - 1]
            if x < n - 1:
                s = s + v[x + 1]
            return s

        weights = [[jnp.where(c, w * INV, 0.0) for w in (lo, hi, ylo, yhi)] for c in colours]

        def sweep(v, colour):
            out = []
            for x in range(n):
                c = (x + colour) % 2
                base = jnp.where(colours[c], fixed(v, x) * INV, v[x])
                out.append(base + beside(v[x], *weights[c]))
            return out

        v = [jnp.where(colours[x % 2], g[x] * INV, 0.0) for x in range(n)]
        v = sweep(v, 1)
        if level == 6:
            for _ in range(CSWEEPS - 1):
                v = sweep(sweep(v, 0), 1)
            return v
        v = sweep(sweep(v, 0), 1)
        r = [(fixed(v, x) - CENTRE * v[x]) + beside(v[x], lo, hi, ylo, yhi) for x in range(n)]
        coarse = []
        for x in range(n // 2):
            t = r[2 * x] + r[2 * x + 1]
            t = t + jnp.where((row // dy) % 2 == 0, roll(t, -dy, 0), roll(t, dy, 0))
            t = t + jnp.where((zl // dz) % 2 == 0, roll(t, -dz, 1), roll(t, dz, 1))
            coarse.append(0.5 * t)
        e = small(coarse, level + 1)
        v = [v[x] + e[x // 2] for x in range(n)]
        for _ in range(2):
            v = sweep(sweep(v, 0), 1)
        return v

    def resid3(x):
        c, s = sum3(x)
        return g3[x] - (CENTRE * c - s)

    g4 = []
    for x in range(16):
        t = resid3(2 * x) + resid3(2 * x + 1)
        t = t + roll(t, 64, 1)
        t = t + jnp.where(lane % 2 == 0, roll(t, -1, 1), roll(t, 1, 1))
        g4.append(0.5 * t)
    e4 = small(g4, 4)
    for x in range(32):
        v3[4 + x] = v3[4 + x] + e4[x // 2]
    for _ in range(2):
        half3(0)
        half3(1)

    for x in range(12):
        e = v3[4 * ix + x]
        for yl in range(2):
            tmp2[yl, 16 + 8 * x : 24 + 8 * x, :] = pltpu.roll(e, (128 - 16 * iz + 64 * yl) % 128, 1)
    for j in range(10):
        e = tmp2[j % 2, pl.ds(16 + iy - 2 + j // 2, 12, stride=8), :]
        pe2[j, pl.ds(8, 12, stride=2), :] = e
        pe2[j, pl.ds(9, 12, stride=2), :] = e
    arrive(r_v2, lambda *c: units2(*c) + units2b(*c))
    add2 = corrected(lev2, lambda i, dst, num: pe2[(i + 1) // 2, dst : dst + num, :])
    unpack2(vt2, v2_r, (-2, -1, 0, 1, 2), add2, 1)
    half(lev2, 1, 17, True)
    half(lev2, 2, 16, False)
    half(lev2, 3, 15, True)
    half(lev2, 4, 14, False)

    def cells(level, i, a, b):
        even = level.even(i, a, b)
        r, k = level.vr[i, a:b, :], level.vb[i, a:b, :]
        first, second = jnp.where(even, r, k), roll(jnp.where(even, k, r), 64, 1)
        lanes = iota((b - a, 128), 1)
        if level is lev0:
            return jnp.where(lanes < 64, first, second)
        return jnp.where((lanes < 40) | (lanes >= 104), first, second)

    def merged(level, planes, a, b, matrix):
        rows = []
        for i in range(0, len(planes), 2):
            rows.append(jnp.concatenate([cells(level, j, a, b) for j in planes[i : i + 2]], axis=1))
        u = moved(jnp.concatenate(rows, axis=0), matrix)
        n = b - a
        return [u[n * (i // 2) : n * (i // 2) + n, 128 * (i % 2) : 128 * (i % 2) + 128] for i in range(len(planes))]

    for i, e in enumerate(merged(lev2, range(3, 15), 8, 32, from_pairs)):
        tmp1[24 * i : 24 * i + 24, :] = e
    for k in range(14):
        e = tmp1[pl.ds(5 + k, 12, stride=24), :]
        pe1[k, pl.ds(8, 12, stride=2), :] = e
        pe1[k, pl.ds(9, 12, stride=2), :] = e
    arrive(r_v1, units1)
    add1 = corrected(lev1, lambda i, dst, num: pe1[i // 2, dst : dst + num, :])
    unpack1(vk1, v1x_r, v1y_r, v1xy_r, v1z_r, add1, 1)
    half(lev1, 1, 27, True)
    half(lev1, 2, 26, False)
    half(lev1, 3, 25, True)
    half(lev1, 4, 24, False)

    for k, e in enumerate(merged(lev1, range(4, 24), 14, 30, from_pairs)):
        e = e[0:12]
        pe0[k, pl.ds(4, 12, stride=2), :] = e
        pe0[k, pl.ds(5, 12, stride=2), :] = e
    arrive(r_v0, units0)
    add0 = corrected(lev0, lambda i, dst, num: pe0[i // 2, dst : dst + num, :])
    unpack0(lambda x: vb0[4 + x, 8:24, :], vx_r, vy_r, vxy_r, vz_r, add0, 1)
    half(lev0, 1, 39, True)
    half(lev0, 2, 38, False)
    half(lev0, 3, 37, True)
    half(lev0, 4, 36, False, (8, 24))

    for part in range(4):
        planes = range(4 + 8 * part, 12 + 8 * part)
        for x, e in enumerate(merged(lev0, planes, 8, 24, to_cells)):
            out[8 * part + x] = e
    arrive(s_all, lambda *c: 2 * (units0(*c) + units1(*c) + units2(*c) + units2b(*c)) + 38)


def on_device(density):
    def vmem(*shape):
        return pltpu.VMEM(shape, F32)

    coef = vmem(2, 32, 128)
    level0 = [vmem(BX, BY, BZ)] * 3 + [vmem(40, 32, 128)] * 5 + [coef, vmem(16, 16, 128), vmem(20, 32, 128)]
    level1 = [vmem(28, 40, 128)] * 5 + [coef, vmem(64, 128), vmem(14, 32, 128), vmem(288, 128)]
    level2 = [vmem(18, 40, 128)] * 5 + [coef, vmem(16, 128), vmem(10, 32, 128), vmem(2, 128, 128)]
    packs = [vmem(2, 16, 8, 128), vmem(2, 16, 128)] * 2 + [vmem(2, 4, 16, 128)] + [vmem(8, 8, 128), vmem(2, 8, 128)] * 2
    packs += [vmem(8, 128)] * 2
    recv0 = [vmem(2, 4, 16, 128), vmem(2, 16, 8, 128), vmem(4, 2, 8, 128), vmem(18, 16, 128)] * 2
    recv1 = [vmem(2, 3, 8, 128), vmem(2, 8, 8, 128), vmem(4, 3, 8, 128), vmem(18, 8, 128)] * 2
    recv2 = [vmem(44, 8, 128)] * 2
    gather = [vmem(8, 128), vmem(7, 8, 128), vmem(4, 8, 128), vmem(8, 4, 8, 128), vmem(32, 8, 128), vmem(40, 8, 128)]
    dma = pltpu.SemaphoreType.DMA
    token = pltpu.SemaphoreType.REGULAR
    sems = [vmem(400, 8, 128), token, token] + [dma] * 12
    return pl.pallas_call(
        kernel,
        out_shape=jax.ShapeDtypeStruct((BX, BY, BZ), F32),
        in_specs=[pl.BlockSpec(memory_space=pltpu.HBM)],
        out_specs=pl.BlockSpec(memory_space=pltpu.VMEM),
        scratch_shapes=level0 + level1 + level2 + packs + recv0 + recv1 + recv2 + gather + sems,
        compiler_params=pltpu.CompilerParams(
            collective_id=0, has_side_effects=True, vmem_limit_bytes=48 * 1024 * 1024
        ),
    )(pltpu.with_memory_space_constraint(density, pltpu.HBM))


def solution(mesh):
    spec = P("gx", "gy", "gz")
    return jax.shard_map(on_device, mesh=mesh, in_specs=(spec,), out_specs=spec, check_vma=False)
```

```python
import itertools

import jax
import jax.numpy as jnp
from jax import lax
from jax.experimental import pallas as pl
from jax.experimental.pallas import tpu as pltpu
from jax.sharding import PartitionSpec as P

MESH = pl.DeviceIdType.MESH
F32 = jnp.float32
BF16 = jnp.bfloat16

NGX, NGY, NGZ = 8, 8, 4
BX, BY, BZ = 32, 16, 128
CSWEEPS = 4
BETA1 = 1.5
CENTRE = 4.0 + 2.0 * BETA1
INV = 1.0 / CENTRE

D26 = [d for d in itertools.product((-1, 0, 1), repeat=3) if d != (0, 0, 0)]
D26.sort(key=lambda d: -sum(map(abs, d)))
D44 = D26 + [d for d in itertools.product((-1, 0, 1), (-2, 2), (-1, 0, 1))]
XY4 = [(-1, -1), (-1, 1), (1, -1), (1, 1)]
Z18 = [d for d in D26 if d[2] != 0]


def roll(x, shift, axis):
    size = x.shape[axis]
    shift = shift % size
    return x if shift == 0 else pltpu.roll(x, shift, axis)


def iota(shape, dim):
    return lax.broadcasted_iota(jnp.int32, shape, dim)


def side(n):
    return 0 if n < 0 else 1


def neg(n):
    return (-n[0], -n[1], -n[2])


def moved(x, matrix):
    hi = x.astype(BF16)
    rest = x - hi.astype(F32)
    mid = rest.astype(BF16)
    lo = (rest - mid.astype(F32)).astype(BF16)
    return (
        jnp.dot(lo, matrix, preferred_element_type=F32)
        + jnp.dot(mid, matrix, preferred_element_type=F32)
        + jnp.dot(hi, matrix, preferred_element_type=F32)
    )


def kernel(
    f_hbm, out,
    f0, p0, turned, fr0, fb0, vr0, vb0, rest0, k0, s0, pe0,
    fr1, fb1, vr1, vb1, rest1, k1, s1, pe1, tmp1,
    fr2, fb2, vr2, vb2, rest2, k2, s2, pe2, tmp2,
    fy0, fz0, vy0, vz0, vx0, fk1, fz1, vk1, vz1, ft2, vt2,
    fx_r, fy_r, fxy_r, fz_r, vx_r, vy_r, vxy_r, vz_r,
    f1x_r, f1y_r, f1xy_r, f1z_r, v1x_r, v1y_r, v1xy_r, v1z_r,
    f2_r, v2_r,
    t3, gy_r, gzb, gxb, g3, v3,
    spare, tok, tok4, io_sem, s_all, r_f0, r_v0, r_f1, r_v1, r_f2, r_f2b, r_v2, r_gy, r_gz, r_gx,
):
    ix, iy, iz = lax.axis_index("gx"), lax.axis_index("gy"), lax.axis_index("gz")

    def there(n):
        nx, ny, nz = ix + n[0], iy + n[1], iz + n[2]
        return (nx >= 0) & (nx < NGX) & (ny >= 0) & (ny < NGY) & (nz >= 0) & (nz < NGZ)

    def at(n):
        return (
            jnp.clip(ix + n[0], 0, NGX - 1),
            jnp.clip(iy + n[1], 0, NGY - 1),
            jnp.clip(iz + n[2], 0, NGZ - 1),
        )

    load = pltpu.make_async_copy(f_hbm, f0, io_sem)
    load.start()

    barrier = pltpu.get_barrier_semaphore()
    count = 0
    for d in D26:
        ok = there(d)
        count = count + ok.astype(jnp.int32)

        @pl.when(ok)
        def _(d=d):
            pl.semaphore_signal(barrier, inc=1, device_id=at(d), device_id_type=MESH)

    def token(sem, reach):
        for d in ((-reach, 0, 0), (reach, 0, 0), (0, -reach, 0), (0, reach, 0)):
            @pl.when(there(d))
            def _(d=d):
                pl.semaphore_signal(sem, inc=1, device_id=at(d), device_id_type=MESH)

    lane = iota((8, 128), 1)
    row = iota((8, 128), 0)
    lane16 = iota((16, 128), 1)
    r32, l32 = iota((32, 128), 0), iota((32, 128), 1)
    signed = jnp.where(l32 < 96, l32, l32 - 128)

    class Level:
        def __init__(self, fr, fb, vr, vb, rest, k, first, main, rows, window, odd, start, total):
            self.fr, self.fb, self.vr, self.vb, self.rest, self.k = fr, fb, vr, vb, rest, k
            self.first, self.main, self.rows, self.window = first, main, rows, window
            self.odd, self.start, self.total = odd, start, total
            self.planes = main + 2 * first

        def coefficient(self, i, lo, hi):
            if self.first <= i < self.first + self.main:
                return self.k[1, lo:hi, :]
            pos = self.start + i
            return self.k[jnp.where((pos >= 0) & (pos < self.total), 1, 0), lo:hi, :]

        def even(self, i, lo, hi):
            return (iota((hi - lo, 128), 0) + (lo + i + self.odd)) % 2 == 0

    lev0 = Level(fr0, fb0, vr0, vb0, rest0, k0, 4, BX, (8, 24), (4, 28), 0, ix * BX - 4, NGX * BX)
    lev1 = Level(fr1, fb1, vr1, vb1, rest1, k1, 6, 16, (16, 24), (8, 32), 0, ix * 16 - 6, NGX * 16)
    lev2 = Level(fr2, fb2, vr2, vb2, rest2, k2, 7, 4, (16, 24), (8, 32), 1, iy * 4 - 7, NGY * 4)

    def around(level, src, i, lo, hi, red):
        c0, c1 = src[i, lo:hi, :], src[i + 1, lo:hi, :]
        even = level.even(i, lo, hi)
        first, second = (c0, c1) if red else (c1, c0)
        up = roll(jnp.where(even, first, second), 1, 1)
        down = roll(jnp.where(even, second, first), -1, 1)
        z0, z1 = jnp.where(even, up, down), jnp.where(even, down, up)
        if not red:
            z0, z1 = z1, z0

        def plane(j, other, c, z):
            s = (other + src[j, lo - 1 : hi - 1, :]) + src[j, lo + 1 : hi + 1, :]
            return s + BETA1 * (c + z)

        return (
            plane(i, src[i - 1, lo:hi, :] + c1, c0, z0),
            plane(i + 1, c0 + src[i + 2, lo:hi, :], c1, z1),
        )

    def half(level, lo, hi, red, rows=None, keep=False):
        dst, src = (level.vr, level.vb) if red else (level.vb, level.vr)
        source = level.fr if red else level.fb
        a, b = rows or level.window
        for i in range(lo, hi, 2):
            for j, s in enumerate(around(level, src, i, a, b, red)):
                s = source[i + j, a:b, :] + s
                v = s * level.coefficient(i + j, a, b)
                dst[i + j, a:b, :] = v
                if keep and level.first <= i + j < level.first + level.main:
                    level.rest[i + j, a:b, :] = s - CENTRE * v

    def first_half(level, lo, hi):
        a, b = level.window
        for i in range(lo, hi):
            level.vr[i, a:b, :] = level.fr[i, a:b, :] * level.coefficient(i, a, b)

    def smooth_down(level):
        n, m = level.first, level.first + level.main
        first_half(level, n - 4, m + 4)
        half(level, n - 3, m + 3, False)
        half(level, n - 2, m + 2, True)
        half(level, n - 1, m + 1, False, keep=True)

    def residual(level, i):
        a, b = level.rows
        total = level.rest[i, a:b, :] + level.rest[i + 1, a:b, :]
        for j, s in enumerate(around(level, level.vb, i, a, b, True)):
            total = total + (level.fr[i + j, a:b, :] - (CENTRE * level.vr[i + j, a:b, :] - s))
        return total

    def split_rows(a, even):
        return jnp.concatenate([jnp.where(even, a, 0.0), jnp.where(even, 0.0, a)], axis=1)

    k256, c128 = iota((256, 128), 0), iota((256, 128), 1)
    z256 = k256 % 128
    red256 = (z256 + k256 // 128) % 2 == 0

    load.wait()

    kk2, cc2 = iota((256, 256), 0), iota((256, 256), 1)
    same = kk2 // 128 == cc2 // 128
    kk2, cc2 = kk2 % 128, cc2 % 128
    to_pairs = jnp.where(same & (cc2 == kk2 // 2 + 64 * (kk2 % 2)), 1.0, 0.0).astype(BF16)
    to_cells = jnp.where(same & (kk2 == cc2 // 2 + 64 * (cc2 % 2)), 1.0, 0.0).astype(BF16)
    for part in range(4):
        rows = []
        for x in range(8 * part, 8 * part + 8, 2):
            rows.append(jnp.concatenate([f0[x], f0[x + 1]], axis=1))
        p = moved(jnp.concatenate(rows, axis=0), to_pairs)
        for x in range(8):
            q = p[16 * (x // 2) : 16 * (x // 2) + 16, 128 * (x % 2) : 128 * (x % 2) + 128]
            p0[8 * part + x] = jnp.where((iota((16, 128), 0) + x) % 2 == 0, q, roll(q, 64, 1))

    def pack0(plane, yp, zp):
        lo = jnp.zeros((16, 128), F32)
        hi = jnp.zeros((16, 128), F32)
        slot = (lane16 % 64) // 2
        for x in range(BX):
            p = plane(x)
            half_tile = slice(4 * (x % 2), 4 * (x % 2) + 4)
            yp[0, x // 2, half_tile, :] = p[0:4]
            yp[1, x // 2, half_tile, :] = p[12:16]
            t = roll(p, 2 * x, 1)
            lo = jnp.where(slot == x, t, lo)
            hi = jnp.where(slot == (x - 1) % BX, t, hi)
        zp[0] = lo
        zp[1] = hi

    def copies0(xs, yp, zp, xr, yr, xyr, zr, ss, rs):
        out = []
        for d in D26:
            dx, dy, dz = d
            if dz == 0 and dy == 0:
                s, t = xs(dx), xr.at[side(-dx)]
            elif dz == 0 and dx == 0:
                s, t = yp.at[side(dy)], yr.at[side(-dy)]
            elif dz == 0:
                s = yp.at[side(dy), pl.ds(0 if dx < 0 else 14, 2)]
                t = xyr.at[XY4.index((-dx, -dy))]
            else:
                slot = Z18.index(neg(d))
                if dy == 0:
                    s, t = zp.at[side(dz)], zr.at[slot]
                else:
                    rows = pl.ds(0 if dy < 0 else 8, 8)
                    s, t = zp.at[side(dz), rows], zr.at[slot, rows]
            out.append((d, pltpu.make_async_remote_copy(s, t, ss, rs, at(d), MESH)))
        return out

    def start(copies):
        for d, c in copies:
            @pl.when(there(d))
            def _(c=c):
                c.start()

    near_x = jnp.where((ix > 0) & (ix < NGX - 1), 2, 1)
    near_z = jnp.where((iz > 0) & (iz < NGZ - 1), 2, 1)
    near_y = jnp.where((iy > 0) & (iy < NGY - 1), 2, 1)
    far_y = jnp.where((iy > 1) & (iy < NGY - 2), 2, 1)

    def units0(x, y, y2, z):
        return x * 8 + y * 16 + x * y * 2 + z * (2 + 2 * x + y + x * y)

    def units1(x, y, y2, z):
        return x * 3 + y * 8 + x * y * 3 + z * (1 + x) * (1 + y)

    def units2(x, y, y2, z):
        return (1 + x) * (1 + y) * (1 + z) - 1

    def units2b(x, y, y2, z):
        return (1 + x) * y2 * (1 + z)

    def wait_units(sem, n):
        pltpu.make_async_copy(spare.at[pl.ds(0, n)], spare.at[pl.ds(0, n)], sem).wait()

    def arrive(sem, units):
        for x, (y, y2), z in itertools.product((1, 2), ((1, 1), (2, 1), (2, 2)), (1, 2)):
            @pl.when((near_x == x) & (near_y == y) & (far_y == y2) & (near_z == z))
            def _(n=units(x, y, y2, z)):
                wait_units(sem, n)

    def unpack0(own, xr, yr, xyr, zr, put, colours):
        for nx in (-1, 0, 1):
            for ny, src, dst, num in ((-1, 8, 0, 8), (0, 0, 8, 16), (1, 0, 24, 8)):
                low = zr[Z18.index((nx, ny, -1)), src : src + num, :]
                high = zr[Z18.index((nx, ny, 1)), src : src + num, :]
                lanes = iota((num, 128), 1)
                xs = range(28, 32) if nx < 0 else (range(32) if nx == 0 else range(4))
                for x in xs:
                    if ny == 0:
                        p = own(x) if nx == 0 else xr[side(nx), x % 4]
                    elif nx == 0:
                        p = yr[side(ny), x // 2]
                    else:
                        p = xyr[XY4.index((nx, ny)), (x % 4) // 2]
                    if ny != 0 and (x % 2 == 0) == (ny < 0):
                        p = roll(p, 4, 0)
                    mixed = jnp.where((lanes % 64) // 2 == x, high, low)
                    i = 32 * nx + x + 4
                    put(0, i, dst, num, jnp.where(lanes < 64, p, roll(mixed, 64 - 2 * x, 1)))
                    if colours == 2:
                        q = turned[x] if nx == 0 and ny == 0 else roll(p, 64, 1)
                        put(1, i, dst, num, jnp.where(lanes < 64, q, roll(mixed, -2 * x, 1)))

    def clean(level):
        def put(colour, i, dst, num, value):
            ok = level.coefficient(i, dst, dst + num) > 0.0
            (level.fr if colour == 0 else level.fb)[i, dst : dst + num, :] = jnp.where(ok, value, 0.0)

        return put

    def corrected(level, add):
        def put(colour, i, dst, num, value):
            ok = level.coefficient(i, dst, dst + num) > 0.0
            level.vb[i, dst : dst + num, :] = jnp.where(ok, value + add(i, dst, num), 0.0)

        return put

    ef0 = copies0(
        lambda dx: p0.at[pl.ds(0 if dx < 0 else 28, 4)], fy0, fz0, fx_r, fy_r, fxy_r, fz_r, s_all, r_f0
    )
    ev0 = copies0(
        lambda dx: vx0.at[side(dx)],
        vy0, vz0, vx_r, vy_r, vxy_r, vz_r, s_all, r_v0,
    )

    pack0(lambda x: p0[x], fy0, fz0)
    pl.semaphore_wait(barrier, count)
    start(ef0)

    def fill(ref, halo, pairs, start_pairs, total_pairs, rows_at, total_rows):
        zp = start_pairs + signed
        ok = (signed >= -halo) & (signed < pairs + halo) & (zp >= 0) & (zp < total_pairs)
        ok = ok & (rows_at >= 0) & (rows_at < total_rows)
        ref[0] = jnp.zeros((32, 128), F32)
        ref[1] = jnp.where(ok, INV, 0.0)

    fill(k0, 2, 64, iz * 64, NGZ * 64, iy * BY + r32 - 8, NGY * BY)
    fill(k1, 3, 32, iz * 32, NGZ * 32, iy * 8 + r32 - 16, NGY * 8)
    fill(k2, 4, 16, iz * 16, NGZ * 16, ix * 8 + r32 - 16, NGX * 8)

    def zero(ref):
        @pl.loop(0, ref.shape[0])
        def _(i):
            ref[i] = jnp.zeros(ref.shape[1:], F32)

    for ref in (vr0, vb0, vr1, vb1, vr2, vb2, pe0, pe1, pe2, v3, tmp2):
        zero(ref)

    to_pairs1 = jnp.where(
        (z256 < 64) & (c128 % 32 == z256 // 2) & ((c128 < 64) == red256), 0.5, 0.0
    ).astype(BF16)
    to_pairs2 = jnp.where(
        (z256 < 32) & (c128 % 32 == z256 // 2 + jnp.where(red256, 0, 16)), 0.5, 0.0
    ).astype(BF16)
    csign = jnp.where(cc2 < 96, cc2, cc2 - 128)
    wanted = ((csign + 128) // 2 - 64 + 64 * (csign % 2)) % 128
    from_pairs = jnp.where(same & (kk2 == wanted) & (csign >= -4) & (csign < 68), 1.0, 0.0).astype(BF16)

    for x in range(BX):
        turned[x] = roll(p0[x], 64, 1)

    arrive(r_f0, units0)
    token(tok, 2)
    unpack0(lambda x: p0[x], fx_r, fy_r, fxy_r, fz_r, clean(lev0), 2)
    smooth_down(lev0)
    for x in range(16):
        s0[x] = residual(lev0, 4 + 2 * x)

    rows = []
    for x in range(16):
        a = s0[x, pl.ds(0, 8, stride=2), :] + s0[x, pl.ds(1, 8, stride=2), :]
        rows.append(split_rows(a, (row + x) % 2 == 0))
    b1 = moved(jnp.concatenate(rows, axis=0), to_pairs1)

    def zpack1(plane, zp):
        lo = jnp.zeros((8, 128), F32)
        hi = jnp.zeros((8, 128), F32)
        for x in range(16):
            p = plane(x)
            lo = jnp.where((lane % 64) // 3 == x, roll(p, 3 * x, 1), lo)
            hi = jnp.where(((lane + 35) % 64) // 3 == x, roll(p, 3 * x + 64, 1), hi)
        zp[0] = lo
        zp[1] = hi

    def copies1(pk, zp, xr, yr, xyr, zr, ss, rs):
        out = []
        for d in D26:
            dx, dy, dz = d
            if dz == 0 and dx == 0:
                s, t = pk, yr.at[side(-dy)]
            elif dz == 0:
                s = pk.at[pl.ds(0 if dx < 0 else 5, 3)]
                t = xr.at[side(-dx)] if dy == 0 else xyr.at[XY4.index((-dx, -dy))]
            else:
                s, t = zp.at[side(dz)], zr.at[Z18.index(neg(d))]
            out.append((d, pltpu.make_async_remote_copy(s, t, ss, rs, at(d), MESH)))
        return out

    def unpack1(pk, xr, yr, xyr, zr, put, colours):
        for xe in range(28):
            nx, x = (-1, 10 + xe) if xe < 6 else ((0, xe - 6) if xe < 22 else (1, xe - 22))
            for ny in (-1, 0, 1):
                if nx == 0:
                    mid = pk[x // 2] if ny == 0 else yr[side(ny), x // 2]
                else:
                    tile = x // 2 - 5 if nx < 0 else x // 2
                    mid = xr[side(nx), tile] if ny == 0 else xyr[XY4.index((nx, ny)), tile]
                low, high = zr[Z18.index((nx, ny, -1))], zr[Z18.index((nx, ny, 1))]
                mixed = jnp.where((lane % 64) // 3 == x, high, low)
                for colour in range(colours):
                    a = roll(mid, -32 * (x % 2) - 64 * colour, 1)
                    b = roll(mixed, 32 - 3 * x - 64 * colour, 1)
                    put(colour, xe, 16 + 8 * ny, 8, jnp.where(lane < 32, a, b))

    ef1 = copies1(fk1, fz1, f1x_r, f1y_r, f1xy_r, f1z_r, s_all, r_f1)
    ev1 = copies1(vk1, vz1, v1x_r, v1y_r, v1xy_r, v1z_r, s_all, r_v1)
    for t in range(8):
        fk1[t] = jnp.where(lane % 64 < 32, b1[16 * t : 16 * t + 8], b1[16 * t + 8 : 16 * t + 16])
    zpack1(lambda x: b1[8 * x : 8 * x + 8], fz1)
    start(ef1)
    arrive(r_f1, units1)
    pl.semaphore_wait(tok, jnp.where((ix > 1) & (ix < NGX - 2), 2, 1) + far_y)
    token(tok4, 4)
    unpack1(fk1, f1x_r, f1y_r, f1xy_r, f1z_r, clean(lev1), 2)
    smooth_down(lev1)
    for x in range(8):
        s1[8 * x : 8 * x + 8, :] = residual(lev1, 6 + 2 * x)

    rows = []
    for y in range(4):
        a = s1[pl.ds(2 * y, 8, stride=8), :] + s1[pl.ds(2 * y + 1, 8, stride=8), :]
        rows.append(split_rows(a, (row + y) % 2 == 0))
    b2 = moved(jnp.concatenate(rows, axis=0), to_pairs2)

    def copies2(t, tr, ss, rs, directions):
        out = []
        for d in directions:
            dst = tr.at[D44.index(neg(d))]
            out.append((d, pltpu.make_async_remote_copy(t, dst, ss, rs, at(d), MESH)))
        return out

    def unpack2(own, tr, which, put, colours):
        part = lane % 32
        for ny in which:
            if ny == -2:
                ys = [(i, 1 + i) for i in range(3)]
            elif ny == 2:
                ys = [(15 + i, i) for i in range(3)]
            else:
                ys = [(7 + 4 * ny + i, i) for i in range(4)]
            for nx in (-1, 0, 1):
                mid = own[...] if (nx, ny) == (0, 0) else tr[D44.index((nx, ny, 0))]
                low, high = tr[D44.index((nx, ny, -1))], tr[D44.index((nx, ny, 1))]
                for colour in range(colours):
                    a = roll(mid, -16 * colour, 1)
                    b = roll(high, 16 - 16 * colour, 1)
                    c = roll(low, 112 - 16 * colour, 1)
                    mixed = jnp.where(part < 16, a, jnp.where(part < 24, b, c))
                    for e, y in ys:
                        put(colour, e, 16 + 8 * nx, 8, roll(mixed, -32 * y, 1))

    ef2 = copies2(ft2, f2_r, s_all, r_f2, D26)
    ef2b = copies2(ft2, f2_r, s_all, r_f2b, D44[26:])
    ev2 = copies2(vt2, v2_r, s_all, r_v2, D44)
    acc = b2[0:8]
    for y in range(1, 4):
        acc = jnp.where(lane // 32 == y, b2[8 * y : 8 * y + 8], acc)
    ft2[...] = acc
    start(ef2)
    arrive(r_f2, units2)
    unpack2(ft2, f2_r, (-1, 0, 1), clean(lev2), 2)
    smooth_down(lev2)

    for y in range(2):
        s2[8 * y : 8 * y + 8, :] = residual(lev2, 7 + 2 * y)
    a3 = s2[pl.ds(0, 8, stride=2), :] + s2[pl.ds(1, 8, stride=2), :]
    a3 = jnp.where(lane < 16, 0.5 * a3, 0.0)
    a3 = pltpu.roll(a3, 0, 1, stride=16, stride_axis=0)
    a3 = jnp.sum(a3, axis=0, keepdims=True)
    t3[...] = jnp.where(row == iy, a3, 0.0)

    egy, egz, egx = [], [], []
    for k in (4, 3, 5, 2, 6, 1, 7):
        peer = (ix, lax.rem(iy + k, NGY), iz)
        egy.append(pltpu.make_async_remote_copy(t3, gy_r.at[k - 1], s_all, r_gy, peer, MESH))
    for k in (2, 1, 3):
        peer = (ix, iy, lax.rem(iz + k, NGZ))
        egz.append(pltpu.make_async_remote_copy(gzb.at[iz], gzb.at[iz], s_all, r_gz, peer, MESH))
    for k in (4, 3, 5, 2, 6, 1, 7):
        peer = (lax.rem(ix + k, NGX), iy, iz)
        egx.append(pltpu.make_async_remote_copy(gzb, gxb.at[ix], s_all, r_gx, peer, MESH))

    pl.semaphore_wait(tok4, 2)
    for c in egy:
        c.start()
    start(ef2b)
    acc = jnp.zeros((8, 128), F32)
    for y in range(4):
        acc = jnp.where(lane // 32 == y, roll(vb2[7 + y, 16:24, :], 32 * y, 1), acc)
    vt2[...] = acc
    for t in range(8):
        vk1[t] = jnp.where(lane % 64 < 32, vb1[6 + 2 * t, 16:24, :], roll(vb1[7 + 2 * t, 16:24, :], 32, 1))
    zpack1(lambda x: vb1[6 + x, 16:24, :], vz1)
    pack0(lambda x: vb0[4 + x, 8:24, :], vy0, vz0)
    for x in range(4):
        vx0[0, x] = vb0[4 + x, 8:24, :]
        vx0[1, x] = vb0[32 + x, 8:24, :]
    wait_units(r_gy, 7)
    line = t3[...]
    for k in range(NGY - 1):
        line = line + gy_r[k]
    gzb[iz] = line
    for c in egz:
        c.start()
    wait_units(r_gz, 3)
    for c in egx:
        c.start()
    start(ev2)
    start(ev1)
    start(ev0)
    gxb[ix] = gzb[...]
    arrive(r_f2b, units2b)
    unpack2(ft2, f2_r, (-2, 2), clean(lev2), 2)
    wait_units(r_gx, 28)

    for gx in range(NGX):
        for xl in range(4):
            acc = jnp.zeros((8, 128), F32)
            for gz in range(NGZ):
                acc = jnp.where((lane % 64) // 16 == gz, roll(gxb[gx, gz], (gz - xl) * 16, 1), acc)
            g3[4 * gx + xl] = acc

    zl = lane % 64
    w_lo = jnp.where(zl == 0, 0.0, BETA1)
    w_hi = jnp.where(zl == 63, 0.0, BETA1)
    y_edge = jnp.where(((row == 0) & (lane < 64)) | ((row == 7) & (lane >= 64)), 0.0, 1.0)
    par3 = (lane // 64 + lane) & 1
    colours3 = (par3 == 0, par3 == 1)

    def sum3(x):
        c = v3[x + 4]
        a = roll(c, 64, 1)
        w = jnp.where(lane < 64, roll(a, 1, 0), roll(a, -1, 0)) * y_edge
        s = (v3[x + 3] + v3[x + 5]) + (a + w)
        return c, s + (roll(c, 1, 1) * w_lo + roll(c, -1, 1) * w_hi)

    def half3(colour):
        for j in range(4):
            done = []
            for x in range(8 * j, 8 * j + 8):
                c, s = sum3(x)
                done.append(jnp.where(colours3[(x + colour) % 2], (g3[x] + s) * INV, c))
            for u in range(8):
                v3[8 * j + u + 4] = done[u]

    for x in range(32):
        v3[x + 4] = jnp.where(colours3[x % 2], g3[x] * INV, 0.0)
    half3(1)
    half3(0)
    half3(1)

    def small(g, level):
        n = len(g)
        dz, dy = 2 ** (level - 3), 2 ** (level - 4)
        lo = jnp.where(zl < dz, 0.0, BETA1)
        hi = jnp.where(zl >= 64 - dz, 0.0, BETA1)
        ylo = jnp.where(row < dy, 0.0, 1.0)
        yhi = jnp.where(row >= 8 - dy, 0.0, 1.0)
        par = (row // dy + zl // dz) & 1
        colours = (par == 0, par == 1)

        def beside(c, lo, hi, ylo, yhi):
            z = roll(c, dz, 1) * lo + roll(c, -dz, 1) * hi
            return z + (roll(c, dy, 0) * ylo + roll(c, -dy, 0) * yhi)

        def fixed(v, x):
            s = g[x]
            if x > 0:
                s = s + v[x - 1]
            if x < n - 1:
                s = s + v[x + 1]
            return s

        weights = [[jnp.where(c, w * INV, 0.0) for w in (lo, hi, ylo, yhi)] for c in colours]

        def sweep(v, colour):
            out = []
            for x in range(n):
                c = (x + colour) % 2
                base = jnp.where(colours[c], fixed(v, x) * INV, v[x])
                out.append(base + beside(v[x], *weights[c]))
            return out

        v = [jnp.where(colours[x % 2], g[x] * INV, 0.0) for x in range(n)]
        v = sweep(v, 1)
        if level == 6:
            for _ in range(CSWEEPS - 1):
                v = sweep(sweep(v, 0), 1)
            return v
        v = sweep(sweep(v, 0), 1)
        r = [(fixed(v, x) - CENTRE * v[x]) + beside(v[x], lo, hi, ylo, yhi) for x in range(n)]
        coarse = []
        for x in range(n // 2):
            t = r[2 * x] + r[2 * x + 1]
            t = t + jnp.where((row // dy) % 2 == 0, roll(t, -dy, 0), roll(t, dy, 0))
            t = t + jnp.where((zl // dz) % 2 == 0, roll(t, -dz, 1), roll(t, dz, 1))
            coarse.append(0.5 * t)
        e = small(coarse, level + 1)
        v = [v[x] + e[x // 2] for x in range(n)]
        for _ in range(2):
            v = sweep(sweep(v, 0), 1)
        return v

    def resid3(x):
        c, s = sum3(x)
        return g3[x] - (CENTRE * c - s)

    g4 = []
    for x in range(16):
        t = resid3(2 * x) + resid3(2 * x + 1)
        t = t + roll(t, 64, 1)
        t = t + jnp.where(lane % 2 == 0, roll(t, -1, 1), roll(t, 1, 1))
        g4.append(0.5 * t)
    e4 = small(g4, 4)
    for x in range(32):
        v3[4 + x] = v3[4 + x] + e4[x // 2]
    for _ in range(2):
        half3(0)
        half3(1)

    for x in range(12):
        e = v3[4 * ix + x]
        for yl in range(2):
            tmp2[yl, 16 + 8 * x : 24 + 8 * x, :] = pltpu.roll(e, (128 - 16 * iz + 64 * yl) % 128, 1)
    for j in range(10):
        e = tmp2[j % 2, pl.ds(16 + iy - 2 + j // 2, 12, stride=8), :]
        pe2[j, pl.ds(8, 12, stride=2), :] = e
        pe2[j, pl.ds(9, 12, stride=2), :] = e
    arrive(r_v2, lambda *c: units2(*c) + units2b(*c))
    add2 = corrected(lev2, lambda i, dst, num: pe2[(i + 1) // 2, dst : dst + num, :])
    unpack2(vt2, v2_r, (-2, -1, 0, 1, 2), add2, 1)
    half(lev2, 1, 17, True)
    half(lev2, 2, 16, False)
    half(lev2, 3, 15, True)
    half(lev2, 4, 14, False)

    def cells(level, i, a, b):
        even = level.even(i, a, b)
        r, k = level.vr[i, a:b, :], level.vb[i, a:b, :]
        first, second = jnp.where(even, r, k), roll(jnp.where(even, k, r), 64, 1)
        lanes = iota((b - a, 128), 1)
        if level is lev0:
            return jnp.where(lanes < 64, first, second)
        return jnp.where((lanes < 40) | (lanes >= 104), first, second)

    def merged(level, planes, a, b, matrix):
        rows = []
        for i in range(0, len(planes), 2):
            rows.append(jnp.concatenate([cells(level, j, a, b) for j in planes[i : i + 2]], axis=1))
        u = moved(jnp.concatenate(rows, axis=0), matrix)
        n = b - a
        return [u[n * (i // 2) : n * (i // 2) + n, 128 * (i % 2) : 128 * (i % 2) + 128] for i in range(len(planes))]

    for i, e in enumerate(merged(lev2, range(3, 15), 8, 32, from_pairs)):
        tmp1[24 * i : 24 * i + 24, :] = e
    for k in range(14):
        e = tmp1[pl.ds(5 + k, 12, stride=24), :]
        pe1[k, pl.ds(8, 12, stride=2), :] = e
        pe1[k, pl.ds(9, 12, stride=2), :] = e
    arrive(r_v1, units1)
    add1 = corrected(lev1, lambda i, dst, num: pe1[i // 2, dst : dst + num, :])
    unpack1(vk1, v1x_r, v1y_r, v1xy_r, v1z_r, add1, 1)
    half(lev1, 1, 27, True)
    half(lev1, 2, 26, False)
    half(lev1, 3, 25, True)
    half(lev1, 4, 24, False)

    for k, e in enumerate(merged(lev1, range(4, 24), 14, 30, from_pairs)):
        e = e[0:12]
        pe0[k, pl.ds(4, 12, stride=2), :] = e
        pe0[k, pl.ds(5, 12, stride=2), :] = e
    arrive(r_v0, units0)
    add0 = corrected(lev0, lambda i, dst, num: pe0[i // 2, dst : dst + num, :])
    unpack0(lambda x: vb0[4 + x, 8:24, :], vx_r, vy_r, vxy_r, vz_r, add0, 1)
    half(lev0, 1, 39, True)
    half(lev0, 2, 38, False)
    half(lev0, 3, 37, True)
    half(lev0, 4, 36, False, (8, 24))

    for part in range(4):
        planes = range(4 + 8 * part, 12 + 8 * part)
        for x, e in enumerate(merged(lev0, planes, 8, 24, to_cells)):
            out[8 * part + x] = e
    arrive(s_all, lambda *c: 2 * (units0(*c) + units1(*c) + units2(*c) + units2b(*c)) + 38)


def on_device(density):
    def vmem(*shape):
        return pltpu.VMEM(shape, F32)

    coef = vmem(2, 32, 128)
    level0 = [vmem(BX, BY, BZ)] * 3 + [vmem(40, 32, 128)] * 5 + [coef, vmem(16, 16, 128), vmem(20, 40, 128)]
    level1 = [vmem(28, 40, 128)] * 5 + [coef, vmem(64, 128), vmem(14, 40, 128), vmem(400, 128)]
    level2 = [vmem(18, 40, 128)] * 5 + [coef, vmem(16, 128), vmem(10, 40, 128), vmem(2, 160, 128)]
    packs = [vmem(2, 16, 8, 128), vmem(2, 16, 128)] * 2 + [vmem(2, 4, 16, 128)] + [vmem(8, 8, 128), vmem(2, 8, 128)] * 2
    packs += [vmem(8, 128)] * 2
    recv0 = [vmem(2, 4, 16, 128), vmem(2, 16, 8, 128), vmem(4, 2, 8, 128), vmem(18, 16, 128)] * 2
    recv1 = [vmem(2, 3, 8, 128), vmem(2, 8, 8, 128), vmem(4, 3, 8, 128), vmem(18, 8, 128)] * 2
    recv2 = [vmem(44, 8, 128)] * 2
    gather = [vmem(8, 128), vmem(7, 8, 128), vmem(4, 8, 128), vmem(8, 4, 8, 128), vmem(32, 8, 128), vmem(40, 8, 128)]
    dma = pltpu.SemaphoreType.DMA
    token = pltpu.SemaphoreType.REGULAR
    sems = [vmem(400, 8, 128), token, token] + [dma] * 12
    return pl.pallas_call(
        kernel,
        out_shape=jax.ShapeDtypeStruct((BX, BY, BZ), F32),
        in_specs=[pl.BlockSpec(memory_space=pltpu.HBM)],
        out_specs=pl.BlockSpec(memory_space=pltpu.VMEM),
        scratch_shapes=level0 + level1 + level2 + packs + recv0 + recv1 + recv2 + gather + sems,
        compiler_params=pltpu.CompilerParams(
            collective_id=0, has_side_effects=True, vmem_limit_bytes=48 * 1024 * 1024
        ),
    )(pltpu.with_memory_space_constraint(density, pltpu.HBM))


def solution(mesh):
    spec = P("gx", "gy", "gz")
    return jax.shard_map(on_device, mesh=mesh, in_specs=(spec,), out_specs=spec, check_vma=False)
```
